128 devices in a mesh: tp: 4 (over x), dp: 32 (over z, y, core).
Axes of the slice: x: 4, y: 4, z: 4, core: 2. Of those that a mesh axis runs over, the one named last changes fastest.
Arguments:
- x_saved: bfloat16 [32, 1024, 2048], P('dp', 'tp')
- dy_out: bfloat16 [32, 1024, 2048], P('dp', 'tp')
- ln_params: float32 [4, 2048], replicated
- w_qkv: bfloat16 [2048, 16, 3, 128], P(None, 'tp')
- w_out: bfloat16 [2048, 2048], P('tp')
- w_up: bfloat16 [2048, 8192], P(None, 'tp')
- w_down: bfloat16 [8192, 2048], P('tp')
Outputs:
- output 1: bfloat16 [32, 1024, 2048], P('dp', 'tp')
- output 2: float32 [4, 2048], replicated
- output 3: float32 [2048, 16, 3, 128], P('dp', 'tp')
- output 4: float32 [2048, 2048], P(('tp', 'dp'))
- output 5: float32 [2048, 8192], P('dp', 'tp')
- output 6: float32 [8192, 2048], P(('tp', 'dp'))
All inputs are finite; a program needn't handle non-finite values.
Results may differ from the reference program's by a relative error of at most 0.0110607.
Values are sent between devices in bfloat16 or wider.
A program may use at most 1 GiB of HBM per device.

```python
import jax
import jax.numpy as jnp
from jax import lax

NUM_SEQS = 32
SEQ_LEN = 1024
D_MODEL = 2048
NUM_HEADS = 16
KV_HEADS = 16
HEAD_DIM = 128
FF_DIM = 8192
Q_PER_GROUP = NUM_HEADS // KV_HEADS
NORM_EPS = 1e-5
ROPE_BASE = 10000.0


def layer_norm(x_rows, norm_gain, norm_shift):
    row_mean = jnp.mean(x_rows, axis=-1, keepdims=True)
    centered = x_rows - row_mean
    row_var = jnp.mean(centered * centered, axis=-1, keepdims=True)
    return (centered * lax.rsqrt(row_var + NORM_EPS) * norm_gain + norm_shift).astype(jnp.bfloat16)


def rope_tables(positions):
    half_dim = HEAD_DIM // 2
    inv_freq = ROPE_BASE ** (-2.0 * jnp.arange(half_dim, dtype=jnp.float32) / HEAD_DIM)
    angles = positions.astype(jnp.float32)[:, None] * inv_freq[None, :]
    return jnp.cos(angles), jnp.sin(angles)


def apply_rope(tensor, cos_t, sin_t):
    half_dim = tensor.shape[-1] // 2
    t_f32 = tensor.astype(jnp.float32)
    lo_half = t_f32[..., :half_dim]
    hi_half = t_f32[..., half_dim:]
    return jnp.concatenate([lo_half * cos_t - hi_half * sin_t, hi_half * cos_t + lo_half * sin_t], axis=-1).astype(jnp.bfloat16)


def attention(qkv_proj):
    positions = jnp.arange(SEQ_LEN)
    cos_t, sin_t = rope_tables(positions)
    rotated = apply_rope(qkv_proj[:, :, :Q_PER_GROUP + 1, :], cos_t[:, None, None, :], sin_t[:, None, None, :])
    query_rot = rotated[:, :, :Q_PER_GROUP, :]
    key_rot = rotated[:, :, Q_PER_GROUP, :]
    values = qkv_proj[:, :, Q_PER_GROUP + 1, :]
    scores = jnp.einsum('tgqh,sgh->gqts', query_rot.astype(jnp.float32), key_rot.astype(jnp.float32)) * (HEAD_DIM ** -0.5)
    causal = positions[:, None] >= positions[None, :]
    attn_probs = jax.nn.softmax(jnp.where(causal, scores, -1e30), axis=-1).astype(jnp.bfloat16)
    return jnp.einsum('gqts,sgh->tgqh', attn_probs.astype(jnp.float32), values.astype(jnp.float32)).astype(jnp.bfloat16)


def layer_forward(x_seq, ln_params, w_qkv, w_out, w_up, w_down):
    x_f32 = x_seq.astype(jnp.float32)
    h_attn = layer_norm(x_f32, ln_params[0], ln_params[1])
    h_mlp = layer_norm(x_f32, ln_params[2], ln_params[3])
    qkv_proj = jnp.dot(h_attn.astype(jnp.float32), w_qkv.reshape(D_MODEL, -1), preferred_element_type=jnp.float32).astype(jnp.bfloat16)
    context = attention(qkv_proj.reshape(SEQ_LEN, KV_HEADS, Q_PER_GROUP + 2, HEAD_DIM))
    attn_out = jnp.dot(context.reshape(SEQ_LEN, NUM_HEADS * HEAD_DIM).astype(jnp.float32), w_out, preferred_element_type=jnp.float32)
    hidden = jnp.dot(h_mlp.astype(jnp.float32), w_up, preferred_element_type=jnp.float32).astype(jnp.bfloat16)
    gelu_out = jax.nn.gelu(hidden.astype(jnp.float32), approximate=False).astype(jnp.bfloat16)
    mlp_out = jnp.dot(gelu_out.astype(jnp.float32), w_down, preferred_element_type=jnp.float32)
    return x_f32 + attn_out + mlp_out


def setup_inputs(seed: int = 0) -> dict:
    key_list = jax.random.split(jax.random.key(seed), 8)
    act_shape = (NUM_SEQS, SEQ_LEN, D_MODEL)
    x_saved = jax.random.normal(key_list[0], act_shape, jnp.float32)
    shared_dir = jax.random.normal(key_list[1], (NUM_SEQS, 1, D_MODEL), jnp.float32)
    dy_out = 0.6 * shared_dir + 0.8 * jax.random.normal(key_list[2], act_shape, jnp.float32)
    ln_base = jnp.array([1.0, 0.0, 1.0, 0.0], jnp.float32)[:, None]
    ln_spread = jnp.array([0.3, 0.5, 0.3, 0.5], jnp.float32)[:, None]
    ln_params = ln_base + ln_spread * jax.random.normal(key_list[3], (4, D_MODEL), jnp.float32)
    w_qkv = jax.random.normal(key_list[4], (D_MODEL, KV_HEADS, Q_PER_GROUP + 2, HEAD_DIM), jnp.float32) * D_MODEL ** -0.5
    w_out = jax.random.normal(key_list[5], (NUM_HEADS * HEAD_DIM, D_MODEL), jnp.float32) * (NUM_HEADS * HEAD_DIM) ** -0.5
    w_up = jax.random.normal(key_list[6], (D_MODEL, FF_DIM), jnp.float32) * D_MODEL ** -0.5
    w_down = jax.random.normal(key_list[7], (FF_DIM, D_MODEL), jnp.float32) * FF_DIM ** -0.5
    return {'x_saved': x_saved.astype(jnp.bfloat16), 'dy_out': dy_out.astype(jnp.bfloat16), 'ln_params': ln_params, 'w_qkv': w_qkv.astype(jnp.bfloat16), 'w_out': w_out.astype(jnp.bfloat16), 'w_up': w_up.astype(jnp.bfloat16), 'w_down': w_down.astype(jnp.bfloat16)}


def reference(x_saved, dy_out, ln_params, w_qkv, w_out, w_up, w_down):
    weights = (ln_params, w_qkv.astype(jnp.float32), w_out.astype(jnp.float32), w_up.astype(jnp.float32), w_down.astype(jnp.float32))

    def seq_step(grad_sums, seq_pair):
        x_seq, dy_seq = seq_pair
        _, pull_back = jax.vjp(layer_forward, x_seq, *weights)
        grads = pull_back(dy_seq.astype(jnp.float32))
        return tuple(grad_total + grad_part for grad_total, grad_part in zip(grad_sums, grads[1:])), grads[0]

    zero_sums = tuple(jnp.zeros_like(weight) for weight in weights)
    grad_sums, grad_x = lax.scan(seq_step, zero_sums, (x_saved, dy_out))
    return (grad_x, grad_sums[0], grad_sums[1], grad_sums[2], grad_sums[3], grad_sums[4])
```

```python
import functools

import jax
import jax.numpy as jnp
from jax import lax
from jax.experimental import pallas as pl
from jax.experimental.pallas import tpu as pltpu
from jax.sharding import PartitionSpec as P

NORM_EPS = 1e-5
ROPE_BASE = 10000.0
MESH = pl.DeviceIdType.MESH
PIECES = 12
SLOTS = 6
F32 = jnp.float32
BF16 = jnp.bfloat16


def rope_tables(positions, head_dim):
    half_dim = head_dim // 2
    inv_freq = ROPE_BASE ** (-2.0 * jnp.arange(half_dim, dtype=jnp.float32) / head_dim)
    angles = positions.astype(jnp.float32)[:, None] * inv_freq[None, :]
    return jnp.cos(angles), jnp.sin(angles)


def apply_rope(tensor, cos_t, sin_t):
    half_dim = tensor.shape[-1] // 2
    t_f32 = tensor.astype(jnp.float32)
    lo_half = t_f32[..., :half_dim]
    hi_half = t_f32[..., half_dim:]
    return jnp.concatenate([lo_half * cos_t - hi_half * sin_t, hi_half * cos_t + lo_half * sin_t], axis=-1).astype(jnp.bfloat16)


def gelu_bf16(hidden):
    return jax.nn.gelu(hidden.astype(jnp.float32), approximate=False).astype(jnp.bfloat16)


def attention_core(qkv_proj, cos_t, sin_t):
    q_slots = qkv_proj.shape[3] - 2
    positions = jnp.arange(qkv_proj.shape[1])
    rotated = apply_rope(qkv_proj[:, :, :, :q_slots + 1, :], cos_t[:, None, None, :], sin_t[:, None, None, :])
    query_rot = rotated[:, :, :, :q_slots, :]
    key_rot = rotated[:, :, :, q_slots, :]
    values = qkv_proj[:, :, :, q_slots + 1, :]
    scores = jnp.einsum('btgqh,bsgh->bgqts', query_rot, key_rot, preferred_element_type=jnp.float32) * (qkv_proj.shape[4] ** -0.5)
    causal = positions[:, None] >= positions[None, :]
    attn_probs = jax.nn.softmax(jnp.where(causal, scores, -1e30), axis=-1).astype(jnp.bfloat16)
    return jnp.einsum('bgqts,bsgh->btgqh', attn_probs, values, preferred_element_type=jnp.float32).astype(jnp.bfloat16)


def dot_tt(lhs, rhs):
    return lax.dot_general(lhs, rhs, (((0,), (0,)), ((), ())), preferred_element_type=F32)


def grads_kernel(gelu_ref, dy_ref, hm_ref, dhid_ref, ha_ref, dproj_ref, ctx_ref, lng_ref,
                 o_down, o_up, o_qkv, o_out, o_ln,
                 a_buf, b_buf, p_buf, d_buf, l1, f1, l2, f2, lnb,
                 a_sem, b_sem, ds, dr, s_l1, r_l1, s_f1, r_f1, s_l2, r_l2, s_f2, r_f2, ln_s, ln_r, credit):
    tp = lax.axis_index('tp')
    dp = lax.axis_index('dp')
    core = lax.rem(dp, 2)
    y = lax.rem(dp // 2, 4)
    z = dp // 8
    partner = {'dp': dp + 1 - 2 * core}

    def dev_y(i):
        return {'dp': z * 8 + i * 2 + core}

    def dev_z(i):
        return {'dp': i * 8 + y * 2 + core}

    def dev_x(i):
        return {'tp': i}

    def ring(i, d):
        return lax.rem(i + d, 4)

    barrier = pltpu.get_barrier_semaphore()
    peers = [partner]
    for d in (1, 2, 3):
        peers += [dev_x(ring(tp, d)), dev_y(ring(y, d)), dev_z(ring(z, d))]
    for peer in peers:
        pl.semaphore_signal(barrier, inc=1, device_id=peer, device_id_type=MESH)

    def load_a(src, slot):
        return pltpu.make_async_copy(src, a_buf.at[slot], a_sem.at[slot])

    def load_b(src, col, slot):
        return pltpu.make_async_copy(src.at[:, pl.ds(pl.multiple_of(col * 512, 512), 512)], b_buf.at[slot], b_sem.at[slot])

    def start_b(p, slot):
        @pl.when(p < 4)
        def _():
            load_b(dy_ref, p, slot).start()

        @pl.when((p >= 4) & (p < 8))
        def _():
            load_b(dhid_ref, p - 4, slot).start()

        @pl.when((p >= 8) & (p < 11))
        def _():
            load_b(dproj_ref, p - 8, slot).start()

        @pl.when(p == 11)
        def _():
            load_b(ctx_ref, 0, slot).start()

    load_a(gelu_ref, 0).start()
    start_b(jnp.int32(0), 0)
    load_a(hm_ref, 1).start()
    pl.semaphore_wait(barrier, len(peers))

    def remote(src, dst, ssem, rsem, device):
        return pltpu.make_async_remote_copy(src_ref=src, dst_ref=dst, send_sem=ssem, recv_sem=rsem, device_id=device, device_id_type=MESH)

    def drain(ref, sem):
        pltpu.make_async_copy(ref, ref, sem).wait()

    def pair_copy(p):
        return remote(p_buf.at[p % 2, :, :, :, 1 - core], d_buf.at[lax.rem(p, SLOTS)], ds.at[p], dr.at[p], partner)

    def blk1(slot, col, i, half):
        rows = pl.ds(32 * half, 32)
        if col == 0:
            return d_buf.at[slot, 0, :, i, rows, :]
        return d_buf.at[slot, 1, i, :, rows, :]

    def blk2(slot, col, i, half):
        rows = pl.ds(32 * half, 32)
        if col == 0:
            return d_buf.at[slot, 0, i, y, rows, :]
        return d_buf.at[slot, 1, z, i, rows, :]

    me1 = (y, z)
    dev1 = (dev_y, dev_z)
    me2 = (z, y)
    dev2 = (dev_z, dev_y)

    def compute(p):
        ps = lax.rem(p, 2)

        @pl.when(p >= 2)
        def _():
            drain(p_buf.at[ps, :, :, :, 0], ds.at[p - 2])

        @pl.when(p < PIECES - 1)
        def _():
            start_b(p + 1, 1 - ps)

        @pl.when((p == 0) | (p == 8))
        def _():
            load_a(gelu_ref, 0).wait()

        @pl.when((p == 4) | (p == 11))
        def _():
            load_a(gelu_ref, 1).wait()

        load_b(dy_ref, 0, ps).wait()

        @pl.when(p < PIECES - 1)
        def _():
            sa = lax.rem(p // 4, 2)

            @pl.loop(0, 8)
            def _(m):
                lhs = a_buf[sa, :, pl.ds(pl.multiple_of(m * 256, 256), 256)]
                tile = dot_tt(lhs, b_buf[ps])
                for i in range(4):
                    for col in range(2):
                        p_buf[ps, col, m // 2, lax.rem(m, 2) * 2 + i // 2, i % 2] = tile[64 * i:64 * i + 64, 256 * col:256 * col + 256]

        @pl.when(p == PIECES - 1)
        def _():
            @pl.loop(0, 8)
            def _(m):
                k = m // 2
                half = lax.rem(m, 2)
                lhs = b_buf[ps]
                rhs = a_buf[1, :, pl.ds(pl.multiple_of(m * 256, 256), 256)]
                tile = dot_tt(lhs, rhs)
                for i in range(32):
                    p_buf[ps, half, i // 8, (i // 2) % 4, i % 2, pl.ds(pl.multiple_of(k * 16, 16), 16), :] = tile[16 * i:16 * i + 16, :]

        @pl.when(p == 3)
        def _():
            load_a(ha_ref, 0).start()

        @pl.when(p == 7)
        def _():
            load_a(dy_ref, 1).start()

        @pl.when(p >= SLOTS)
        def _():
            pl.semaphore_wait(credit, 1)

        pair_copy(p).start()

    def stage_s(q):
        slot = lax.rem(q, SLOTS)
        ps = lax.rem(q, 2)
        drain(d_buf.at[slot], dr.at[q])

        @pl.loop(0, 32)
        def _(i):
            col, zi, yi = i // 16, lax.rem(i // 4, 4), lax.rem(i, 4)
            d_buf[slot, col, zi, yi] = d_buf[slot, col, zi, yi] + p_buf[ps, col, zi, yi, core]

        for col in range(2):
            me, dev = me1[col], dev1[col]
            nxt, opp, prv = ring(me, 1), ring(me, 2), ring(me, 3)
            remote(blk1(slot, col, opp, 0), l1.at[q, col, 0], s_l1.at[q], r_l1.at[q], dev(nxt)).start()
            remote(blk1(slot, col, opp, 1), l1.at[q, col, 1], s_l1.at[q], r_l1.at[q], dev(prv)).start()
        for col in range(2):
            me, dev = me1[col], dev1[col]
            nxt, prv = ring(me, 1), ring(me, 3)
            remote(blk1(slot, col, nxt, 1), f1.at[q, col, 0, 1], s_f1.at[q], r_f1.at[q], dev(nxt)).start()
            remote(blk1(slot, col, prv, 0), f1.at[q, col, 0, 0], s_f1.at[q], r_f1.at[q], dev(prv)).start()

    def stage_l1(q):
        slot = lax.rem(q, SLOTS)
        drain(l1.at[q], r_l1.at[q])
        for col in range(2):
            me, dev = me1[col], dev1[col]
            nxt, prv = ring(me, 1), ring(me, 3)
            for half, to in ((0, nxt), (1, prv)):
                ref = blk1(slot, col, to, half)
                ref[...] = ref[...] + l1[q, col, half]
                remote(ref, f1.at[q, col, 1, half], s_f1.at[q], r_f1.at[q], dev(to)).start()

    def stage_f1(q):
        slot = lax.rem(q, SLOTS)
        drain(f1.at[q], r_f1.at[q])
        for col in range(2):
            for half in range(2):
                ref = blk1(slot, col, me1[col], half)
                ref[...] = ref[...] + (f1[q, col, 0, half] + f1[q, col, 1, half])
        for col in range(2):
            me, dev = me2[col], dev2[col]
            nxt, opp, prv = ring(me, 1), ring(me, 2), ring(me, 3)
            remote(blk2(slot, col, opp, 0), l2.at[q, col, 0], s_l2.at[q], r_l2.at[q], dev(nxt)).start()
            remote(blk2(slot, col, opp, 1), l2.at[q, col, 1], s_l2.at[q], r_l2.at[q], dev(prv)).start()
        for col in range(2):
            me, dev = me2[col], dev2[col]
            nxt, prv = ring(me, 1), ring(me, 3)
            remote(blk2(slot, col, nxt, 1), f2.at[q, col, 0, 1], s_f2.at[q], r_f2.at[q], dev(nxt)).start()
            remote(blk2(slot, col, prv, 0), f2.at[q, col, 0, 0], s_f2.at[q], r_f2.at[q], dev(prv)).start()

    def stage_l2(q):
        slot = lax.rem(q, SLOTS)
        drain(l2.at[q], r_l2.at[q])
        for col in range(2):
            me, dev = me2[col], dev2[col]
            nxt, prv = ring(me, 1), ring(me, 3)
            for half, to in ((0, nxt), (1, prv)):
                ref = blk2(slot, col, to, half)
                ref[...] = ref[...] + l2[q, col, half]
                remote(ref, f2.at[q, col, 1, half], s_f2.at[q], r_f2.at[q], dev(to)).start()

    def stage_f2(q):
        slot = lax.rem(q, SLOTS)
        drain(f2.at[q], r_f2.at[q])
        for col in range(2):
            for half in range(2):
                rows = pl.ds(32 * half, 32)
                val = blk2(slot, col, me2[col], half)[...] + (f2[q, col, 0, half] + f2[q, col, 1, half])
                for out, lo, hi in ((o_down, 0, 4), (o_up, 4, 8), (o_qkv, 8, 11), (o_out, 11, 12)):
                    @pl.when((q >= lo) & (q < hi))
                    def _():
                        out[rows, pl.ds(pl.multiple_of((q - lo) * 512 + col * 256, 256), 256)] = val
        drain(l1.at[q], s_l1.at[q])
        drain(f1.at[q], s_f1.at[q])
        drain(l2.at[q], s_l2.at[q])
        drain(f2.at[q], s_f2.at[q])

        @pl.when(q < PIECES - SLOTS)
        def _():
            pl.semaphore_signal(credit, inc=1, device_id=partner, device_id_type=MESH)

    def ln_send(stage):
        me, dev, n = ((core, None, 2), (tp, dev_x, 4), (y, dev_y, 4), (z, dev_z, 4))[stage]
        for d in range(1, n):
            to = partner if dev is None else dev(ring(me, d))
            remote(lnb.at[stage, me], lnb.at[stage, me], ln_s.at[stage], ln_r.at[stage], to).start()

    def ln_sum(stage):
        n = 2 if stage == 0 else 4
        ref = lnb.at[stage, pl.ds(0, n - 1)]
        drain(ref, ln_r.at[stage])
        drain(ref, ln_s.at[stage])
        if n == 2:
            return lnb[0, 0] + lnb[0, 1]
        return (lnb[stage, 0] + lnb[stage, 1]) + (lnb[stage, 2] + lnb[stage, 3])

    lnb[0, core] = lng_ref[...]

    @pl.loop(0, PIECES + 5)
    def _(p):
        @pl.when(p < PIECES)
        def _():
            compute(p)

        for lag, stage in ((5, stage_f2), (4, stage_l2), (3, stage_f1), (2, stage_l1), (1, stage_s)):
            @pl.when((p >= lag) & (p < PIECES + lag))
            def _():
                stage(p - lag)

        @pl.when(p == 0)
        def _():
            ln_send(0)
        for stage, me in ((1, tp), (2, y), (3, z)):
            @pl.when(p == stage)
            def _():
                lnb[stage, me] = ln_sum(stage - 1)
                ln_send(stage)

        @pl.when(p == 4)
        def _():
            o_ln[...] = ln_sum(3)

    for p in (PIECES - 2, PIECES - 1):
        drain(p_buf.at[p % 2, :, :, :, 0], ds.at[p])


def grads_call(gelu_out, dy_full, h_mlp, d_hidden, h_attn, d_proj, context, ln_part):
    hbm = pl.BlockSpec(memory_space=pl.ANY)
    vmem = pl.BlockSpec(memory_space=pltpu.VMEM)
    dma = pltpu.SemaphoreType.DMA
    tokens = 1024
    flops = 2 * tokens * 2048 * 512 * PIECES
    return pl.pallas_call(
        grads_kernel,
        out_shape=[jax.ShapeDtypeStruct((64, 2048), F32), jax.ShapeDtypeStruct((64, 2048), F32), jax.ShapeDtypeStruct((64, 1536), F32),
                   jax.ShapeDtypeStruct((64, 512), F32), jax.ShapeDtypeStruct((8, 1024), F32)],
        in_specs=[hbm] * 7 + [vmem],
        out_specs=[vmem] * 5,
        scratch_shapes=[
            pltpu.VMEM((2, tokens, 2048), BF16),
            pltpu.VMEM((2, tokens, 512), BF16),
            pltpu.VMEM((2, 2, 4, 4, 2, 64, 256), F32),
            pltpu.VMEM((SLOTS, 2, 4, 4, 64, 256), F32),
            pltpu.VMEM((PIECES, 2, 2, 4, 32, 256), F32),
            pltpu.VMEM((PIECES, 2, 2, 2, 4, 32, 256), F32),
            pltpu.VMEM((PIECES, 2, 2, 32, 256), F32),
            pltpu.VMEM((PIECES, 2, 2, 2, 32, 256), F32),
            pltpu.VMEM((4, 4, 8, 1024), F32),
            dma((2,)), dma((2,)), dma((PIECES,)), dma((PIECES,)),
            dma((PIECES,)), dma((PIECES,)), dma((PIECES,)), dma((PIECES,)),
            dma((PIECES,)), dma((PIECES,)), dma((PIECES,)), dma((PIECES,)),
            dma((4,)), dma((4,)),
            pltpu.SemaphoreType.REGULAR,
        ],
        compiler_params=pltpu.CompilerParams(collective_id=0, has_side_effects=True, vmem_limit_bytes=64000 * 1024),
        cost_estimate=pl.CostEstimate(flops=flops * 4, bytes_accessed=100_000_000, transcendentals=0),
        name='weight_grads',
    )(gelu_out, dy_full, h_mlp, d_hidden, h_attn, d_proj, context, ln_part)


def solution(mesh):
    def local_step(x_loc, dy_loc, ln_params, w_qkv, w_out, w_up, w_down):
        x_full = lax.all_gather(x_loc, 'tp', axis=1, tiled=True)[0]
        dy_full = lax.all_gather(dy_loc, 'tp', axis=1, tiled=True)[0]
        seq_len, width = x_full.shape
        groups, slots, head_dim = w_qkv.shape[1:]

        def normed(rows):
            row_mean = jnp.mean(rows, axis=-1, keepdims=True)
            centered = rows - row_mean
            row_var = jnp.mean(centered * centered, axis=-1, keepdims=True)
            rstd = lax.rsqrt(row_var + NORM_EPS)
            return centered * rstd, rstd

        x_hat, _ = normed(x_full.astype(F32))
        h_attn = (x_hat * ln_params[0] + ln_params[1]).astype(BF16)
        h_mlp = (x_hat * ln_params[2] + ln_params[3]).astype(BF16)
        w_qkv2 = w_qkv.reshape(width, -1)
        qkv_proj = jnp.dot(h_attn, w_qkv2, preferred_element_type=F32).astype(BF16)
        cos_t, sin_t = rope_tables(jnp.arange(seq_len), head_dim)
        context, attn_pull = jax.vjp(lambda qkv_in: attention_core(qkv_in, cos_t, sin_t), qkv_proj.reshape(1, seq_len, groups, slots, head_dim))
        hidden = jnp.dot(h_mlp, w_up, preferred_element_type=F32).astype(BF16)
        gelu_out, gelu_pull = jax.vjp(gelu_bf16, hidden)

        def dot_nt(lhs, rhs):
            return lax.dot_general(lhs, rhs, (((1,), (1,)), ((), ())), preferred_element_type=F32).astype(BF16)

        d_ctx = dot_nt(dy_full, w_out)
        (d_proj,) = attn_pull(d_ctx.reshape(context.shape))
        d_proj = d_proj.reshape(seq_len, -1)
        d_gelu = dot_nt(dy_full, w_down)
        (d_hidden,) = gelu_pull(d_gelu)
        d_hattn = dot_nt(d_proj, w_qkv2).astype(F32)
        d_hmlp = dot_nt(d_hidden, w_up).astype(F32)
        c_part = (d_hattn * ln_params[0] + d_hmlp * ln_params[2]).astype(BF16)
        ln_part = jnp.stack([jnp.sum(d_hattn * x_hat, 0), jnp.sum(d_hattn, 0), jnp.sum(d_hmlp * x_hat, 0), jnp.sum(d_hmlp, 0)])
        c_loc = lax.psum_scatter(c_part, 'tp', scatter_dimension=0, tiled=True)
        g_down, g_up, g_qkv, g_out, g_ln = grads_call(
            gelu_out, dy_full, h_mlp, d_hidden, h_attn, d_proj, context.reshape(seq_len, -1), ln_part.reshape(8, 1024))
        x_hat_loc, rstd_loc = normed(x_loc[0].astype(F32))
        c_loc = c_loc.astype(F32)
        dx = rstd_loc * (c_loc - jnp.mean(c_loc, -1, keepdims=True) - x_hat_loc * jnp.mean(c_loc * x_hat_loc, -1, keepdims=True))
        grad_x = (dy_loc[0].astype(F32) + dx).astype(BF16)[None]
        g_out = g_out.reshape(4, 16, 512).transpose(1, 0, 2).reshape(16, 2048)
        return grad_x, g_ln.reshape(4, width), g_qkv.reshape(64, groups, slots, head_dim), g_out, g_up, g_down

    act_spec = P('dp', 'tp', None)
    in_specs = (act_spec, act_spec, P(None, None), P(None, 'tp', None, None), P('tp', None), P(None, 'tp'), P('tp', None))
    out_specs = (act_spec, P(None, None), P('dp', 'tp', None, None), P(('tp', 'dp'), None), P('dp', 'tp'), P(('tp', 'dp'), None))
    return jax.shard_map(local_step, mesh=mesh, in_specs=in_specs, out_specs=out_specs, check_vma=False)
```

```python
import functools

import jax
import jax.numpy as jnp
from jax import lax
from jax.experimental import pallas as pl
from jax.experimental.pallas import tpu as pltpu
from jax.sharding import PartitionSpec as P

NORM_EPS = 1e-5
ROPE_BASE = 10000.0
MESH = pl.DeviceIdType.MESH
PIECES = 12
SLOTS = 6
F32 = jnp.float32
BF16 = jnp.bfloat16


def rope_tables(positions, head_dim):
    half_dim = head_dim // 2
    inv_freq = ROPE_BASE ** (-2.0 * jnp.arange(half_dim, dtype=jnp.float32) / head_dim)
    angles = positions.astype(jnp.float32)[:, None] * inv_freq[None, :]
    return jnp.cos(angles), jnp.sin(angles)


def dot_nn(lhs, rhs):
    return lax.dot_general(lhs, rhs, (((1,), (0,)), ((), ())), preferred_element_type=F32)


def dot_nt(lhs, rhs):
    return lax.dot_general(lhs, rhs, (((1,), (1,)), ((), ())), preferred_element_type=F32)


def dot_tt(lhs, rhs):
    return lax.dot_general(lhs, rhs, (((0,), (0,)), ((), ())), preferred_element_type=F32)


def grads_kernel(gelu_ref, dy_ref, hm_ref, dhid_ref, ha_ref, dproj_ref, ctx_ref, lng_ref,
                 o_down, o_up, o_qkv, o_out, o_ln,
                 a_buf, b_buf, p_buf, d_buf, l1, f1, l2, f2, lnb,
                 a_sem, b_sem, ds, dr, s_l1, r_l1, s_f1, r_f1, s_l2, r_l2, s_f2, r_f2, ln_s, ln_r, credit):
    tp = lax.axis_index('tp')
    dp = lax.axis_index('dp')
    core = lax.rem(dp, 2)
    y = lax.rem(dp // 2, 4)
    z = dp // 8
    partner = {'dp': dp + 1 - 2 * core}

    def dev_y(i):
        return {'dp': z * 8 + i * 2 + core}

    def dev_z(i):
        return {'dp': i * 8 + y * 2 + core}

    def dev_x(i):
        return {'tp': i}

    def ring(i, d):
        return lax.rem(i + d, 4)

    barrier = pltpu.get_barrier_semaphore()
    peers = [partner]
    for d in (1, 2, 3):
        peers += [dev_x(ring(tp, d)), dev_y(ring(y, d)), dev_z(ring(z, d))]
    for peer in peers:
        pl.semaphore_signal(barrier, inc=1, device_id=peer, device_id_type=MESH)

    def load_a(src, slot):
        return pltpu.make_async_copy(src, a_buf.at[slot], a_sem.at[slot])

    def load_b(src, col, slot):
        return pltpu.make_async_copy(src.at[:, pl.ds(pl.multiple_of(col * 512, 512), 512)], b_buf.at[slot], b_sem.at[slot])

    def start_b(p, slot):
        @pl.when(p < 4)
        def _():
            load_b(dy_ref, p, slot).start()

        @pl.when((p >= 4) & (p < 8))
        def _():
            load_b(dhid_ref, p - 4, slot).start()

        @pl.when((p >= 8) & (p < 11))
        def _():
            load_b(dproj_ref, p - 8, slot).start()

        @pl.when(p == 11)
        def _():
            load_b(ctx_ref, 0, slot).start()

    load_a(gelu_ref, 0).start()
    start_b(jnp.int32(0), 0)
    load_a(hm_ref, 1).start()
    pl.semaphore_wait(barrier, len(peers))

    def remote(src, dst, ssem, rsem, device):
        return pltpu.make_async_remote_copy(src_ref=src, dst_ref=dst, send_sem=ssem, recv_sem=rsem, device_id=device, device_id_type=MESH)

    def drain(ref, sem):
        pltpu.make_async_copy(ref, ref, sem).wait()

    def pair_copy(p):
        return remote(p_buf.at[p % 2, :, :, :, 1 - core], d_buf.at[lax.rem(p, SLOTS)], ds.at[p], dr.at[p], partner)

    def blk1(slot, col, i, half):
        rows = pl.ds(32 * half, 32)
        if col == 0:
            return d_buf.at[slot, 0, :, i, rows, :]
        return d_buf.at[slot, 1, i, :, rows, :]

    def blk2(slot, col, i, half):
        rows = pl.ds(32 * half, 32)
        if col == 0:
            return d_buf.at[slot, 0, i, y, rows, :]
        return d_buf.at[slot, 1, z, i, rows, :]

    me1 = (y, z)
    dev1 = (dev_y, dev_z)
    me2 = (z, y)
    dev2 = (dev_z, dev_y)

    def compute(p):
        ps = lax.rem(p, 2)

        @pl.when(p >= 2)
        def _():
            drain(p_buf.at[ps, :, :, :, 0], ds.at[p - 2])

        @pl.when(p < PIECES - 1)
        def _():
            start_b(p + 1, 1 - ps)

        @pl.when((p == 0) | (p == 8))
        def _():
            load_a(gelu_ref, 0).wait()

        @pl.when((p == 4) | (p == 11))
        def _():
            load_a(gelu_ref, 1).wait()

        load_b(dy_ref, 0, ps).wait()

        @pl.when(p < PIECES - 1)
        def _():
            sa = lax.rem(p // 4, 2)

            @pl.loop(0, 8)
            def _(m):
                lhs = a_buf[sa, :, pl.ds(pl.multiple_of(m * 256, 256), 256)]
                tile = dot_tt(lhs, b_buf[ps])
                for i in range(4):
                    for col in range(2):
                        p_buf[ps, col, m // 2, lax.rem(m, 2) * 2 + i // 2, i % 2] = tile[64 * i:64 * i + 64, 256 * col:256 * col + 256]

        @pl.when(p == PIECES - 1)
        def _():
            @pl.loop(0, 8)
            def _(m):
                k = m // 2
                half = lax.rem(m, 2)
                lhs = b_buf[ps]
                rhs = a_buf[1, :, pl.ds(pl.multiple_of(m * 256, 256), 256)]
                tile = dot_tt(lhs, rhs)
                for i in range(32):
                    p_buf[ps, half, i // 8, (i // 2) % 4, i % 2, pl.ds(pl.multiple_of(k * 16, 16), 16), :] = tile[16 * i:16 * i + 16, :]

        @pl.when(p == 3)
        def _():
            load_a(ha_ref, 0).start()

        @pl.when(p == 7)
        def _():
            load_a(dy_ref, 1).start()

        @pl.when(p >= SLOTS)
        def _():
            pl.semaphore_wait(credit, 1)

        pair_copy(p).start()

    def stage_s(q):
        slot = lax.rem(q, SLOTS)
        ps = lax.rem(q, 2)
        drain(d_buf.at[slot], dr.at[q])

        @pl.loop(0, 32)
        def _(i):
            col, zi, yi = i // 16, lax.rem(i // 4, 4), lax.rem(i, 4)
            d_buf[slot, col, zi, yi] = d_buf[slot, col, zi, yi] + p_buf[ps, col, zi, yi, core]

        for col in range(2):
            me, dev = me1[col], dev1[col]
            nxt, opp, prv = ring(me, 1), ring(me, 2), ring(me, 3)
            remote(blk1(slot, col, opp, 0), l1.at[q, col, 0], s_l1.at[q], r_l1.at[q], dev(nxt)).start()
            remote(blk1(slot, col, opp, 1), l1.at[q, col, 1], s_l1.at[q], r_l1.at[q], dev(prv)).start()
        for col in range(2):
            me, dev = me1[col], dev1[col]
            nxt, prv = ring(me, 1), ring(me, 3)
            remote(blk1(slot, col, nxt, 1), f1.at[q, col, 0, 1], s_f1.at[q], r_f1.at[q], dev(nxt)).start()
            remote(blk1(slot, col, prv, 0), f1.at[q, col, 0, 0], s_f1.at[q], r_f1.at[q], dev(prv)).start()

    def stage_l1(q):
        slot = lax.rem(q, SLOTS)
        drain(l1.at[q], r_l1.at[q])
        for col in range(2):
            me, dev = me1[col], dev1[col]
            nxt, prv = ring(me, 1), ring(me, 3)
            for half, to in ((0, nxt), (1, prv)):
                ref = blk1(slot, col, to, half)
                ref[...] = ref[...] + l1[q, col, half]
                remote(ref, f1.at[q, col, 1, half], s_f1.at[q], r_f1.at[q], dev(to)).start()

    def stage_f1(q):
        slot = lax.rem(q, SLOTS)
        drain(f1.at[q], r_f1.at[q])
        for col in range(2):
            for half in range(2):
                ref = blk1(slot, col, me1[col], half)
                ref[...] = ref[...] + (f1[q, col, 0, half] + f1[q, col, 1, half])
        for col in range(2):
            me, dev = me2[col], dev2[col]
            nxt, opp, prv = ring(me, 1), ring(me, 2), ring(me, 3)
            remote(blk2(slot, col, opp, 0), l2.at[q, col, 0], s_l2.at[q], r_l2.at[q], dev(nxt)).start()
            remote(blk2(slot, col, opp, 1), l2.at[q, col, 1], s_l2.at[q], r_l2.at[q], dev(prv)).start()
        for col in range(2):
            me, dev = me2[col], dev2[col]
            nxt, prv = ring(me, 1), ring(me, 3)
            remote(blk2(slot, col, nxt, 1), f2.at[q, col, 0, 1], s_f2.at[q], r_f2.at[q], dev(nxt)).start()
            remote(blk2(slot, col, prv, 0), f2.at[q, col, 0, 0], s_f2.at[q], r_f2.at[q], dev(prv)).start()

    def stage_l2(q):
        slot = lax.rem(q, SLOTS)
        drain(l2.at[q], r_l2.at[q])
        for col in range(2):
            me, dev = me2[col], dev2[col]
            nxt, prv = ring(me, 1), ring(me, 3)
            for half, to in ((0, nxt), (1, prv)):
                ref = blk2(slot, col, to, half)
                ref[...] = ref[...] + l2[q, col, half]
                remote(ref, f2.at[q, col, 1, half], s_f2.at[q], r_f2.at[q], dev(to)).start()

    def stage_f2(q):
        slot = lax.rem(q, SLOTS)
        drain(f2.at[q], r_f2.at[q])
        for col in range(2):
            for half in range(2):
                rows = pl.ds(32 * half, 32)
                val = blk2(slot, col, me2[col], half)[...] + (f2[q, col, 0, half] + f2[q, col, 1, half])
                for out, lo, hi in ((o_down, 0, 4), (o_up, 4, 8), (o_qkv, 8, 11)):
                    @pl.when((q >= lo) & (q < hi))
                    def _():
                        out[rows, pl.ds(pl.multiple_of((q - lo) * 512 + col * 256, 256), 256)] = val

                @pl.when(q == 11)
                def _():
                    for k in range(2):
                        lo = (2 * half + k) * 512 + col * 256
                        o_out[:, lo:lo + 256] = val[16 * k:16 * k + 16, :]
        drain(l1.at[q], s_l1.at[q])
        drain(f1.at[q], s_f1.at[q])
        drain(l2.at[q], s_l2.at[q])
        drain(f2.at[q], s_f2.at[q])

        @pl.when(q < PIECES - SLOTS)
        def _():
            pl.semaphore_signal(credit, inc=1, device_id=partner, device_id_type=MESH)

    def ln_send(stage):
        me, dev, n = ((core, None, 2), (tp, dev_x, 4), (y, dev_y, 4), (z, dev_z, 4))[stage]
        for d in range(1, n):
            to = partner if dev is None else dev(ring(me, d))
            remote(lnb.at[stage, me], lnb.at[stage, me], ln_s.at[stage], ln_r.at[stage], to).start()

    def ln_sum(stage):
        n = 2 if stage == 0 else 4
        ref = lnb.at[stage, pl.ds(0, n - 1)]
        drain(ref, ln_r.at[stage])
        drain(ref, ln_s.at[stage])
        if n == 2:
            return lnb[0, 0] + lnb[0, 1]
        return (lnb[stage, 0] + lnb[stage, 1]) + (lnb[stage, 2] + lnb[stage, 3])

    lnb[0, core] = lng_ref[...]

    @pl.loop(0, PIECES + 5)
    def _(p):
        @pl.when(p < PIECES)
        def _():
            compute(p)

        for lag, stage in ((5, stage_f2), (4, stage_l2), (3, stage_f1), (2, stage_l1), (1, stage_s)):
            @pl.when((p >= lag) & (p < PIECES + lag))
            def _():
                stage(p - lag)

        @pl.when(p == 0)
        def _():
            ln_send(0)
        for stage, me in ((1, tp), (2, y), (3, z)):
            @pl.when(p == stage)
            def _():
                lnb[stage, me] = ln_sum(stage - 1)
                ln_send(stage)

        @pl.when(p == 4)
        def _():
            o_ln[...] = ln_sum(3)

    for p in (PIECES - 2, PIECES - 1):
        drain(p_buf.at[p % 2, :, :, :, 0], ds.at[p])


def grads_call(gelu_out, dy_full, h_mlp, d_hidden, h_attn, d_proj, context, ln_part):
    hbm = pl.BlockSpec(memory_space=pl.ANY)
    vmem = pl.BlockSpec(memory_space=pltpu.VMEM)
    dma = pltpu.SemaphoreType.DMA
    tokens = 1024
    flops = 2 * tokens * 2048 * 512 * PIECES
    return pl.pallas_call(
        grads_kernel,
        out_shape=[jax.ShapeDtypeStruct((64, 2048), F32), jax.ShapeDtypeStruct((64, 2048), F32), jax.ShapeDtypeStruct((64, 1536), F32),
                   jax.ShapeDtypeStruct((16, 2048), F32), jax.ShapeDtypeStruct((8, 1024), F32)],
        in_specs=[hbm] * 7 + [vmem],
        out_specs=[vmem] * 5,
        scratch_shapes=[
            pltpu.VMEM((2, tokens, 2048), BF16),
            pltpu.VMEM((2, tokens, 512), BF16),
            pltpu.VMEM((2, 2, 4, 4, 2, 64, 256), F32),
            pltpu.VMEM((SLOTS, 2, 4, 4, 64, 256), F32),
            pltpu.VMEM((PIECES, 2, 2, 4, 32, 256), F32),
            pltpu.VMEM((PIECES, 2, 2, 2, 4, 32, 256), F32),
            pltpu.VMEM((PIECES, 2, 2, 32, 256), F32),
            pltpu.VMEM((PIECES, 2, 2, 2, 32, 256), F32),
            pltpu.VMEM((4, 4, 8, 1024), F32),
            dma((2,)), dma((2,)), dma((PIECES,)), dma((PIECES,)),
            dma((PIECES,)), dma((PIECES,)), dma((PIECES,)), dma((PIECES,)),
            dma((PIECES,)), dma((PIECES,)), dma((PIECES,)), dma((PIECES,)),
            dma((4,)), dma((4,)),
            pltpu.SemaphoreType.REGULAR,
        ],
        compiler_params=pltpu.CompilerParams(collective_id=0, has_side_effects=True, vmem_limit_bytes=64000 * 1024),
        cost_estimate=pl.CostEstimate(flops=flops * 4, bytes_accessed=100_000_000, transcendentals=0),
        name='weight_grads',
    )(gelu_out, dy_full, h_mlp, d_hidden, h_attn, d_proj, context, ln_part)


VMEM_LIMIT = 60000 * 1024


def whole(shape):
    return pl.BlockSpec(shape, lambda i: (0,) * len(shape), pipeline_mode=pl.Buffered(1))


def up_kernel(h_ref, w_ref, gelu_ref, slope_ref):
    @pl.loop(0, 4)
    def _(m):
        rows = pl.ds(pl.multiple_of(m * 256, 256), 256)
        u = dot_nn(h_ref[rows, :], w_ref[...]).astype(BF16).astype(F32)
        cdf = 0.5 * (1.0 + lax.erf(u * (0.5 ** 0.5)))
        gelu_ref[rows, :] = (u * cdf).astype(BF16)
        slope_ref[rows, :] = cdf + u * (jnp.exp(-0.5 * u * u) * ((2.0 * jnp.pi) ** -0.5))


def up_call(h_mlp, w_up):
    t, d = h_mlp.shape
    f, blk = w_up.shape[1], 256
    return pl.pallas_call(
        up_kernel,
        grid=(f // blk,),
        in_specs=[whole((t, d)), pl.BlockSpec((d, blk), lambda i: (0, i))],
        out_specs=[pl.BlockSpec((t, blk), lambda i: (0, i))] * 2,
        out_shape=[jax.ShapeDtypeStruct((t, f), BF16), jax.ShapeDtypeStruct((t, f), F32)],
        compiler_params=pltpu.CompilerParams(vmem_limit_bytes=VMEM_LIMIT),
        cost_estimate=pl.CostEstimate(flops=2 * t * d * f, bytes_accessed=2 * (t * d + d * f + 3 * t * f), transcendentals=2 * t * f),
        name='up',
    )(h_mlp, w_up)


def down_kernel(dy_ref, w_ref, slope_ref, out_ref):
    @pl.loop(0, 4)
    def _(m):
        rows = pl.ds(pl.multiple_of(m * 256, 256), 256)
        d_gelu = dot_nt(dy_ref[rows, :], w_ref[...]).astype(BF16).astype(F32)
        out_ref[rows, :] = (d_gelu * slope_ref[rows, :]).astype(BF16)


def down_call(dy_full, w_down, slope):
    t, d = dy_full.shape
    f, blk = w_down.shape[0], 256
    return pl.pallas_call(
        down_kernel,
        grid=(f // blk,),
        in_specs=[whole((t, d)), pl.BlockSpec((blk, d), lambda i: (i, 0)), pl.BlockSpec((t, blk), lambda i: (0, i))],
        out_specs=pl.BlockSpec((t, blk), lambda i: (0, i)),
        out_shape=jax.ShapeDtypeStruct((t, f), BF16),
        compiler_params=pltpu.CompilerParams(vmem_limit_bytes=VMEM_LIMIT),
        cost_estimate=pl.CostEstimate(flops=2 * t * d * f, bytes_accessed=2 * (t * d + d * f + 3 * t * f), transcendentals=0),
        name='down',
    )(dy_full, w_down, slope)


def attn_kernel(qkv_ref, dy_ref, w_ref, cos_ref, sin_ref, ctx_ref, dqkv_ref, q_s, k_s, dc_s, dk_s, dv_s):
    t, hd = ctx_ref.shape
    blk = 256
    scale = hd ** -0.5

    @pl.loop(0, t // blk)
    def _(m):
        rows = pl.ds(pl.multiple_of(m * blk, blk), blk)
        for i, dst in ((0, q_s), (1, k_s)):
            v = qkv_ref[rows, i * hd:(i + 1) * hd].astype(F32)
            dst[rows, :] = (v * cos_ref[rows, :] + pltpu.roll(v, hd // 2, 1) * sin_ref[rows, :]).astype(BF16)
        dc_s[rows, :] = dot_nt(dy_ref[rows, :], w_ref[...]).astype(BF16)

    def unrope(d, rows):
        d = d.astype(BF16).astype(F32)
        return (d * cos_ref[rows, :] - pltpu.roll(d, hd // 2, 1) * sin_ref[rows, :]).astype(BF16)

    for i in range(t // blk):
        rows, n = slice(i * blk, (i + 1) * blk), (i + 1) * blk
        qi, dci = q_s[rows, :], dc_s[rows, :]
        kn, vn = k_s[:n, :], qkv_ref[:n, 2 * hd:3 * hd]
        s = dot_nt(qi, kn) * scale
        row_id = lax.broadcasted_iota(jnp.int32, (blk, n), 0) + i * blk
        col_id = lax.broadcasted_iota(jnp.int32, (blk, n), 1)
        s = jnp.where(row_id >= col_id, s, -1e30)
        e = jnp.exp(s - jnp.max(s, axis=1, keepdims=True))
        p = e / jnp.sum(e, axis=1, keepdims=True)
        pb = p.astype(BF16)
        ctx_ref[rows, :] = dot_nn(pb, vn).astype(BF16)
        dp = dot_nt(dci, vn).astype(BF16).astype(F32)
        ds = p * (dp - jnp.sum(p * dp, axis=1, keepdims=True))
        dsb = (ds * scale).astype(BF16)
        dqkv_ref[rows, 0:hd] = unrope(dot_nn(dsb, kn), rows)
        dk, dv = dot_tt(dsb, qi), dot_tt(pb, dci)
        lo = n - blk
        dk_s[lo:n, :] = dk[lo:, :]
        dv_s[lo:n, :] = dv[lo:, :]
        if lo:
            dk_s[:lo, :] = dk_s[:lo, :] + dk[:lo, :]
            dv_s[:lo, :] = dv_s[:lo, :] + dv[:lo, :]

    @pl.loop(0, t // blk)
    def _(m):
        rows = pl.ds(pl.multiple_of(m * blk, blk), blk)
        dqkv_ref[rows, hd:2 * hd] = unrope(dk_s[rows, :], rows)
        dqkv_ref[rows, 2 * hd:3 * hd] = dv_s[rows, :].astype(BF16)


def attn_call(qkv, dy_full, w_out, cos_f, sin_f, hd):
    t, d = dy_full.shape
    heads = w_out.shape[0] // hd
    return pl.pallas_call(
        attn_kernel,
        grid=(heads,),
        in_specs=[pl.BlockSpec((t, 3 * hd), lambda i: (0, i)), whole((t, d)), pl.BlockSpec((hd, d), lambda i: (i, 0)),
                  whole((t, hd)), whole((t, hd))],
        out_specs=[pl.BlockSpec((t, hd), lambda i: (0, i)), pl.BlockSpec((t, 3 * hd), lambda i: (0, i))],
        out_shape=[jax.ShapeDtypeStruct((t, heads * hd), BF16), jax.ShapeDtypeStruct((t, 3 * heads * hd), BF16)],
        scratch_shapes=[pltpu.VMEM((t, hd), BF16)] * 3 + [pltpu.VMEM((t, hd), F32)] * 2,
        compiler_params=pltpu.CompilerParams(vmem_limit_bytes=VMEM_LIMIT),
        cost_estimate=pl.CostEstimate(flops=16_000_000_000, bytes_accessed=20_000_000, transcendentals=heads * t * t),
        name='attn',
    )(qkv, dy_full, w_out, cos_f, sin_f)


def inputs_kernel(dproj_ref, dhid_ref, wqkv_ref, wup_ref, x_ref, mean_ref, rstd_ref, ln_ref, c_ref, lng_ref):
    sums = []
    for m in range(4):
        rows = slice(m * 256, (m + 1) * 256)
        dha = dot_nt(dproj_ref[rows, :], wqkv_ref[...]).astype(BF16).astype(F32)
        dhm = dot_nt(dhid_ref[rows, :], wup_ref[...]).astype(BF16).astype(F32)
        x_hat = (x_ref[rows, :].astype(F32) - mean_ref[rows, :]) * rstd_ref[rows, :]
        c_ref[rows, :] = (dha * ln_ref[0:1, :] + dhm * ln_ref[2:3, :]).astype(BF16)
        sums.append([jnp.sum(v, axis=0, keepdims=True) for v in (dha * x_hat, dha, dhm * x_hat, dhm)])
    lng_ref[...] = jnp.concatenate([(sums[0][i] + sums[1][i]) + (sums[2][i] + sums[3][i]) for i in range(4)], axis=0)


def inputs_call(d_proj, d_hidden, w_qkv2, w_up, x_full, mean, rstd, ln_params):
    t, d = x_full.shape
    blk = 256
    n1, n2 = d_proj.shape[1], d_hidden.shape[1]
    return pl.pallas_call(
        inputs_kernel,
        grid=(d // blk,),
        in_specs=[whole((t, n1)), whole((t, n2)), pl.BlockSpec((blk, n1), lambda i: (i, 0)), pl.BlockSpec((blk, n2), lambda i: (i, 0)),
                  pl.BlockSpec((t, blk), lambda i: (0, i)), whole((t, 1)), whole((t, 1)), pl.BlockSpec((4, blk), lambda i: (0, i))],
        out_specs=[pl.BlockSpec((t, blk), lambda i: (0, i)), pl.BlockSpec((4, blk), lambda i: (0, i))],
        out_shape=[jax.ShapeDtypeStruct((t, d), BF16), jax.ShapeDtypeStruct((4, d), F32)],
        compiler_params=pltpu.CompilerParams(vmem_limit_bytes=VMEM_LIMIT),
        cost_estimate=pl.CostEstimate(flops=2 * t * d * (n1 + n2), bytes_accessed=30_000_000, transcendentals=0),
        name='inputs',
    )(d_proj, d_hidden, w_qkv2, w_up, x_full, mean, rstd, ln_params)


def solution(mesh):
    def local_step(x_loc, dy_loc, ln_params, w_qkv, w_out, w_up, w_down):
        x_full = lax.all_gather(x_loc, 'tp', axis=1, tiled=True)[0]
        dy_full = lax.all_gather(dy_loc, 'tp', axis=1, tiled=True)[0]
        seq_len, width = x_full.shape
        groups, slots, head_dim = w_qkv.shape[1:]

        def stats(rows):
            row_mean = jnp.mean(rows, axis=-1, keepdims=True)
            centered = rows - row_mean
            row_var = jnp.mean(centered * centered, axis=-1, keepdims=True)
            return row_mean, lax.rsqrt(row_var + NORM_EPS)

        x_f32 = x_full.astype(F32)
        mean, rstd = stats(x_f32)
        x_hat = (x_f32 - mean) * rstd
        h_attn = (x_hat * ln_params[0] + ln_params[1]).astype(BF16)
        h_mlp = (x_hat * ln_params[2] + ln_params[3]).astype(BF16)
        w_qkv2 = w_qkv.reshape(width, -1)
        qkv_proj = jnp.dot(h_attn, w_qkv2, preferred_element_type=F32).astype(BF16)
        cos_t, sin_t = rope_tables(jnp.arange(seq_len), head_dim)
        cos_f = jnp.concatenate([cos_t, cos_t], axis=1)
        sin_f = jnp.concatenate([-sin_t, sin_t], axis=1)
        gelu_out, slope = up_call(h_mlp, w_up)

        context, d_proj = attn_call(qkv_proj, dy_full, w_out, cos_f, sin_f, head_dim)
        d_hidden = down_call(dy_full, w_down, slope)
        c_part, ln_part = inputs_call(d_proj, d_hidden, w_qkv2, w_up, x_full, mean, rstd, ln_params)
        c_loc = lax.psum_scatter(c_part, 'tp', scatter_dimension=0, tiled=True)
        g_down, g_up, g_qkv, g_out, g_ln = grads_call(
            gelu_out, dy_full, h_mlp, d_hidden, h_attn, d_proj, context, ln_part.reshape(8, 1024))
        x_loc_f32 = x_loc[0].astype(F32)
        mean_loc, rstd_loc = stats(x_loc_f32)
        x_hat_loc = (x_loc_f32 - mean_loc) * rstd_loc
        c_loc = c_loc.astype(F32)
        dx = rstd_loc * (c_loc - jnp.mean(c_loc, -1, keepdims=True) - x_hat_loc * jnp.mean(c_loc * x_hat_loc, -1, keepdims=True))
        grad_x = (dy_loc[0].astype(F32) + dx).astype(BF16)[None]
        return grad_x, g_ln.reshape(4, width), g_qkv.reshape(64, groups, slots, head_dim), g_out, g_up, g_down

    act_spec = P('dp', 'tp', None)
    in_specs = (act_spec, act_spec, P(None, None), P(None, 'tp', None, None), P('tp', None), P(None, 'tp'), P('tp', None))
    out_specs = (act_spec, P(None, None), P('dp', 'tp', None, None), P(('tp', 'dp'), None), P('dp', 'tp'), P(('tp', 'dp'), None))
    return jax.shard_map(local_step, mesh=mesh, in_specs=in_specs, out_specs=out_specs, check_vma=False)
```

```python
import functools

import jax
import jax.numpy as jnp
import numpy as np
from jax import lax
from jax.experimental import pallas as pl
from jax.experimental.pallas import tpu as pltpu
from jax.sharding import PartitionSpec as P

NORM_EPS = 1e-5
ROPE_BASE = 10000.0
MESH = pl.DeviceIdType.MESH
PIECES = 12
SLOTS = 6
F32 = jnp.float32
BF16 = jnp.bfloat16


def rope_tables(seq_len, head_dim):
    half_dim = head_dim // 2
    inv_freq = np.float32(ROPE_BASE) ** (np.float32(-2.0) * np.arange(half_dim, dtype=np.float32) / np.float32(head_dim))
    angles = np.arange(seq_len, dtype=np.float32)[:, None] * inv_freq[None, :].astype(np.float32)
    cos_t, sin_t = np.cos(angles), np.sin(angles)
    return np.concatenate([cos_t, cos_t], axis=1), np.concatenate([-sin_t, sin_t], axis=1)


def dot_nn(lhs, rhs):
    return lax.dot_general(lhs, rhs, (((1,), (0,)), ((), ())), preferred_element_type=F32)


def dot_nt(lhs, rhs):
    return lax.dot_general(lhs, rhs, (((1,), (1,)), ((), ())), preferred_element_type=F32)


def dot_tt(lhs, rhs):
    return lax.dot_general(lhs, rhs, (((0,), (0,)), ((), ())), preferred_element_type=F32)


def grads_kernel(gelu_ref, dy_ref, hm_ref, dhid_ref, ha_ref, dproj_ref, ctx_ref, lng_ref,
                 o_down, o_up, o_qkv, o_out, o_ln,
                 a_buf, b_buf, p_buf, d_buf, l1, f1, l2, f2, lnb,
                 a_sem, b_sem, ds, dr, s_l1, r_l1, s_f1, r_f1, s_l2, r_l2, s_f2, r_f2, ln_s, ln_r, credit):
    tp = lax.axis_index('tp')
    dp = lax.axis_index('dp')
    core = lax.rem(dp, 2)
    y = lax.rem(dp // 2, 4)
    z = dp // 8
    partner = {'dp': dp + 1 - 2 * core}

    def dev_y(i):
        return {'dp': z * 8 + i * 2 + core}

    def dev_z(i):
        return {'dp': i * 8 + y * 2 + core}

    def dev_x(i):
        return {'tp': i}

    def ring(i, d):
        return lax.rem(i + d, 4)

    barrier = pltpu.get_barrier_semaphore()
    peers = [partner]
    for d in (1, 2, 3):
        peers += [dev_x(ring(tp, d)), dev_y(ring(y, d)), dev_z(ring(z, d))]
    for peer in peers:
        pl.semaphore_signal(barrier, inc=1, device_id=peer, device_id_type=MESH)

    def load_a(src, slot):
        return pltpu.make_async_copy(src, a_buf.at[slot], a_sem.at[slot])

    def load_b(src, col, slot):
        return pltpu.make_async_copy(src.at[:, pl.ds(pl.multiple_of(col * 512, 512), 512)], b_buf.at[slot], b_sem.at[slot])

    def start_b(p, slot):
        @pl.when(p < 4)
        def _():
            load_b(dy_ref, p, slot).start()

        @pl.when((p >= 4) & (p < 8))
        def _():
            load_b(dhid_ref, p - 4, slot).start()

        @pl.when((p >= 8) & (p < 11))
        def _():
            load_b(dproj_ref, p - 8, slot).start()

        @pl.when(p == 11)
        def _():
            load_b(ctx_ref, 0, slot).start()

    load_a(gelu_ref, 0).start()
    start_b(jnp.int32(0), 0)
    load_a(hm_ref, 1).start()
    pl.semaphore_wait(barrier, len(peers))

    def remote(src, dst, ssem, rsem, device):
        return pltpu.make_async_remote_copy(src_ref=src, dst_ref=dst, send_sem=ssem, recv_sem=rsem, device_id=device, device_id_type=MESH)

    def drain(ref, sem):
        pltpu.make_async_copy(ref, ref, sem).wait()

    def pair_copy(p):
        return remote(p_buf.at[p % 2, :, :, :, 1 - core], d_buf.at[lax.rem(p, SLOTS)], ds.at[p], dr.at[p], partner)

    def blk1(slot, col, i, half):
        rows = pl.ds(32 * half, 32)
        if col == 0:
            return d_buf.at[slot, 0, :, i, rows, :]
        return d_buf.at[slot, 1, i, :, rows, :]

    def blk2(slot, col, i, half):
        rows = pl.ds(32 * half, 32)
        if col == 0:
            return d_buf.at[slot, 0, i, y, rows, :]
        return d_buf.at[slot, 1, z, i, rows, :]

    me1 = (y, z)
    dev1 = (dev_y, dev_z)
    me2 = (z, y)
    dev2 = (dev_z, dev_y)

    def compute(p):
        ps = lax.rem(p, 2)

        @pl.when(p >= 2)
        def _():
            drain(p_buf.at[ps, :, :, :, 0], ds.at[p - 2])

        @pl.when(p < PIECES - 1)
        def _():
            start_b(p + 1, 1 - ps)

        @pl.when((p == 0) | (p == 8))
        def _():
            load_a(gelu_ref, 0).wait()

        @pl.when((p == 4) | (p == 11))
        def _():
            load_a(gelu_ref, 1).wait()

        load_b(dy_ref, 0, ps).wait()

        @pl.when(p < PIECES - 1)
        def _():
            sa = lax.rem(p // 4, 2)

            @pl.loop(0, 8)
            def _(m):
                lhs = a_buf[sa, :, pl.ds(pl.multiple_of(m * 256, 256), 256)]
                tile = dot_tt(lhs, b_buf[ps])
                for i in range(4):
                    for col in range(2):
                        p_buf[ps, col, m // 2, lax.rem(m, 2) * 2 + i // 2, i % 2] = tile[64 * i:64 * i + 64, 256 * col:256 * col + 256]

        @pl.when(p == PIECES - 1)
        def _():
            @pl.loop(0, 8)
            def _(m):
                k = m // 2
                half = lax.rem(m, 2)
                lhs = b_buf[ps]
                rhs = a_buf[1, :, pl.ds(pl.multiple_of(m * 256, 256), 256)]
                tile = dot_tt(lhs, rhs)
                for i in range(32):
                    p_buf[ps, half, i // 8, (i // 2) % 4, i % 2, pl.ds(pl.multiple_of(k * 16, 16), 16), :] = tile[16 * i:16 * i + 16, :]

        @pl.when(p == 3)
        def _():
            load_a(ha_ref, 0).start()

        @pl.when(p == 7)
        def _():
            load_a(dy_ref, 1).start()

        @pl.when(p >= SLOTS)
        def _():
            pl.semaphore_wait(credit, 1)

        pair_copy(p).start()

    def stage_s(q):
        slot = lax.rem(q, SLOTS)
        ps = lax.rem(q, 2)
        drain(d_buf.at[slot], dr.at[q])

        @pl.loop(0, 32)
        def _(i):
            col, zi, yi = i // 16, lax.rem(i // 4, 4), lax.rem(i, 4)
            d_buf[slot, col, zi, yi] = d_buf[slot, col, zi, yi] + p_buf[ps, col, zi, yi, core]

        for col in range(2):
            me, dev = me1[col], dev1[col]
            nxt, opp, prv = ring(me, 1), ring(me, 2), ring(me, 3)
            remote(blk1(slot, col, opp, 0), l1.at[q, col, 0], s_l1.at[q], r_l1.at[q], dev(nxt)).start()
            remote(blk1(slot, col, opp, 1), l1.at[q, col, 1], s_l1.at[q], r_l1.at[q], dev(prv)).start()
        for col in range(2):
            me, dev = me1[col], dev1[col]
            nxt, prv = ring(me, 1), ring(me, 3)
            remote(blk1(slot, col, nxt, 1), f1.at[q, col, 0, 1], s_f1.at[q], r_f1.at[q], dev(nxt)).start()
            remote(blk1(slot, col, prv, 0), f1.at[q, col, 0, 0], s_f1.at[q], r_f1.at[q], dev(prv)).start()

    def stage_l1(q):
        slot = lax.rem(q, SLOTS)
        drain(l1.at[q], r_l1.at[q])
        for col in range(2):
            me, dev = me1[col], dev1[col]
            nxt, prv = ring(me, 1), ring(me, 3)
            for half, to in ((0, nxt), (1, prv)):
                ref = blk1(slot, col, to, half)
                ref[...] = ref[...] + l1[q, col, half]
                remote(ref, f1.at[q, col, 1, half], s_f1.at[q], r_f1.at[q], dev(to)).start()

    def stage_f1(q):
        slot = lax.rem(q, SLOTS)
        drain(f1.at[q], r_f1.at[q])
        for col in range(2):
            for half in range(2):
                ref = blk1(slot, col, me1[col], half)
                ref[...] = ref[...] + (f1[q, col, 0, half] + f1[q, col, 1, half])
        for col in range(2):
            me, dev = me2[col], dev2[col]
            nxt, opp, prv = ring(me, 1), ring(me, 2), ring(me, 3)
            remote(blk2(slot, col, opp, 0), l2.at[q, col, 0], s_l2.at[q], r_l2.at[q], dev(nxt)).start()
            remote(blk2(slot, col, opp, 1), l2.at[q, col, 1], s_l2.at[q], r_l2.at[q], dev(prv)).start()
        for col in range(2):
            me, dev = me2[col], dev2[col]
            nxt, prv = ring(me, 1), ring(me, 3)
            remote(blk2(slot, col, nxt, 1), f2.at[q, col, 0, 1], s_f2.at[q], r_f2.at[q], dev(nxt)).start()
            remote(blk2(slot, col, prv, 0), f2.at[q, col, 0, 0], s_f2.at[q], r_f2.at[q], dev(prv)).start()

    def stage_l2(q):
        slot = lax.rem(q, SLOTS)
        drain(l2.at[q], r_l2.at[q])
        for col in range(2):
            me, dev = me2[col], dev2[col]
            nxt, prv = ring(me, 1), ring(me, 3)
            for half, to in ((0, nxt), (1, prv)):
                ref = blk2(slot, col, to, half)
                ref[...] = ref[...] + l2[q, col, half]
                remote(ref, f2.at[q, col, 1, half], s_f2.at[q], r_f2.at[q], dev(to)).start()

    def stage_f2(q):
        slot = lax.rem(q, SLOTS)
        drain(f2.at[q], r_f2.at[q])
        for col in range(2):
            for half in range(2):
                rows = pl.ds(32 * half, 32)
                val = blk2(slot, col, me2[col], half)[...] + (f2[q, col, 0, half] + f2[q, col, 1, half])
                for out, lo, hi in ((o_down, 0, 4), (o_up, 4, 8), (o_qkv, 8, 11)):
                    @pl.when((q >= lo) & (q < hi))
                    def _():
                        out[rows, pl.ds(pl.multiple_of((q - lo) * 512 + col * 256, 256), 256)] = val

                @pl.when(q == 11)
                def _():
                    for k in range(2):
                        lo = (2 * half + k) * 512 + col * 256
                        o_out[:, lo:lo + 256] = val[16 * k:16 * k + 16, :]
        drain(l1.at[q], s_l1.at[q])
        drain(f1.at[q], s_f1.at[q])
        drain(l2.at[q], s_l2.at[q])
        drain(f2.at[q], s_f2.at[q])

        @pl.when(q < PIECES - SLOTS)
        def _():
            pl.semaphore_signal(credit, inc=1, device_id=partner, device_id_type=MESH)

    def ln_send(stage):
        me, dev, n = ((core, None, 2), (tp, dev_x, 4), (y, dev_y, 4), (z, dev_z, 4))[stage]
        for d in range(1, n):
            to = partner if dev is None else dev(ring(me, d))
            remote(lnb.at[stage, me], lnb.at[stage, me], ln_s.at[stage], ln_r.at[stage], to).start()

    def ln_sum(stage):
        n = 2 if stage == 0 else 4
        ref = lnb.at[stage, pl.ds(0, n - 1)]
        drain(ref, ln_r.at[stage])
        drain(ref, ln_s.at[stage])
        if n == 2:
            return lnb[0, 0] + lnb[0, 1]
        return (lnb[stage, 0] + lnb[stage, 1]) + (lnb[stage, 2] + lnb[stage, 3])

    lnb[0, core] = lng_ref[...]

    @pl.loop(0, PIECES + 5)
    def _(p):
        @pl.when(p < PIECES)
        def _():
            compute(p)

        for lag, stage in ((5, stage_f2), (4, stage_l2), (3, stage_f1), (2, stage_l1), (1, stage_s)):
            @pl.when((p >= lag) & (p < PIECES + lag))
            def _():
                stage(p - lag)

        @pl.when(p == 0)
        def _():
            ln_send(0)
        for stage, me in ((1, tp), (2, y), (3, z)):
            @pl.when(p == stage)
            def _():
                lnb[stage, me] = ln_sum(stage - 1)
                ln_send(stage)

        @pl.when(p == 4)
        def _():
            o_ln[...] = ln_sum(3)

    for p in (PIECES - 2, PIECES - 1):
        drain(p_buf.at[p % 2, :, :, :, 0], ds.at[p])


def grads_call(gelu_out, dy_full, h_mlp, d_hidden, h_attn, d_proj, context, ln_part):
    hbm = pl.BlockSpec(memory_space=pl.ANY)
    vmem = pl.BlockSpec(memory_space=pltpu.VMEM)
    dma = pltpu.SemaphoreType.DMA
    tokens = 1024
    flops = 2 * tokens * 2048 * 512 * PIECES
    return pl.pallas_call(
        grads_kernel,
        out_shape=[jax.ShapeDtypeStruct((64, 2048), F32), jax.ShapeDtypeStruct((64, 2048), F32), jax.ShapeDtypeStruct((64, 1536), F32),
                   jax.ShapeDtypeStruct((16, 2048), F32), jax.ShapeDtypeStruct((4, 2048), F32)],
        in_specs=[hbm] * 7 + [vmem],
        out_specs=[vmem] * 5,
        scratch_shapes=[
            pltpu.VMEM((2, tokens, 2048), BF16),
            pltpu.VMEM((2, tokens, 512), BF16),
            pltpu.VMEM((2, 2, 4, 4, 2, 64, 256), F32),
            pltpu.VMEM((SLOTS, 2, 4, 4, 64, 256), F32),
            pltpu.VMEM((PIECES, 2, 2, 4, 32, 256), F32),
            pltpu.VMEM((PIECES, 2, 2, 2, 4, 32, 256), F32),
            pltpu.VMEM((PIECES, 2, 2, 32, 256), F32),
            pltpu.VMEM((PIECES, 2, 2, 2, 32, 256), F32),
            pltpu.VMEM((4, 4, 4, 2048), F32),
            dma((2,)), dma((2,)), dma((PIECES,)), dma((PIECES,)),
            dma((PIECES,)), dma((PIECES,)), dma((PIECES,)), dma((PIECES,)),
            dma((PIECES,)), dma((PIECES,)), dma((PIECES,)), dma((PIECES,)),
            dma((4,)), dma((4,)),
            pltpu.SemaphoreType.REGULAR,
        ],
        compiler_params=pltpu.CompilerParams(collective_id=0, has_side_effects=True, vmem_limit_bytes=64000 * 1024),
        cost_estimate=pl.CostEstimate(flops=flops * 4, bytes_accessed=100_000_000, transcendentals=0),
        name='weight_grads',
    )(gelu_out, dy_full, h_mlp, d_hidden, h_attn, d_proj, context, ln_part)


VMEM_LIMIT = 60000 * 1024


def whole(shape):
    return pl.BlockSpec(shape, lambda i: (0,) * len(shape), pipeline_mode=pl.Buffered(1))


def front_kernel(x_ref, dy_ref, ln_ref, wq_ref, wu_ref, wd_ref,
                 o_x, o_dy, o_ha, o_hm, o_qkv, o_gelu, o_dhid, o_w, mean_ref, rstd_ref,
                 x_v, dy_v, w2, wu, wd, wq_b, wq_f, slope, ha, hm, qkv, ge, dh,
                 xs, xr, ds, dr, in_sem, wq_sem, out_sem, fin_sem):
    tp = lax.axis_index('tp')
    nxt, opp, prv = lax.rem(tp + 1, 4), lax.rem(tp + 2, 4), lax.rem(tp + 3, 4)
    d_model = x_ref.shape[1]
    rows = x_ref.shape[0]
    half = rows // 2
    part = wq_b.shape[1]
    barrier = pltpu.get_barrier_semaphore()
    for peer in (nxt, prv):
        pl.semaphore_signal(barrier, inc=1, device_id={'tp': peer}, device_id_type=MESH)

    def wq_copy(i):
        return pltpu.make_async_copy(wq_ref.at[pl.ds(i * part, part)], wq_b.at[i % 2], wq_sem.at[i % 2])

    loads = [pltpu.make_async_copy(x_ref, x_v.at[tp], in_sem.at[0]), pltpu.make_async_copy(dy_ref, dy_v.at[tp], in_sem.at[1]),
             pltpu.make_async_copy(wu_ref, wu, in_sem.at[2]), pltpu.make_async_copy(wd_ref, wd, in_sem.at[3])]
    wq_copy(0).start()
    loads[0].start()
    wq_copy(1).start()
    loads[2].start()
    loads[1].start()
    loads[3].start()
    pl.semaphore_wait(barrier, 2)

    A, B = pl.ds(0, half), pl.ds(half, half)

    def moves(src, buf, ssem, rsem):
        def one(i, ref, slot, piece, to):
            return pltpu.make_async_remote_copy(src_ref=ref, dst_ref=buf.at[slot, piece], send_sem=ssem.at[i], recv_sem=rsem.at[i],
                                                device_id={'tp': to}, device_id_type=MESH)
        return [one(0, src.at[A], tp, A, nxt), one(1, src.at[B], tp, B, prv), one(2, src.at[B], tp, B, nxt), one(3, src.at[A], tp, A, prv),
                one(4, buf.at[prv, A], prv, A, nxt), one(5, buf.at[nxt, B], nxt, B, prv)]

    xm = moves(x_ref, x_v, xs, xr)
    dm = moves(dy_ref, dy_v, ds, dr)
    for i in range(4):
        xm[i].start()

    per = part // 12
    for i in range(wq_ref.shape[0] // part):
        wq_copy(i).wait()

        @pl.loop(0, part // 256)
        def _(r):
            at = pl.ds(pl.multiple_of(r * 256, 256), 256)
            wq_f[at, :] = wq_b[i % 2, at, :].astype(F32)

        if i + 2 < wq_ref.shape[0] // part:
            wq_copy(i + 2).start()
        for j in range(3):
            for g in range(4):
                w2[i * per:(i + 1) * per, g * 384 + j * 128:g * 384 + j * 128 + 128] = wq_f[pl.ds(j * 4 + g, per, stride=12), :].astype(BF16)
    w_out_copy = pltpu.make_async_copy(w2, o_w, fin_sem.at[8])
    w_out_copy.start()

    outs = {}

    def put(kind, n, buf, ref, slot):
        copy = pltpu.make_async_copy(buf.at[n % 2], ref.at[pl.ds(pl.multiple_of(slot * rows, rows), rows)], out_sem.at[kind, n % 2])
        copy.start()
        outs[kind, n % 2] = copy

    def free(kind, n):
        if (kind, n % 2) in outs:
            outs.pop((kind, n % 2)).wait()

    def forward(slot, n):
        s = n % 2
        base = slot * rows
        for kind in range(4):
            free(kind, n)

        @pl.loop(0, rows // 32)
        def _(r):
            at = pl.ds(pl.multiple_of(r * 32, 32), 32)
            to = pl.ds(pl.multiple_of(base + r * 32, 32), 32)
            xf = x_v[slot, at, :].astype(F32)
            mean = jnp.mean(xf, axis=-1, keepdims=True)
            cen = xf - mean
            rstd = lax.rsqrt(jnp.mean(cen * cen, axis=-1, keepdims=True) + NORM_EPS)
            mean_ref[to, :] = mean
            rstd_ref[to, :] = rstd
            x_hat = cen * rstd
            ha[s, at, :] = (x_hat * ln_ref[0:1, :] + ln_ref[1:2, :]).astype(BF16)
            hm[s, at, :] = (x_hat * ln_ref[2:3, :] + ln_ref[3:4, :]).astype(BF16)

        put(0, n, ha, o_ha, slot)
        put(1, n, hm, o_hm, slot)

        @pl.loop(0, 3)
        def _(c):
            cols = pl.ds(pl.multiple_of(c * 512, 512), 512)
            qkv[s, :, cols] = dot_nn(ha[s], w2[:, cols]).astype(BF16)

        put(2, n, qkv, o_qkv, slot)

    def up(slot, n):
        s = n % 2

        @pl.loop(0, 4)
        def _(c):
            cols = pl.ds(pl.multiple_of(c * 512, 512), 512)
            u = dot_nn(hm[s], wu[:, cols]).astype(BF16).astype(F32)
            cdf = 0.5 * (1.0 + lax.erf(u * (0.5 ** 0.5)))
            ge[s, :, cols] = (u * cdf).astype(BF16)
            slope[slot, :, cols] = cdf + u * (jnp.exp(-0.5 * u * u) * ((2.0 * jnp.pi) ** -0.5))

        put(3, n, ge, o_gelu, slot)

    def down(slot, n):
        s = n % 2
        free(4, n)

        @pl.loop(0, 4)
        def _(c):
            cols = pl.ds(pl.multiple_of(c * 512, 512), 512)
            d_gelu = dot_nt(dy_v[slot], wd[cols, :]).astype(BF16).astype(F32)
            dh[s, :, cols] = (d_gelu * slope[slot, :, cols]).astype(BF16)

        put(4, n, dh, o_dhid, slot)

    fins = []

    def keep(buf, ref, slot, i):
        copy = pltpu.make_async_copy(buf.at[slot], ref.at[pl.ds(pl.multiple_of(slot * rows, rows), rows)], fin_sem.at[i])
        copy.start()
        fins.append(copy)

    loads[0].wait()
    forward(tp, 0)
    loads[2].wait()
    up(tp, 0)
    keep(x_v, o_x, tp, 0)
    xm[0].wait_recv()
    xm[4].start()
    xm[1].wait_recv()
    xm[5].start()
    for i in range(4):
        dm[i].start()
    loads[1].wait()
    loads[3].wait()
    down(tp, 0)
    keep(dy_v, o_dy, tp, 4)
    xm[2].wait_recv()
    forward(prv, 1)
    up(prv, 1)
    keep(x_v, o_x, prv, 1)
    xm[3].wait_recv()
    forward(nxt, 2)
    up(nxt, 2)
    keep(x_v, o_x, nxt, 2)
    dm[0].wait_recv()
    dm[4].start()
    dm[1].wait_recv()
    dm[5].start()
    xm[4].wait_recv()
    xm[5].wait_recv()
    forward(opp, 3)
    up(opp, 3)
    keep(x_v, o_x, opp, 3)
    dm[2].wait_recv()
    down(prv, 1)
    keep(dy_v, o_dy, prv, 5)
    dm[3].wait_recv()
    down(nxt, 2)
    keep(dy_v, o_dy, nxt, 6)
    dm[4].wait_recv()
    dm[5].wait_recv()
    down(opp, 3)
    keep(dy_v, o_dy, opp, 7)
    for m in xm + dm:
        m.wait_send()
    for copy in list(outs.values()) + fins + [w_out_copy]:
        copy.wait()


def front_call(x_loc, dy_loc, ln_params, w_rows, w_up, w_down):
    r, d = x_loc.shape
    t, f, n = 4 * r, w_up.shape[1], w_rows.shape[0] * 128 // d
    part = w_rows.shape[0] // 4
    hbm = pl.BlockSpec(memory_space=pl.ANY)
    vmem = pl.BlockSpec(memory_space=pltpu.VMEM)
    dma = pltpu.SemaphoreType.DMA
    shape = jax.ShapeDtypeStruct
    return pl.pallas_call(
        front_kernel,
        in_specs=[hbm, hbm, vmem, hbm, hbm, hbm],
        out_specs=[hbm] * 8 + [vmem] * 2,
        out_shape=[shape((t, d), BF16)] * 4 + [shape((t, n), BF16), shape((t, f), BF16), shape((t, f), BF16), shape((d, n), BF16),
                                               shape((t, 1), F32), shape((t, 1), F32)],
        scratch_shapes=[
            pltpu.VMEM((4, r, d), BF16), pltpu.VMEM((4, r, d), BF16),
            pltpu.VMEM((d, n), BF16), pltpu.VMEM((d, f), BF16), pltpu.VMEM((f, d), BF16),
            pltpu.VMEM((2, part, 128), BF16), pltpu.VMEM((part, 128), F32),
            pltpu.VMEM((4, r, f), F32),
            pltpu.VMEM((2, r, d), BF16), pltpu.VMEM((2, r, d), BF16), pltpu.VMEM((2, r, n), BF16),
            pltpu.VMEM((2, r, f), BF16), pltpu.VMEM((2, r, f), BF16),
            dma((6,)), dma((6,)), dma((6,)), dma((6,)), dma((4,)), dma((2,)), dma((5, 2)), dma((9,)),
        ],
        compiler_params=pltpu.CompilerParams(collective_id=1, has_side_effects=True, vmem_limit_bytes=64000 * 1024),
        cost_estimate=pl.CostEstimate(flops=2 * t * d * (n + 2 * f), bytes_accessed=70_000_000, transcendentals=2 * t * f),
        name='front',
    )(x_loc, dy_loc, ln_params, w_rows, w_up, w_down)


def attn_kernel(qkv_ref, dy_ref, w_ref, cos_ref, sin_ref, ctx_ref, dqkv_ref, q_s, k_s, dc_s, dk_s, dv_s):
    t, hd = ctx_ref.shape
    blk = 256
    scale = hd ** -0.5

    @pl.loop(0, t // blk)
    def _(m):
        rows = pl.ds(pl.multiple_of(m * blk, blk), blk)
        for i, dst in ((0, q_s), (1, k_s)):
            v = qkv_ref[rows, i * hd:(i + 1) * hd].astype(F32)
            dst[rows, :] = (v * cos_ref[rows, :] + pltpu.roll(v, hd // 2, 1) * sin_ref[rows, :]).astype(BF16)
        dc_s[rows, :] = dot_nt(dy_ref[rows, :], w_ref[...]).astype(BF16)

    def unrope(d, rows):
        d = d.astype(BF16).astype(F32)
        return (d * cos_ref[rows, :] - pltpu.roll(d, hd // 2, 1) * sin_ref[rows, :]).astype(BF16)

    for i in range(t // blk):
        rows, n = slice(i * blk, (i + 1) * blk), (i + 1) * blk
        qi, dci = q_s[rows, :], dc_s[rows, :]
        kn, vn = k_s[:n, :], qkv_ref[:n, 2 * hd:3 * hd]
        s = dot_nt(qi, kn) * scale
        row_id = lax.broadcasted_iota(jnp.int32, (blk, n), 0) + i * blk
        col_id = lax.broadcasted_iota(jnp.int32, (blk, n), 1)
        s = jnp.where(row_id >= col_id, s, -1e30)
        e = jnp.exp(s - jnp.max(s, axis=1, keepdims=True))
        p = e / jnp.sum(e, axis=1, keepdims=True)
        pb = p.astype(BF16)
        ctx_ref[rows, :] = dot_nn(pb, vn).astype(BF16)
        dp = dot_nt(dci, vn).astype(BF16).astype(F32)
        ds = p * (dp - jnp.sum(p * dp, axis=1, keepdims=True))
        dsb = (ds * scale).astype(BF16)
        dqkv_ref[rows, 0:hd] = unrope(dot_nn(dsb, kn), rows)
        dk, dv = dot_tt(dsb, qi), dot_tt(pb, dci)
        lo = n - blk
        dk_s[lo:n, :] = dk[lo:, :]
        dv_s[lo:n, :] = dv[lo:, :]
        if lo:
            dk_s[:lo, :] = dk_s[:lo, :] + dk[:lo, :]
            dv_s[:lo, :] = dv_s[:lo, :] + dv[:lo, :]

    @pl.loop(0, t // blk)
    def _(m):
        rows = pl.ds(pl.multiple_of(m * blk, blk), blk)
        dqkv_ref[rows, hd:2 * hd] = unrope(dk_s[rows, :], rows)
        dqkv_ref[rows, 2 * hd:3 * hd] = dv_s[rows, :].astype(BF16)


def attn_call(qkv, dy_full, w_out, cos_f, sin_f, hd):
    t, d = dy_full.shape
    heads = w_out.shape[0] // hd
    return pl.pallas_call(
        attn_kernel,
        grid=(heads,),
        in_specs=[pl.BlockSpec((t, 3 * hd), lambda i: (0, i)), whole((t, d)), pl.BlockSpec((hd, d), lambda i: (i, 0)),
                  whole((t, hd)), whole((t, hd))],
        out_specs=[pl.BlockSpec((t, hd), lambda i: (0, i)), pl.BlockSpec((t, 3 * hd), lambda i: (0, i))],
        out_shape=[jax.ShapeDtypeStruct((t, heads * hd), BF16), jax.ShapeDtypeStruct((t, 3 * heads * hd), BF16)],
        scratch_shapes=[pltpu.VMEM((t, hd), BF16)] * 3 + [pltpu.VMEM((t, hd), F32)] * 2,
        compiler_params=pltpu.CompilerParams(vmem_limit_bytes=VMEM_LIMIT),
        cost_estimate=pl.CostEstimate(flops=16_000_000_000, bytes_accessed=20_000_000, transcendentals=heads * t * t),
        name='attn',
    )(qkv, dy_full, w_out, cos_f, sin_f)


def inputs_kernel(dproj_ref, dhid_ref, wqkv_ref, wup_ref, x_ref, mean_ref, rstd_ref, ln_ref, c_ref, lng_ref):
    dha = dot_nt(dproj_ref[...], wqkv_ref[...]).astype(BF16).astype(F32)
    dhm = dot_nt(dhid_ref[...], wup_ref[...]).astype(BF16).astype(F32)
    x_hat = (x_ref[...].astype(F32) - mean_ref[...]) * rstd_ref[...]
    c_ref[...] = (dha * ln_ref[0:1, :] + dhm * ln_ref[2:3, :]).astype(BF16)
    sums = [jnp.sum(v, axis=0, keepdims=True) for v in (dha * x_hat, dha, dhm * x_hat, dhm)]
    lng_ref[...] = jnp.concatenate(sums, axis=0)


def inputs_call(d_proj, d_hidden, w_qkv2, w_up, x_full, mean, rstd, ln_params):
    t, d = x_full.shape
    blk = 256
    n1, n2 = d_proj.shape[1], d_hidden.shape[1]
    return pl.pallas_call(
        inputs_kernel,
        grid=(d // blk,),
        in_specs=[whole((t, n1)), whole((t, n2)), pl.BlockSpec((blk, n1), lambda i: (i, 0)), pl.BlockSpec((blk, n2), lambda i: (i, 0)),
                  pl.BlockSpec((t, blk), lambda i: (0, i)), whole((t, 1)), whole((t, 1)), pl.BlockSpec((4, blk), lambda i: (0, i))],
        out_specs=[pl.BlockSpec((t, blk), lambda i: (0, i)), pl.BlockSpec((4, blk), lambda i: (0, i))],
        out_shape=[jax.ShapeDtypeStruct((t, d), BF16), jax.ShapeDtypeStruct((4, d), F32)],
        compiler_params=pltpu.CompilerParams(vmem_limit_bytes=VMEM_LIMIT),
        cost_estimate=pl.CostEstimate(flops=2 * t * d * (n1 + n2), bytes_accessed=30_000_000, transcendentals=0),
        name='inputs',
    )(d_proj, d_hidden, w_qkv2, w_up, x_full, mean, rstd, ln_params)


def solution(mesh):
    def local_step(x_loc, dy_loc, ln_params, w_qkv, w_out, w_up, w_down):
        width, groups, slots, head_dim = w_qkv.shape
        seq_len = 4 * x_loc.shape[1]

        def stats(rows):
            row_mean = jnp.mean(rows, axis=-1, keepdims=True)
            centered = rows - row_mean
            row_var = jnp.mean(centered * centered, axis=-1, keepdims=True)
            return row_mean, lax.rsqrt(row_var + NORM_EPS)

        w_rows = w_qkv.transpose(0, 2, 1, 3).reshape(width * slots * groups, head_dim)
        x_full, dy_full, h_attn, h_mlp, qkv_proj, gelu_out, d_hidden, w_qkv2, mean, rstd = front_call(
            x_loc[0], dy_loc[0], ln_params, w_rows, w_up, w_down)
        cos_f, sin_f = rope_tables(seq_len, head_dim)
        context, d_proj = attn_call(qkv_proj, dy_full, w_out, jnp.asarray(cos_f), jnp.asarray(sin_f), head_dim)
        c_part, ln_part = inputs_call(d_proj, d_hidden, w_qkv2, w_up, x_full, mean, rstd, ln_params)
        c_loc = lax.psum_scatter(c_part, 'tp', scatter_dimension=0, tiled=True)
        g_down, g_up, g_qkv, g_out, g_ln = grads_call(
            gelu_out, dy_full, h_mlp, d_hidden, h_attn, d_proj, context, ln_part)
        x_loc_f32 = x_loc[0].astype(F32)
        mean_loc, rstd_loc = stats(x_loc_f32)
        x_hat_loc = (x_loc_f32 - mean_loc) * rstd_loc
        c_loc = c_loc.astype(F32)
        dx = rstd_loc * (c_loc - jnp.mean(c_loc, -1, keepdims=True) - x_hat_loc * jnp.mean(c_loc * x_hat_loc, -1, keepdims=True))
        grad_x = (dy_loc[0].astype(F32) + dx).astype(BF16)[None]
        return grad_x, g_ln, g_qkv.reshape(64, groups, slots, head_dim), g_out, g_up, g_down

    act_spec = P('dp', 'tp', None)
    in_specs = (act_spec, act_spec, P(None, None), P(None, 'tp', None, None), P('tp', None), P(None, 'tp'), P('tp', None))
    out_specs = (act_spec, P(None, None), P('dp', 'tp', None, None), P(('tp', 'dp'), None), P('dp', 'tp'), P(('tp', 'dp'), None))
    return jax.shard_map(local_step, mesh=mesh, in_specs=in_specs, out_specs=out_specs, check_vma=False)
```

```python
import functools

import jax
import jax.numpy as jnp
import numpy as np
from jax import lax
from jax.experimental import pallas as pl
from jax.experimental.pallas import tpu as pltpu
from jax.sharding import PartitionSpec as P

NORM_EPS = 1e-5
ROPE_BASE = 10000.0
MESH = pl.DeviceIdType.MESH
PIECES = 24
SLOTS = 8
STEPS = PIECES + 7
F32 = jnp.float32
BF16 = jnp.bfloat16


def rope_tables(seq_len, head_dim):
    half_dim = head_dim // 2
    inv_freq = np.float32(ROPE_BASE) ** (np.float32(-2.0) * np.arange(half_dim, dtype=np.float32) / np.float32(head_dim))
    angles = np.arange(seq_len, dtype=np.float32)[:, None] * inv_freq[None, :].astype(np.float32)
    cos_t, sin_t = np.cos(angles), np.sin(angles)
    return np.concatenate([cos_t, cos_t], axis=1), np.concatenate([-sin_t, sin_t], axis=1)


def dot_nn(lhs, rhs):
    return lax.dot_general(lhs, rhs, (((1,), (0,)), ((), ())), preferred_element_type=F32)


def dot_nt(lhs, rhs):
    return lax.dot_general(lhs, rhs, (((1,), (1,)), ((), ())), preferred_element_type=F32)


def dot_tt(lhs, rhs):
    return lax.dot_general(lhs, rhs, (((0,), (0,)), ((), ())), preferred_element_type=F32)


def front_kernel(x_ref, dy_ref, ln_ref, cos_ref, sin_ref, wq_ref, wu_ref, wd_ref, wo_ref,
                 o_x, o_dy, o_ha, o_hm, o_qkv, o_gelu, o_dhid, o_dctx, o_w, mean_ref, rstd_ref,
                 x_v, dy_v, w2, wu, wd, wo, wq_b, wq_f, slope, ha, hm, hat, hmt, get, qkv, dh, dc,
                 xs, xr, ds, dr, in_sem, wq_sem, out_sem, fin_sem):
    tp = lax.axis_index('tp')
    nxt, opp, prv = lax.rem(tp + 1, 4), lax.rem(tp + 2, 4), lax.rem(tp + 3, 4)
    d_model = x_ref.shape[1]
    rows = x_ref.shape[0]
    half = rows // 2
    part = wq_b.shape[1]
    barrier = pltpu.get_barrier_semaphore()
    for peer in (nxt, prv):
        pl.semaphore_signal(barrier, inc=1, device_id={'tp': peer}, device_id_type=MESH)

    def wq_copy(i):
        return pltpu.make_async_copy(wq_ref.at[pl.ds(i * part, part)], wq_b.at[i % 2], wq_sem.at[i % 2])

    loads = [pltpu.make_async_copy(x_ref, x_v.at[tp], in_sem.at[0]), pltpu.make_async_copy(dy_ref, dy_v.at[tp], in_sem.at[1]),
             pltpu.make_async_copy(wu_ref, wu, in_sem.at[2]), pltpu.make_async_copy(wd_ref, wd, in_sem.at[3]),
             pltpu.make_async_copy(wo_ref, wo, in_sem.at[4])]
    wq_copy(0).start()
    loads[0].start()
    wq_copy(1).start()
    loads[2].start()
    loads[1].start()
    loads[3].start()
    loads[4].start()
    pl.semaphore_wait(barrier, 2)

    A, B = pl.ds(0, half), pl.ds(half, half)

    def moves(src, buf, ssem, rsem):
        def one(i, ref, slot, piece, to):
            return pltpu.make_async_remote_copy(src_ref=ref, dst_ref=buf.at[slot, piece], send_sem=ssem.at[i], recv_sem=rsem.at[i],
                                                device_id={'tp': to}, device_id_type=MESH)
        return [one(0, src.at[A], tp, A, nxt), one(1, src.at[B], tp, B, prv), one(2, src.at[B], tp, B, nxt), one(3, src.at[A], tp, A, prv),
                one(4, buf.at[prv, A], prv, A, nxt), one(5, buf.at[nxt, B], nxt, B, prv)]

    xm = moves(x_ref, x_v, xs, xr)
    dm = moves(dy_ref, dy_v, ds, dr)
    for i in range(4):
        xm[i].start()

    per = part // 12
    for i in range(wq_ref.shape[0] // part):
        wq_copy(i).wait()

        @pl.loop(0, part // 256)
        def _(r):
            at = pl.ds(pl.multiple_of(r * 256, 256), 256)
            wq_f[at, :] = wq_b[i % 2, at, :].astype(F32)

        if i + 2 < wq_ref.shape[0] // part:
            wq_copy(i + 2).start()
        for j in range(3):
            for g in range(4):
                w2[i * per:(i + 1) * per, g * 384 + j * 128:g * 384 + j * 128 + 128] = wq_f[pl.ds(j * 4 + g, per, stride=12), :].astype(BF16)
    w_out_copy = pltpu.make_async_copy(w2, o_w, fin_sem.at[8])
    w_out_copy.start()

    outs = {}

    def start(kind, n, src, dst):
        copy = pltpu.make_async_copy(src, dst, out_sem.at[kind, n % 2])
        copy.start()
        outs[kind, n % 2] = copy

    def put(kind, n, buf, ref, slot):
        start(kind, n, buf.at[n % 2], ref.at[pl.ds(pl.multiple_of(slot * rows, rows), rows)])

    def put_t(kind, buf, ref, slot):
        start(kind, 0, buf, ref.at[:, pl.ds(pl.multiple_of(slot * rows, rows), rows)])

    def free(kind, n):
        if (kind, n % 2) in outs:
            outs.pop((kind, n % 2)).wait()

    def forward(slot, n):
        s = n % 2
        base = slot * rows

        @pl.loop(0, rows // 32)
        def _(r):
            at = pl.ds(pl.multiple_of(r * 32, 32), 32)
            to = pl.ds(pl.multiple_of(base + r * 32, 32), 32)
            xf = x_v[slot, at, :].astype(F32)
            mean = jnp.mean(xf, axis=-1, keepdims=True)
            cen = xf - mean
            rstd = lax.rsqrt(jnp.mean(cen * cen, axis=-1, keepdims=True) + NORM_EPS)
            mean_ref[to, :] = mean
            rstd_ref[to, :] = rstd
            x_hat = cen * rstd
            ha[at, :] = (x_hat * ln_ref[0:1, :] + ln_ref[1:2, :]).astype(BF16)
            hm[at, :] = (x_hat * ln_ref[2:3, :] + ln_ref[3:4, :]).astype(BF16)

        for kind in (0, 1, 3):
            free(kind, 0)
        free(2, n)

        @pl.loop(0, d_model // 256)
        def _(c):
            cols = pl.ds(pl.multiple_of(c * 256, 256), 256)
            hat[cols, :] = ha[:, cols].T
            hmt[cols, :] = hm[:, cols].T

        put_t(0, hat, o_ha, slot)
        put_t(1, hmt, o_hm, slot)
        pos = pl.ds(pl.multiple_of(base, rows), rows)
        cos_t, sin_t = cos_ref[pos, :], sin_ref[pos, :]

        @pl.loop(0, 4)
        def _(g):
            cols = pl.ds(pl.multiple_of(g * 384, 128), 384)
            t = dot_nn(ha[...], w2[:, cols]).astype(BF16)
            for j in range(2):
                v = t[:, j * 128:j * 128 + 128].astype(F32)
                qkv[s, :, pl.ds(pl.multiple_of(g * 384 + j * 128, 128), 128)] = (v * cos_t + pltpu.roll(v, 64, 1) * sin_t).astype(BF16)
            qkv[s, :, pl.ds(pl.multiple_of(g * 384 + 256, 128), 128)] = t[:, 256:384]

        put(2, n, qkv, o_qkv, slot)

    def up(slot, n):
        @pl.loop(0, 4)
        def _(c):
            cols = pl.ds(pl.multiple_of(c * 512, 512), 512)
            u = dot_nn(hm[...], wu[:, cols]).astype(BF16).astype(F32)
            cdf = 0.5 * (1.0 + lax.erf(u * (0.5 ** 0.5)))
            get[cols, :] = (u * cdf).astype(BF16).T
            slope[slot, :, cols] = cdf + u * (jnp.exp(-0.5 * u * u) * ((2.0 * jnp.pi) ** -0.5))

        put_t(3, get, o_gelu, slot)

    def down(slot, n):
        s = n % 2
        free(4, n)
        free(5, n)
        dc[s] = dot_nt(dy_v[slot], wo[...]).astype(BF16)
        put(5, n, dc, o_dctx, slot)

        @pl.loop(0, 4)
        def _(c):
            cols = pl.ds(pl.multiple_of(c * 512, 512), 512)
            d_gelu = dot_nt(dy_v[slot], wd[cols, :]).astype(BF16).astype(F32)
            dh[s, :, cols] = (d_gelu * slope[slot, :, cols]).astype(BF16)

        put(4, n, dh, o_dhid, slot)

    fins = []

    def keep(buf, ref, slot, i):
        copy = pltpu.make_async_copy(buf.at[slot], ref.at[pl.ds(pl.multiple_of(slot * rows, rows), rows)], fin_sem.at[i])
        copy.start()
        fins.append(copy)

    loads[0].wait()
    forward(tp, 0)
    loads[2].wait()
    up(tp, 0)
    keep(x_v, o_x, tp, 0)
    xm[0].wait_recv()
    xm[4].start()
    xm[1].wait_recv()
    xm[5].start()
    for i in range(4):
        dm[i].start()
    loads[1].wait()
    loads[3].wait()
    loads[4].wait()
    down(tp, 0)
    keep(dy_v, o_dy, tp, 4)
    xm[2].wait_recv()
    forward(prv, 1)
    up(prv, 1)
    keep(x_v, o_x, prv, 1)
    xm[3].wait_recv()
    forward(nxt, 2)
    up(nxt, 2)
    keep(x_v, o_x, nxt, 2)
    dm[0].wait_recv()
    dm[4].start()
    dm[1].wait_recv()
    dm[5].start()
    xm[4].wait_recv()
    xm[5].wait_recv()
    forward(opp, 3)
    up(opp, 3)
    keep(x_v, o_x, opp, 3)
    dm[2].wait_recv()
    down(prv, 1)
    keep(dy_v, o_dy, prv, 5)
    dm[3].wait_recv()
    down(nxt, 2)
    keep(dy_v, o_dy, nxt, 6)
    dm[4].wait_recv()
    dm[5].wait_recv()
    down(opp, 3)
    keep(dy_v, o_dy, opp, 7)
    for m in xm + dm:
        m.wait_send()
    for copy in list(outs.values()) + fins + [w_out_copy]:
        copy.wait()


def front_call(x_loc, dy_loc, ln_params, cos_f, sin_f, w_rows, w_up, w_down, w_out):
    r, d = x_loc.shape
    t, f, n, m = 4 * r, w_up.shape[1], w_rows.shape[0] * 128 // d, w_out.shape[0]
    part = w_rows.shape[0] // 4
    hbm = pl.BlockSpec(memory_space=pl.ANY)
    vmem = pl.BlockSpec(memory_space=pltpu.VMEM)
    dma = pltpu.SemaphoreType.DMA
    shape = jax.ShapeDtypeStruct
    return pl.pallas_call(
        front_kernel,
        in_specs=[hbm, hbm, vmem, vmem, vmem, hbm, hbm, hbm, hbm],
        out_specs=[hbm] * 9 + [vmem] * 2,
        out_shape=[shape((t, d), BF16)] * 2 + [shape((d, t), BF16)] * 2 + [
            shape((t, n), BF16), shape((f, t), BF16), shape((t, f), BF16), shape((t, m), BF16), shape((d, n), BF16),
            shape((t, 1), F32), shape((t, 1), F32)],
        scratch_shapes=[
            pltpu.VMEM((4, r, d), BF16), pltpu.VMEM((4, r, d), BF16),
            pltpu.VMEM((d, n), BF16), pltpu.VMEM((d, f), BF16), pltpu.VMEM((f, d), BF16), pltpu.VMEM((m, d), BF16),
            pltpu.VMEM((2, part, 128), BF16), pltpu.VMEM((part, 128), F32),
            pltpu.VMEM((4, r, f), F32),
            pltpu.VMEM((r, d), BF16), pltpu.VMEM((r, d), BF16),
            pltpu.VMEM((d, r), BF16), pltpu.VMEM((d, r), BF16), pltpu.VMEM((f, r), BF16),
            pltpu.VMEM((2, r, n), BF16), pltpu.VMEM((2, r, f), BF16), pltpu.VMEM((2, r, m), BF16),
            dma((6,)), dma((6,)), dma((6,)), dma((6,)), dma((5,)), dma((2,)), dma((6, 2)), dma((9,)),
        ],
        compiler_params=pltpu.CompilerParams(collective_id=1, has_side_effects=True, vmem_limit_bytes=64000 * 1024),
        cost_estimate=pl.CostEstimate(flops=2 * t * d * (n + 2 * f), bytes_accessed=70_000_000, transcendentals=2 * t * f),
        name='front',
    )(x_loc, dy_loc, ln_params, cos_f, sin_f, w_rows, w_up, w_down, w_out)


def back_kernel(get_ref, hmt_ref, hat_ref, dy_ref, dhid_ref, qkv_ref, dctx_ref, w2_ref, wup_ref, x_ref, xloc_ref, dyloc_ref,
                ln_ref, mean_ref, rstd_ref, cos_ref, sin_ref,
                o_gx, o_ln, o_qkv, o_out, o_up, o_down,
                a_buf, b_buf, p_buf, d_buf, l1, f1, l2, f2, lnb, dh_v, dproj_v, ctxt, qkv_b, dctx_b, dk_s, dv_s,
                wq_t, wu_t, x_t, c_buf, cl1, cf1, c_loc,
                a_sem, b_sem, dh_sem, h_sem, t_sem, g_sem, ds, dr, s_l1, r_l1, s_f1, r_f1, s_l2, r_l2, s_f2, r_f2, ln_s, ln_r,
                cs_l1, cr_l1, cs_f1, cr_f1, credit):
    tp = lax.axis_index('tp')
    dp = lax.axis_index('dp')
    core = lax.rem(dp, 2)
    y = lax.rem(dp // 2, 4)
    z = dp // 8
    partner = {'dp': dp + 1 - 2 * core}
    n_head = 4
    hd = 128
    blk = 256
    scale = hd ** -0.5

    def dev_y(i):
        return {'dp': z * 8 + i * 2 + core}

    def dev_z(i):
        return {'dp': i * 8 + y * 2 + core}

    def dev_x(i):
        return {'tp': i}

    def ring(i, d):
        return lax.rem(i + d, 4)

    def al(i, m):
        return pl.multiple_of(i * m, m)

    barrier = pltpu.get_barrier_semaphore()
    peers = [partner]
    for d in (1, 2, 3):
        peers += [dev_x(ring(tp, d)), dev_y(ring(y, d)), dev_z(ring(z, d))]
    for peer in peers:
        pl.semaphore_signal(barrier, inc=1, device_id=peer, device_id_type=MESH)

    def load_a(src, slot):
        return [pltpu.make_async_copy(src.at[pl.ds(1024 * w, 1024)], a_buf.at[slot, w], a_sem.at[slot, w]) for w in range(2)]

    def load_dy():
        return [pltpu.make_async_copy(dy_ref.at[:, pl.ds(1024 * w, 1024)], a_buf.at[1, w], a_sem.at[1, w]) for w in range(2)]

    def load_last():
        out = []
        for w in range(2):
            for i, src in enumerate((xloc_ref, dyloc_ref)):
                out.append(pltpu.make_async_copy(src.at[:, pl.ds(1024 * w, 1024)], a_buf.at[0, w, pl.ds(256 * i, 256)], g_sem.at[w, i]))
        return out

    def load_b(p, slot):
        return pltpu.make_async_copy(dy_ref.at[:, pl.ds(al(p, 256), 256)], b_buf.at[slot], b_sem.at[slot])

    def load_head(h, slot):
        return [pltpu.make_async_copy(qkv_ref.at[:, pl.ds(pl.multiple_of(h * 384, 128), 384)], qkv_b.at[slot], h_sem.at[slot, 0]),
                pltpu.make_async_copy(dctx_ref.at[:, pl.ds(al(h, 128), 128)], dctx_b.at[slot], h_sem.at[slot, 1])]

    def load_t(u, slot):
        at = pl.ds(al(u, 256), 256)
        return [pltpu.make_async_copy(w2_ref.at[at], wq_t.at[slot], t_sem.at[slot, 0]),
                pltpu.make_async_copy(wup_ref.at[at], wu_t.at[slot], t_sem.at[slot, 1]),
                pltpu.make_async_copy(x_ref.at[:, at], x_t.at[slot], t_sem.at[slot, 2])]

    def start(copies):
        for copy in copies:
            copy.start()

    def wait(copies):
        for copy in copies:
            copy.wait()

    start(load_a(get_ref, 0))
    load_b(jnp.int32(0), 0).start()
    start(load_head(jnp.int32(0), 0))
    start(load_a(hmt_ref, 1))
    dh_load = pltpu.make_async_copy(dhid_ref, dh_v, dh_sem)
    dh_load.start()
    pl.semaphore_wait(barrier, len(peers))

    def remote(src, dst, ssem, rsem, device):
        return pltpu.make_async_remote_copy(src_ref=src, dst_ref=dst, send_sem=ssem, recv_sem=rsem, device_id=device, device_id_type=MESH)

    def drain(ref, sem):
        pltpu.make_async_copy(ref, ref, sem).wait()

    def pair_copy(p):
        slot = lax.rem(p, SLOTS)
        return remote(p_buf.at[lax.rem(p, 2), :, :, :, 1 - core], d_buf.at[slot], ds.at[slot], dr.at[slot], partner)

    def blk1(slot, col, i, half):
        rows = pl.ds(32 * half, 32)
        if col == 0:
            return d_buf.at[slot, 0, :, i, rows, :]
        return d_buf.at[slot, 1, i, :, rows, :]

    def blk2(slot, col, i, half):
        rows = pl.ds(32 * half, 32)
        if col == 0:
            return d_buf.at[slot, 0, i, y, rows, :]
        return d_buf.at[slot, 1, z, i, rows, :]

    me1 = (y, z)
    dev1 = (dev_y, dev_z)
    me2 = (z, y)
    dev2 = (dev_z, dev_y)

    def compute(p):
        ps = lax.rem(p, 2)

        @pl.when(p >= 2)
        def _():
            drain(p_buf.at[ps, :, :, :, 0], ds.at[lax.rem(p - 2, SLOTS)])

        @pl.when(p < 7)
        def _():
            load_b(p + 1, 1 - ps).start()

        @pl.when((p == 0) | (p == 16))
        def _():
            wait(load_a(get_ref, 0))

        @pl.when((p == 8) | (p == 22))
        def _():
            wait(load_a(get_ref, 1))

        @pl.when(p < 8)
        def _():
            load_b(p, ps).wait()

        @pl.when(p == 8)
        def _():
            dh_load.wait()

        @pl.when((p >= 8) & (p < 16))
        def _():
            b_buf[ps] = dh_v[:, pl.ds(al(p - 8, 256), 256)]

        @pl.when((p >= 16) & (p < 22))
        def _():
            b_buf[ps] = dproj_v[:, pl.ds(al(p - 16, 256), 256)]

        @pl.when(p < 22)
        def _():
            sa = lax.rem(p // 8, 2)

            @pl.loop(0, 2)
            def _(h):
                tile = dot_nn(a_buf[sa, h], b_buf[ps])
                for i in range(16):
                    for col in range(2):
                        p_buf[ps, col, 2 * h + i // 8, (i // 2) % 4, i % 2] = tile[64 * i:64 * i + 64, 128 * col:128 * col + 128]

        @pl.when(p >= 22)
        def _():
            @pl.loop(0, 4)
            def _(k):
                tile = dot_nn(ctxt[...], a_buf[1, p - 22, :, pl.ds(al(k, 256), 256)])
                for i in range(32):
                    for col in range(2):
                        p_buf[ps, col, i // 8, (i // 2) % 4, i % 2, pl.ds(al(k, 16), 16), :] = tile[16 * i:16 * i + 16, 128 * col:128 * col + 128]

        @pl.when(p == 7)
        def _():
            start(load_a(hat_ref, 0))

        @pl.when(p == 15)
        def _():
            start(load_dy())

        @pl.when(p == 21)
        def _():
            start(load_last())

        @pl.when(p >= SLOTS)
        def _():
            pl.semaphore_wait(credit.at[0], 1)

        pair_copy(p).start()

    def first(blk, slot, me, dev, lands, finals, s_a, r_a, s_b, r_b):
        for col in range(2):
            nxt, opp, prv = ring(me[col], 1), ring(me[col], 2), ring(me[col], 3)
            remote(blk(slot, col, opp, 0), lands.at[slot, col, 0], s_a.at[slot], r_a.at[slot], dev[col](nxt)).start()
            remote(blk(slot, col, opp, 1), lands.at[slot, col, 1], s_a.at[slot], r_a.at[slot], dev[col](prv)).start()
        for col in range(2):
            nxt, prv = ring(me[col], 1), ring(me[col], 3)
            remote(blk(slot, col, nxt, 1), finals.at[slot, col, 0, 1], s_b.at[slot], r_b.at[slot], dev[col](nxt)).start()
            remote(blk(slot, col, prv, 0), finals.at[slot, col, 0, 0], s_b.at[slot], r_b.at[slot], dev[col](prv)).start()

    def second(blk, slot, me, dev, lands, finals, r_a, s_b, r_b):
        drain(lands.at[slot], r_a.at[slot])
        for col in range(2):
            nxt, prv = ring(me[col], 1), ring(me[col], 3)
            for half, to in ((0, nxt), (1, prv)):
                ref = blk(slot, col, to, half)
                ref[...] = ref[...] + lands[slot, col, half]
                remote(ref, finals.at[slot, col, 1, half], s_b.at[slot], r_b.at[slot], dev[col](to)).start()

    def stage_s(q):
        slot = lax.rem(q, SLOTS)
        ps = lax.rem(q, 2)
        drain(d_buf.at[slot], dr.at[slot])

        @pl.loop(0, 32)
        def _(i):
            col, zi, yi = i // 16, lax.rem(i // 4, 4), lax.rem(i, 4)
            d_buf[slot, col, zi, yi] = d_buf[slot, col, zi, yi] + p_buf[ps, col, zi, yi, core]

        @pl.when(q >= SLOTS)
        def _():
            for i in range(1, 5):
                pl.semaphore_wait(credit.at[i], 1)

        first(blk1, slot, me1, dev1, l1, f1, s_l1, r_l1, s_f1, r_f1)

    def stage_l1(q):
        second(blk1, lax.rem(q, SLOTS), me1, dev1, l1, f1, r_l1, s_f1, r_f1)

    def stage_f1(q):
        slot = lax.rem(q, SLOTS)
        drain(f1.at[slot], r_f1.at[slot])
        for col in range(2):
            for half in range(2):
                ref = blk1(slot, col, me1[col], half)
                ref[...] = ref[...] + (f1[slot, col, 0, half] + f1[slot, col, 1, half])
        first(blk2, slot, me2, dev2, l2, f2, s_l2, r_l2, s_f2, r_f2)

    def stage_l2(q):
        second(blk2, lax.rem(q, SLOTS), me2, dev2, l2, f2, r_l2, s_f2, r_f2)

    def stage_f2(q):
        slot = lax.rem(q, SLOTS)
        drain(f2.at[slot], r_f2.at[slot])
        for col in range(2):
            for half in range(2):
                rows = pl.ds(32 * half, 32)
                val = blk2(slot, col, me2[col], half)[...] + (f2[slot, col, 0, half] + f2[slot, col, 1, half])
                for out, lo, hi in ((o_down, 0, 8), (o_up, 8, 16), (o_qkv, 16, 22)):
                    @pl.when((q >= lo) & (q < hi))
                    def _():
                        out[rows, pl.ds(pl.multiple_of((q - lo) * 256 + col * 128, 128), 128)] = val

                @pl.when(q >= 22)
                def _():
                    for k in range(2):
                        at = (q - 22) * 1024 + (2 * half + k) * 256 + col * 128
                        o_out[:, pl.ds(pl.multiple_of(at, 128), 128)] = val[16 * k:16 * k + 16, :]
        drain(l1.at[slot], s_l1.at[slot])
        drain(f1.at[slot], s_f1.at[slot])
        drain(l2.at[slot], s_l2.at[slot])
        drain(f2.at[slot], s_f2.at[slot])

        @pl.when(q < PIECES - SLOTS)
        def _():
            to = (partner, dev_y(ring(y, 1)), dev_y(ring(y, 3)), dev_z(ring(z, 1)), dev_z(ring(z, 3)))
            for i in range(5):
                pl.semaphore_signal(credit.at[i], inc=1, device_id=to[i], device_id_type=MESH)

    def ln_send(stage):
        me, dev, n = ((core, None, 2), (tp, dev_x, 4), (y, dev_y, 4), (z, dev_z, 4))[stage]
        for d in range(1, n):
            to = partner if dev is None else dev(ring(me, d))
            remote(lnb.at[stage, me], lnb.at[stage, me], ln_s.at[stage], ln_r.at[stage], to).start()

    def ln_sum(stage):
        n = 2 if stage == 0 else 4
        ref = lnb.at[stage, pl.ds(0, n - 1)]
        drain(ref, ln_r.at[stage])
        drain(ref, ln_s.at[stage])
        if n == 2:
            return lnb[0, 0] + lnb[0, 1]
        return (lnb[stage, 0] + lnb[stage, 1]) + (lnb[stage, 2] + lnb[stage, 3])

    def unrope(d, rows):
        d = d.astype(BF16).astype(F32)
        return (d * cos_ref[rows, :] - pltpu.roll(d, hd // 2, 1) * sin_ref[rows, :]).astype(BF16)

    def attend(h, i):
        hs = lax.rem(h, 2)
        if i == 0:
            wait(load_head(h, hs))

            @pl.when(h < n_head - 1)
            def _():
                start(load_head(h + 1, 1 - hs))

        rows, n = slice(i * blk, (i + 1) * blk), (i + 1) * blk
        qi, dci = qkv_b[hs, rows, 0:hd], dctx_b[hs, rows, :]
        kn, vn = qkv_b[hs, :n, hd:2 * hd], qkv_b[hs, :n, 2 * hd:3 * hd]
        s = dot_nt(qi, kn) * scale
        row_id = lax.broadcasted_iota(jnp.int32, (blk, n), 0) + i * blk
        col_id = lax.broadcasted_iota(jnp.int32, (blk, n), 1)
        s = jnp.where(row_id >= col_id, s, -1e30)
        e = jnp.exp(s - jnp.max(s, axis=1, keepdims=True))
        p = e / jnp.sum(e, axis=1, keepdims=True)
        pb = p.astype(BF16)
        ctxt[pl.ds(al(h, hd), hd), rows] = dot_nn(pb, vn).astype(BF16).T
        dp_ = dot_nt(dci, vn).astype(BF16).astype(F32)
        dsb = (p * (dp_ - jnp.sum(p * dp_, axis=1, keepdims=True)) * scale).astype(BF16)

        def cols(j):
            return pl.ds(pl.multiple_of(h * 384 + j * 128, 128), 128)

        dproj_v[rows, cols(0)] = unrope(dot_nn(dsb, kn), rows)
        dk, dv = dot_tt(dsb, qi), dot_tt(pb, dci)
        lo = n - blk
        dk_s[lo:n, :] = dk[lo:, :]
        dv_s[lo:n, :] = dv[lo:, :]
        if lo:
            dk_s[:lo, :] = dk_s[:lo, :] + dk[:lo, :]
            dv_s[:lo, :] = dv_s[:lo, :] + dv[:lo, :]
        if i == 3:
            @pl.loop(0, 4)
            def _(m):
                at = pl.ds(al(m, blk), blk)
                dproj_v[at, cols(1)] = unrope(dk_s[at, :], at)
                dproj_v[at, cols(2)] = dv_s[at, :].astype(BF16)

    def inputs(u):
        us = lax.rem(u, 2)
        cs = lax.rem(u, 5)
        wait(load_t(u, us))

        @pl.when(u < 7)
        def _():
            start(load_t(u + 1, 1 - us))

        at = pl.ds(al(u, 256), 256)
        gain_a, gain_m = ln_ref[0:1, at], ln_ref[2:3, at]
        sums = []
        for m in range(2):
            rows = slice(512 * m, 512 * m + 512)
            dha = dot_nt(dproj_v[rows, :], wq_t[us]).astype(BF16).astype(F32)
            dhm = dot_nt(dh_v[rows, :], wu_t[us]).astype(BF16).astype(F32)
            x_hat = (x_t[us, rows, :].astype(F32) - mean_ref[rows, :]) * rstd_ref[rows, :]
            c = (dha * gain_a + dhm * gain_m).astype(BF16)
            c_buf[cs, 2 * m] = c[:256]
            c_buf[cs, 2 * m + 1] = c[256:]
            sums.append([jnp.sum(v, axis=0, keepdims=True) for v in (dha * x_hat, dha, dhm * x_hat, dhm)])
        for i in range(4):
            lnb[0, core, i:i + 1, at] = sums[0][i] + sums[1][i]
        nxt, opp, prv = ring(tp, 1), ring(tp, 2), ring(tp, 3)
        remote(c_blk(u, opp, 0), cl1.at[u, 0], cs_l1.at[u], cr_l1.at[u], dev_x(nxt)).start()
        remote(c_blk(u, opp, 1), cl1.at[u, 1], cs_l1.at[u], cr_l1.at[u], dev_x(prv)).start()
        remote(c_blk(u, nxt, 1), cf1.at[u, 0, 1], cs_f1.at[u], cr_f1.at[u], dev_x(nxt)).start()
        remote(c_blk(u, prv, 0), cf1.at[u, 0, 0], cs_f1.at[u], cr_f1.at[u], dev_x(prv)).start()

    def c_blk(u, i, half):
        return c_buf.at[lax.rem(u, 5), i, pl.ds(128 * half, 128), :]

    def c_second(u):
        drain(cl1.at[u], cr_l1.at[u])
        for half, to in ((0, ring(tp, 1)), (1, ring(tp, 3))):
            ref = c_blk(u, to, half)
            ref[...] = (ref[...].astype(F32) + cl1[u, half].astype(F32)).astype(BF16)
            remote(ref, cf1.at[u, 1, half], cs_f1.at[u], cr_f1.at[u], dev_x(to)).start()

    def c_final(u):
        drain(cf1.at[u], cr_f1.at[u])
        for half in range(2):
            c_loc[128 * half:128 * half + 128, pl.ds(al(u, 256), 256)] = c_blk(u, tp, half)[...].astype(F32) + (
                cf1[u, 0, half].astype(F32) + cf1[u, 1, half].astype(F32))
        drain(cl1.at[u], cs_l1.at[u])
        drain(cf1.at[u], cs_f1.at[u])

    def last():
        wait(load_last())

        @pl.loop(0, 8)
        def _(r):
            at = pl.ds(al(r, 32), 32)
            dy_at = pl.ds(pl.multiple_of(256 + r * 32, 32), 32)
            own = pl.ds(pl.multiple_of(tp * 256 + r * 32, 32), 32)
            mean, rstd = mean_ref[own, :], rstd_ref[own, :]
            c = c_loc[at, :]
            x_hat = (jnp.concatenate([a_buf[0, 0, at, :], a_buf[0, 1, at, :]], axis=1).astype(F32) - mean) * rstd
            dy_own = jnp.concatenate([a_buf[0, 0, dy_at, :], a_buf[0, 1, dy_at, :]], axis=1).astype(F32)
            dx = rstd * (c - jnp.mean(c, axis=-1, keepdims=True) - x_hat * jnp.mean(c * x_hat, axis=-1, keepdims=True))
            o_gx[at, :] = (dy_own + dx).astype(BF16)

    @pl.loop(0, STEPS)
    def _(p):
        @pl.when(p < PIECES)
        def _():
            compute(p)

        for lag, stage in ((7, stage_f2), (6, stage_l2), (5, stage_f1), (3, stage_l1), (1, stage_s)):
            @pl.when((p >= lag) & (p < PIECES + lag))
            def _():
                stage(p - lag)

        @pl.when((p >= 20) & (p < 28))
        def _():
            c_final(p - 20)

        @pl.when((p >= 18) & (p < 26))
        def _():
            c_second(p - 18)

        for i in range(4):
            @pl.when((p < 16) & (lax.rem(p, 4) == i))
            def _():
                attend(p // 4, i)

        @pl.when(p == 14)
        def _():
            start(load_t(0, 0))

        @pl.when((p >= 16) & (p < 24))
        def _():
            inputs(p - 16)

        @pl.when(p == 24)
        def _():
            ln_send(0)

        for stage, me in ((1, tp), (2, y), (3, z)):
            @pl.when(p == 24 + stage)
            def _():
                lnb[stage, me] = ln_sum(stage - 1)
                ln_send(stage)

        @pl.when(p == 28)
        def _():
            last()

        @pl.when(p == 29)
        def _():
            o_ln[...] = ln_sum(3)

    for p in (PIECES - 2, PIECES - 1):
        drain(p_buf.at[p % 2, :, :, :, 0], ds.at[p % SLOTS])


def back_call(get, hmt, hat, dy_full, d_hidden, qkv, d_ctx, w2, w_up, x_full, x_loc, dy_loc, ln_params, mean, rstd, cos_f, sin_f):
    hbm = pl.BlockSpec(memory_space=pl.ANY)
    vmem = pl.BlockSpec(memory_space=pltpu.VMEM)
    dma = pltpu.SemaphoreType.DMA
    shape = jax.ShapeDtypeStruct
    k = (SLOTS,)
    return pl.pallas_call(
        back_kernel,
        in_specs=[hbm] * 12 + [vmem] * 5,
        out_specs=[vmem] * 6,
        out_shape=[shape((256, 2048), BF16), shape((4, 2048), F32), shape((64, 1536), F32), shape((16, 2048), F32),
                   shape((64, 2048), F32), shape((64, 2048), F32)],
        scratch_shapes=[
            pltpu.VMEM((2, 2, 1024, 1024), BF16), pltpu.VMEM((2, 1024, 256), BF16),
            pltpu.VMEM((2, 2, 4, 4, 2, 64, 128), F32), pltpu.VMEM(k + (2, 4, 4, 64, 128), F32),
            pltpu.VMEM(k + (2, 2, 4, 32, 128), F32), pltpu.VMEM(k + (2, 2, 2, 4, 32, 128), F32),
            pltpu.VMEM(k + (2, 2, 32, 128), F32), pltpu.VMEM(k + (2, 2, 2, 32, 128), F32),
            pltpu.VMEM((4, 4, 4, 2048), F32),
            pltpu.VMEM((1024, 2048), BF16), pltpu.VMEM((1024, 1536), BF16), pltpu.VMEM((512, 1024), BF16),
            pltpu.VMEM((2, 1024, 384), BF16), pltpu.VMEM((2, 1024, 128), BF16),
            pltpu.VMEM((1024, 128), F32), pltpu.VMEM((1024, 128), F32),
            pltpu.VMEM((2, 256, 1536), BF16), pltpu.VMEM((2, 256, 2048), BF16), pltpu.VMEM((2, 1024, 256), BF16),
            pltpu.VMEM((5, 4, 256, 256), BF16), pltpu.VMEM((8, 2, 128, 256), BF16), pltpu.VMEM((8, 2, 2, 128, 256), BF16),
            pltpu.VMEM((256, 2048), F32),
            dma((2, 2)), dma((2,)), dma, dma((2, 2)), dma((2, 3)), dma((2, 2)),
            dma(k), dma(k), dma(k), dma(k), dma(k), dma(k), dma(k), dma(k), dma(k), dma(k),
            dma((4,)), dma((4,)), dma((8,)), dma((8,)), dma((8,)), dma((8,)),
            pltpu.SemaphoreType.REGULAR((5,)),
        ],
        compiler_params=pltpu.CompilerParams(collective_id=0, has_side_effects=True, vmem_limit_bytes=65400 * 1024),
        cost_estimate=pl.CostEstimate(flops=50_000_000_000, bytes_accessed=100_000_000, transcendentals=0),
        name='back',
    )(get, hmt, hat, dy_full, d_hidden, qkv, d_ctx, w2, w_up, x_full, x_loc, dy_loc, ln_params, mean, rstd, cos_f, sin_f)


def solution(mesh):
    def local_step(x_loc, dy_loc, ln_params, w_qkv, w_out, w_up, w_down):
        width, groups, slots, head_dim = w_qkv.shape
        cos_f, sin_f = (jnp.asarray(t) for t in rope_tables(4 * x_loc.shape[1], head_dim))
        w_rows = w_qkv.transpose(0, 2, 1, 3).reshape(width * slots * groups, head_dim)
        x_full, dy_full, hat, hmt, qkv, get, d_hidden, d_ctx, w2, mean, rstd = front_call(
            x_loc[0], dy_loc[0], ln_params, cos_f, sin_f, w_rows, w_up, w_down, w_out)
        grad_x, g_ln, g_qkv, g_out, g_up, g_down = back_call(
            get, hmt, hat, dy_full, d_hidden, qkv, d_ctx, w2, w_up, x_full, x_loc[0], dy_loc[0], ln_params, mean, rstd, cos_f, sin_f)
        return grad_x[None], g_ln, g_qkv.reshape(64, groups, slots, head_dim), g_out, g_up, g_down

    act_spec = P('dp', 'tp', None)
    in_specs = (act_spec, act_spec, P(None, None), P(None, 'tp', None, None), P('tp', None), P(None, 'tp'), P('tp', None))
    out_specs = (act_spec, P(None, None), P('dp', 'tp', None, None), P(('tp', 'dp'), None), P('dp', 'tp'), P(('tp', 'dp'), None))
    return jax.shard_map(local_step, mesh=mesh, in_specs=in_specs, out_specs=out_specs, check_vma=False)
```

```python
import functools

import jax
import jax.numpy as jnp
import numpy as np
from jax import lax
from jax.experimental import pallas as pl
from jax.experimental.pallas import tpu as pltpu
from jax.sharding import PartitionSpec as P

NORM_EPS = 1e-5
ROPE_BASE = 10000.0
MESH = pl.DeviceIdType.MESH
PIECES = 24
SLOTS = 8
STEPS = PIECES + 7
EARLY = 768
LATE = 5
F32 = jnp.float32
BF16 = jnp.bfloat16


def rope_tables(seq_len, head_dim):
    half_dim = head_dim // 2
    inv_freq = np.float32(ROPE_BASE) ** (np.float32(-2.0) * np.arange(half_dim, dtype=np.float32) / np.float32(head_dim))
    angles = np.arange(seq_len, dtype=np.float32)[:, None] * inv_freq[None, :].astype(np.float32)
    cos_t, sin_t = np.cos(angles), np.sin(angles)
    return np.concatenate([cos_t, cos_t], axis=1), np.concatenate([-sin_t, sin_t], axis=1)


def dot_nn(lhs, rhs):
    return lax.dot_general(lhs, rhs, (((1,), (0,)), ((), ())), preferred_element_type=F32)


def dot_nt(lhs, rhs):
    return lax.dot_general(lhs, rhs, (((1,), (1,)), ((), ())), preferred_element_type=F32)


def dot_tt(lhs, rhs):
    return lax.dot_general(lhs, rhs, (((0,), (0,)), ((), ())), preferred_element_type=F32)


def front_kernel(x_ref, dy_ref, ln_ref, cos_ref, sin_ref, wq_ref, wu_ref,
                 o_x, o_dy, o_ha, o_hm, o_qkv, o_gelu, o_slope, o_w, mean_ref, rstd_ref,
                 x_v, dy_v, w2, wu, wq_b, wq_f, slope, ha, hm, hat, hmt, get, qkv,
                 xs, xr, ds, dr, in_sem, wq_sem, out_sem, fin_sem):
    tp = lax.axis_index('tp')
    nxt, opp, prv = lax.rem(tp + 1, 4), lax.rem(tp + 2, 4), lax.rem(tp + 3, 4)
    d_model = x_ref.shape[1]
    rows = x_ref.shape[0]
    half = rows // 2
    part = wq_b.shape[1]
    barrier = pltpu.get_barrier_semaphore()
    for peer in (nxt, prv):
        pl.semaphore_signal(barrier, inc=1, device_id={'tp': peer}, device_id_type=MESH)

    def wq_copy(i):
        return pltpu.make_async_copy(wq_ref.at[pl.ds(i * part, part)], wq_b.at[i % 2], wq_sem.at[i % 2])

    dy_own = dy_ref.at[:, pl.ds(0, EARLY)]
    loads = [pltpu.make_async_copy(x_ref, x_v.at[tp], in_sem.at[0]), pltpu.make_async_copy(dy_own, dy_v.at[tp], in_sem.at[1]),
             pltpu.make_async_copy(wu_ref, wu, in_sem.at[2])]
    wq_copy(0).start()
    loads[0].start()
    wq_copy(1).start()
    loads[2].start()
    loads[1].start()
    pl.semaphore_wait(barrier, 2)

    A, B = pl.ds(0, half), pl.ds(half, half)

    def moves(src, buf, ssem, rsem):
        def one(i, ref, slot, piece, to):
            return pltpu.make_async_remote_copy(src_ref=ref, dst_ref=buf.at[slot, piece], send_sem=ssem.at[i], recv_sem=rsem.at[i],
                                                device_id={'tp': to}, device_id_type=MESH)
        return [one(0, src.at[A], tp, A, nxt), one(1, src.at[B], tp, B, prv), one(2, src.at[B], tp, B, nxt), one(3, src.at[A], tp, A, prv),
                one(4, buf.at[prv, A], prv, A, nxt), one(5, buf.at[nxt, B], nxt, B, prv)]

    xm = moves(x_ref, x_v, xs, xr)
    dm = moves(dy_own, dy_v, ds, dr)
    for i in range(4):
        xm[i].start()

    per = part // 12
    for i in range(wq_ref.shape[0] // part):
        wq_copy(i).wait()

        @pl.loop(0, part // 256)
        def _(r):
            at = pl.ds(pl.multiple_of(r * 256, 256), 256)
            wq_f[at, :] = wq_b[i % 2, at, :].astype(F32)

        if i + 2 < wq_ref.shape[0] // part:
            wq_copy(i + 2).start()
        for j in range(3):
            for g in range(4):
                w2[i * per:(i + 1) * per, g * 384 + j * 128:g * 384 + j * 128 + 128] = wq_f[pl.ds(j * 4 + g, per, stride=12), :].astype(BF16)
    w_out_copy = pltpu.make_async_copy(w2, o_w, fin_sem.at[8])
    w_out_copy.start()

    outs = {}

    def tokens(block, i):
        slot, side = block[i]
        return pl.ds(pl.multiple_of(slot * rows + side * half, half), half)

    def put(kind, n, buf, ref, block):
        for i in range(2):
            copy = pltpu.make_async_copy(buf.at[n % 2, pl.ds(i * half, half)], ref.at[tokens(block, i)], out_sem.at[kind, n % 2, i])
            copy.start()
            outs[kind, n % 2, i] = copy

    def put_t(kind, buf, ref, block):
        for i in range(2):
            copy = pltpu.make_async_copy(buf.at[:, pl.ds(i * half, half)], ref.at[:, tokens(block, i)], out_sem.at[kind, 0, i])
            copy.start()
            outs[kind, 0, i] = copy

    def free(kind, n):
        for i in range(2):
            if (kind, n % 2, i) in outs:
                outs.pop((kind, n % 2, i)).wait()

    def forward(block, n):
        s = n % 2
        for i in range(2):
            slot, side = block[i]

            @pl.loop(0, half // 32)
            def _(r):
                src = pl.ds(pl.multiple_of(side * half + r * 32, 32), 32)
                at = pl.ds(pl.multiple_of(i * half + r * 32, 32), 32)
                to = pl.ds(pl.multiple_of(slot * rows + side * half + r * 32, 32), 32)
                xf = x_v[slot, src, :].astype(F32)
                mean = jnp.mean(xf, axis=-1, keepdims=True)
                cen = xf - mean
                rstd = lax.rsqrt(jnp.mean(cen * cen, axis=-1, keepdims=True) + NORM_EPS)
                mean_ref[to, :] = mean
                rstd_ref[to, :] = rstd
                x_hat = cen * rstd
                ha[at, :] = (x_hat * ln_ref[0:1, :] + ln_ref[1:2, :]).astype(BF16)
                hm[at, :] = (x_hat * ln_ref[2:3, :] + ln_ref[3:4, :]).astype(BF16)

        for kind in (0, 1, 3):
            free(kind, 0)
        free(2, n)
        free(4, n)

        @pl.loop(0, d_model // 256)
        def _(c):
            cols = pl.ds(pl.multiple_of(c * 256, 256), 256)
            hat[cols, :] = ha[:, cols].T
            hmt[cols, :] = hm[:, cols].T

        put_t(0, hat, o_ha, block)
        put_t(1, hmt, o_hm, block)
        cos_t, sin_t = (jnp.concatenate([ref[tokens(block, 0), :], ref[tokens(block, 1), :]], axis=0) for ref in (cos_ref, sin_ref))

        @pl.loop(0, 4)
        def _(g):
            cols = pl.ds(pl.multiple_of(g * 384, 128), 384)
            t = dot_nn(ha[...], w2[:, cols]).astype(BF16)
            for j in range(2):
                v = t[:, j * 128:j * 128 + 128].astype(F32)
                qkv[s, :, pl.ds(pl.multiple_of(g * 384 + j * 128, 128), 128)] = (v * cos_t + pltpu.roll(v, 64, 1) * sin_t).astype(BF16)
            qkv[s, :, pl.ds(pl.multiple_of(g * 384 + 256, 128), 128)] = t[:, 256:384]

        put(2, n, qkv, o_qkv, block)

        @pl.loop(0, 4)
        def _(c):
            cols = pl.ds(pl.multiple_of(c * 512, 512), 512)
            u = dot_nn(hm[...], wu[:, cols]).astype(BF16).astype(F32)
            cdf = 0.5 * (1.0 + lax.erf(u * (0.5 ** 0.5)))
            get[cols, :] = (u * cdf).astype(BF16).T
            slope[s, :, cols] = cdf + u * (jnp.exp(-0.5 * u * u) * ((2.0 * jnp.pi) ** -0.5))

        put_t(3, get, o_gelu, block)
        put(4, n, slope, o_slope, block)

    fins = []

    def keep(buf, ref, slot, i):
        copy = pltpu.make_async_copy(buf.at[slot], ref.at[pl.ds(pl.multiple_of(slot * rows, rows), rows)], fin_sem.at[i])
        copy.start()
        fins.append(copy)

    loads[0].wait()
    loads[2].wait()
    keep(x_v, o_x, tp, 0)
    forward(((tp, 0), (tp, 1)), 0)
    xm[0].wait_recv()
    xm[4].start()
    xm[1].wait_recv()
    xm[5].start()
    for i in range(4):
        dm[i].start()
    forward(((prv, 0), (nxt, 1)), 1)
    xm[2].wait_recv()
    xm[3].wait_recv()
    keep(x_v, o_x, prv, 1)
    keep(x_v, o_x, nxt, 2)
    forward(((prv, 1), (nxt, 0)), 2)
    dm[0].wait_recv()
    dm[4].start()
    dm[1].wait_recv()
    dm[5].start()
    xm[4].wait_recv()
    xm[5].wait_recv()
    keep(x_v, o_x, opp, 3)
    forward(((opp, 0), (opp, 1)), 3)
    loads[1].wait()
    for i in range(2, 6):
        dm[i].wait_recv()
    for i, slot in enumerate((tp, prv, nxt, opp)):
        keep(dy_v, o_dy, slot, 4 + i)
    for m in xm + dm:
        m.wait_send()
    for copy in list(outs.values()) + fins + [w_out_copy]:
        copy.wait()


def front_call(x_loc, dy_loc, ln_params, cos_f, sin_f, w_rows, w_up):
    r, d = x_loc.shape
    t, f, n = 4 * r, w_up.shape[1], w_rows.shape[0] * 128 // d
    part = w_rows.shape[0] // 4
    hbm = pl.BlockSpec(memory_space=pl.ANY)
    vmem = pl.BlockSpec(memory_space=pltpu.VMEM)
    dma = pltpu.SemaphoreType.DMA
    shape = jax.ShapeDtypeStruct
    return pl.pallas_call(
        front_kernel,
        in_specs=[hbm, hbm, vmem, vmem, vmem, hbm, hbm],
        out_specs=[hbm] * 8 + [vmem] * 2,
        out_shape=[shape((t, d), BF16), shape((t, EARLY), BF16), shape((d, t), BF16), shape((d, t), BF16),
                   shape((t, n), BF16), shape((f, t), BF16), shape((t, f), F32), shape((d, n), BF16),
                   shape((t, 1), F32), shape((t, 1), F32)],
        scratch_shapes=[
            pltpu.VMEM((4, r, d), BF16), pltpu.VMEM((4, r, EARLY), BF16),
            pltpu.VMEM((d, n), BF16), pltpu.VMEM((d, f), BF16),
            pltpu.VMEM((2, part, 128), BF16), pltpu.VMEM((part, 128), F32),
            pltpu.VMEM((2, r, f), F32),
            pltpu.VMEM((r, d), BF16), pltpu.VMEM((r, d), BF16),
            pltpu.VMEM((d, r), BF16), pltpu.VMEM((d, r), BF16), pltpu.VMEM((f, r), BF16),
            pltpu.VMEM((2, r, n), BF16),
            dma((6,)), dma((6,)), dma((6,)), dma((6,)), dma((3,)), dma((2,)), dma((5, 2, 2)), dma((9,)),
        ],
        compiler_params=pltpu.CompilerParams(collective_id=1, has_side_effects=True, vmem_limit_bytes=64000 * 1024),
        cost_estimate=pl.CostEstimate(flops=2 * t * d * (n + f), bytes_accessed=70_000_000, transcendentals=2 * t * f),
        name='front',
    )(x_loc, dy_loc, ln_params, cos_f, sin_f, w_rows, w_up)


def back_kernel(get_ref, hmt_ref, hat_ref, dyp_ref, slope_ref, qkv_ref, wo_ref, wd_ref, w2_ref, wup_ref, x_ref, xloc_ref, dyloc_ref,
                ln_ref, mean_ref, rstd_ref, cos_ref, sin_ref,
                o_gx, o_ln, o_qkv, o_out, o_up, o_down,
                a_buf, b_buf, p_buf, d_buf, l1, f1, l2, f2, lnb, dh_v, dproj_v, ctxt, qkv_b, dctx_b, dk_s, dv_s,
                wq_t, wu_t, x_t, c_buf, cl1, cf1, sl_buf, dy_v, wo_t,
                a_sem, dy_sem, h_sem, t_sem, d_sem, g_sem, gs, gr, ds, dr, s_l1, r_l1, s_f1, r_f1, s_l2, r_l2, s_f2, r_f2, ln_s, ln_r,
                cs_l1, cr_l1, cs_f1, cr_f1, credit):
    tp = lax.axis_index('tp')
    dp = lax.axis_index('dp')
    core = lax.rem(dp, 2)
    y = lax.rem(dp // 2, 4)
    z = dp // 8
    partner = {'dp': dp + 1 - 2 * core}
    n_head = 4
    hd = 128
    blk = 256
    scale = hd ** -0.5

    def dev_y(i):
        return {'dp': z * 8 + i * 2 + core}

    def dev_z(i):
        return {'dp': i * 8 + y * 2 + core}

    def dev_x(i):
        return {'tp': i}

    def ring(i, d):
        return lax.rem(i + d, 4)

    def al(i, m):
        return pl.multiple_of(i * m, m)

    barrier = pltpu.get_barrier_semaphore()
    peers = [partner]
    for d in (1, 2, 3):
        peers += [dev_x(ring(tp, d)), dev_y(ring(y, d)), dev_z(ring(z, d))]
    for peer in peers:
        pl.semaphore_signal(barrier, inc=1, device_id=peer, device_id_type=MESH)

    def load_a(src, h):
        return pltpu.make_async_copy(src.at[pl.ds(al(h, 1024), 1024)], a_buf.at[h], a_sem.at[h])

    def load_x():
        return [pltpu.make_async_copy(xloc_ref.at[:, pl.ds(256 * u, 256)], x_t.at[u // 4, pl.ds(256 * (u % 4), 256)], g_sem) for u in range(8)]

    def load_head(h, slot):
        return [pltpu.make_async_copy(qkv_ref.at[:, pl.ds(pl.multiple_of(h * 384, 128), 384)], qkv_b.at[slot], h_sem.at[slot, 0]),
                pltpu.make_async_copy(wo_ref.at[pl.ds(al(h, 128), 128)], wo_t.at[slot], h_sem.at[slot, 1])]

    def load_d(k, slot):
        at = pl.ds(al(k, 256), 256)
        return [pltpu.make_async_copy(wd_ref.at[at], wu_t.at[slot], d_sem.at[slot, 0]),
                pltpu.make_async_copy(slope_ref.at[:, at], sl_buf.at[slot], d_sem.at[slot, 1])]

    def load_t(u, slot):
        at = pl.ds(al(u, 256), 256)
        return [pltpu.make_async_copy(w2_ref.at[at], wq_t.at[slot], t_sem.at[slot, 0]),
                pltpu.make_async_copy(wup_ref.at[at], wu_t.at[slot], t_sem.at[slot, 1]),
                pltpu.make_async_copy(x_ref.at[:, at], x_t.at[slot], t_sem.at[slot, 2])]

    def start(copies):
        for copy in copies:
            copy.start()

    def wait(copies):
        for copy in copies:
            copy.wait()

    for h in range(2):
        load_a(get_ref, jnp.int32(h)).start()
    early = pltpu.make_async_copy(dyp_ref, dy_v.at[:, pl.ds(0, EARLY)], dy_sem.at[0])
    early.start()
    late = pltpu.make_async_copy(dyloc_ref.at[:, pl.ds(EARLY, 256 * LATE)],
                                 dy_v.at[pl.ds(al(tp, 256), 256), pl.ds(EARLY, 256 * LATE)], dy_sem.at[1])
    late.start()
    start(load_head(jnp.int32(0), 0))
    start(load_d(jnp.int32(0), 0))
    pl.semaphore_wait(barrier, len(peers))

    def remote(src, dst, ssem, rsem, device):
        return pltpu.make_async_remote_copy(src_ref=src, dst_ref=dst, send_sem=ssem, recv_sem=rsem, device_id=device, device_id_type=MESH)

    def drain(ref, sem):
        pltpu.make_async_copy(ref, ref, sem).wait()

    def slice_copy(j, i):
        cols = pl.ds(pl.multiple_of(EARLY + j * 256, 256), 256)
        nxt, prv = ring(tp, 1), ring(tp, 3)
        owner, half, to = ((tp, 0, nxt), (tp, 1, prv), (tp, 1, nxt), (tp, 0, prv), (prv, 0, nxt), (nxt, 1, prv))[i]
        spot = dy_v.at[pl.ds(pl.multiple_of(owner * 256 + half * 128, 128), 128), cols]
        src = dyloc_ref.at[pl.ds(128 * half, 128), cols] if i < 4 else spot
        return remote(src, spot, gs.at[j, i], gr.at[j, i], dev_x(to))

    def slice_own(j):
        for i in range(4):
            slice_copy(j, i).start()

    def slice_on(j):
        for i in range(2):
            slice_copy(j, i).wait_recv()
            slice_copy(j, 4 + i).start()

    def slice_done(j):
        for i in range(2, 6):
            slice_copy(j, i).wait_recv()

    slice_own(jnp.int32(0))
    slice_own(jnp.int32(1))

    def pair_copy(p):
        slot = lax.rem(p, SLOTS)
        return remote(p_buf.at[lax.rem(p, 2), :, :, :, 1 - core], d_buf.at[slot], ds.at[slot], dr.at[slot], partner)

    def blk1(slot, col, i, half):
        rows = pl.ds(32 * half, 32)
        if col == 0:
            return d_buf.at[slot, 0, :, i, rows, :]
        return d_buf.at[slot, 1, i, :, rows, :]

    def blk2(slot, col, i, half):
        rows = pl.ds(32 * half, 32)
        if col == 0:
            return d_buf.at[slot, 0, i, y, rows, :]
        return d_buf.at[slot, 1, z, i, rows, :]

    me1 = (y, z)
    dev1 = (dev_y, dev_z)
    me2 = (z, y)
    dev2 = (dev_z, dev_y)

    def compute(p):
        ps = lax.rem(p, 2)

        @pl.when(p >= 2)
        def _():
            drain(p_buf.at[ps, :, :, :, 0], ds.at[lax.rem(p - 2, SLOTS)])

        @pl.when(p == 0)
        def _():
            early.wait()

        @pl.when(p == 3)
        def _():
            late.wait()

        @pl.when((p >= 3) & (p < 7))
        def _():
            slice_done(p - 3)

        @pl.when(p == 6)
        def _():
            slice_done(p - 2)

        @pl.when(p < 8)
        def _():
            b_buf[ps] = dy_v[:, pl.ds(al(p, 256), 256)]

        @pl.when((p >= 8) & (p < 16))
        def _():
            b_buf[ps] = dh_v[:, pl.ds(al(p - 8, 256), 256)]

        @pl.when((p >= 16) & (p < 22))
        def _():
            b_buf[ps] = dproj_v[:, pl.ds(al(p - 16, 256), 256)]

        @pl.when(p < 22)
        def _():
            @pl.loop(0, 2)
            def _(h):
                @pl.when((p == 0) | (p == 8) | (p == 16))
                def _():
                    load_a(get_ref, h).wait()

                tile = dot_nn(a_buf[h], b_buf[ps])
                for i in range(16):
                    for col in range(2):
                        p_buf[ps, col, 2 * h + i // 8, (i // 2) % 4, i % 2] = tile[64 * i:64 * i + 64, 128 * col:128 * col + 128]

                @pl.when(p == 7)
                def _():
                    load_a(hmt_ref, h).start()

                @pl.when(p == 15)
                def _():
                    load_a(hat_ref, h).start()

        @pl.when(p >= 22)
        def _():
            @pl.loop(0, 4)
            def _(k):
                tile = dot_nn(ctxt[...], dy_v[:, pl.ds(pl.multiple_of((p - 22) * 1024 + k * 256, 256), 256)])
                for i in range(32):
                    for col in range(2):
                        p_buf[ps, col, i // 8, (i // 2) % 4, i % 2, pl.ds(al(k, 16), 16), :] = tile[16 * i:16 * i + 16, 128 * col:128 * col + 128]

        @pl.when(p >= SLOTS)
        def _():
            pl.semaphore_wait(credit.at[0], 1)

        pair_copy(p).start()

    def first(blk, slot, me, dev, lands, finals, s_a, r_a, s_b, r_b):
        for col in range(2):
            nxt, opp, prv = ring(me[col], 1), ring(me[col], 2), ring(me[col], 3)
            remote(blk(slot, col, opp, 0), lands.at[slot, col, 0], s_a.at[slot], r_a.at[slot], dev[col](nxt)).start()
            remote(blk(slot, col, opp, 1), lands.at[slot, col, 1], s_a.at[slot], r_a.at[slot], dev[col](prv)).start()
        for col in range(2):
            nxt, prv = ring(me[col], 1), ring(me[col], 3)
            remote(blk(slot, col, nxt, 1), finals.at[slot, col, 0, 1], s_b.at[slot], r_b.at[slot], dev[col](nxt)).start()
            remote(blk(slot, col, prv, 0), finals.at[slot, col, 0, 0], s_b.at[slot], r_b.at[slot], dev[col](prv)).start()

    def second(blk, slot, me, dev, lands, finals, r_a, s_b, r_b):
        drain(lands.at[slot], r_a.at[slot])
        for col in range(2):
            nxt, prv = ring(me[col], 1), ring(me[col], 3)
            for half, to in ((0, nxt), (1, prv)):
                ref = blk(slot, col, to, half)
                ref[...] = ref[...] + lands[slot, col, half]
                remote(ref, finals.at[slot, col, 1, half], s_b.at[slot], r_b.at[slot], dev[col](to)).start()

    def stage_s(q):
        slot = lax.rem(q, SLOTS)
        ps = lax.rem(q, 2)
        drain(d_buf.at[slot], dr.at[slot])

        @pl.loop(0, 32)
        def _(i):
            col, zi, yi = i // 16, lax.rem(i // 4, 4), lax.rem(i, 4)
            d_buf[slot, col, zi, yi] = d_buf[slot, col, zi, yi] + p_buf[ps, col, zi, yi, core]

        @pl.when(q >= SLOTS)
        def _():
            for i in range(1, 5):
                pl.semaphore_wait(credit.at[i], 1)

        first(blk1, slot, me1, dev1, l1, f1, s_l1, r_l1, s_f1, r_f1)

    def stage_l1(q):
        second(blk1, lax.rem(q, SLOTS), me1, dev1, l1, f1, r_l1, s_f1, r_f1)

    def stage_f1(q):
        slot = lax.rem(q, SLOTS)
        drain(f1.at[slot], r_f1.at[slot])
        for col in range(2):
            for half in range(2):
                ref = blk1(slot, col, me1[col], half)
                ref[...] = ref[...] + (f1[slot, col, 0, half] + f1[slot, col, 1, half])
        first(blk2, slot, me2, dev2, l2, f2, s_l2, r_l2, s_f2, r_f2)

    def stage_l2(q):
        second(blk2, lax.rem(q, SLOTS), me2, dev2, l2, f2, r_l2, s_f2, r_f2)

    def stage_f2(q):
        slot = lax.rem(q, SLOTS)
        drain(f2.at[slot], r_f2.at[slot])
        for col in range(2):
            for half in range(2):
                rows = pl.ds(32 * half, 32)
                val = blk2(slot, col, me2[col], half)[...] + (f2[slot, col, 0, half] + f2[slot, col, 1, half])
                for out, lo, hi in ((o_down, 0, 8), (o_up, 8, 16), (o_qkv, 16, 22)):
                    @pl.when((q >= lo) & (q < hi))
                    def _():
                        out[rows, pl.ds(pl.multiple_of((q - lo) * 256 + col * 128, 128), 128)] = val

                @pl.when(q >= 22)
                def _():
                    for k in range(2):
                        at = (q - 22) * 1024 + (2 * half + k) * 256 + col * 128
                        o_out[:, pl.ds(pl.multiple_of(at, 128), 128)] = val[16 * k:16 * k + 16, :]
        drain(l1.at[slot], s_l1.at[slot])
        drain(f1.at[slot], s_f1.at[slot])
        drain(l2.at[slot], s_l2.at[slot])
        drain(f2.at[slot], s_f2.at[slot])

        @pl.when(q < PIECES - SLOTS)
        def _():
            to = (partner, dev_y(ring(y, 1)), dev_y(ring(y, 3)), dev_z(ring(z, 1)), dev_z(ring(z, 3)))
            for i in range(5):
                pl.semaphore_signal(credit.at[i], inc=1, device_id=to[i], device_id_type=MESH)

    def ln_send(stage):
        me, dev, n = ((core, None, 2), (tp, dev_x, 4), (y, dev_y, 4), (z, dev_z, 4))[stage]
        for d in range(1, n):
            to = partner if dev is None else dev(ring(me, d))
            remote(lnb.at[stage, me], lnb.at[stage, me], ln_s.at[stage], ln_r.at[stage], to).start()

    def ln_sum(stage):
        n = 2 if stage == 0 else 4
        ref = lnb.at[stage, pl.ds(0, n - 1)]
        drain(ref, ln_r.at[stage])
        drain(ref, ln_s.at[stage])
        if n == 2:
            return lnb[0, 0] + lnb[0, 1]
        return (lnb[stage, 0] + lnb[stage, 1]) + (lnb[stage, 2] + lnb[stage, 3])

    def unrope(d, rows):
        d = d.astype(BF16).astype(F32)
        return (d * cos_ref[rows, :] - pltpu.roll(d, hd // 2, 1) * sin_ref[rows, :]).astype(BF16)

    def attend(h, side):
        hs = lax.rem(h, 2)

        def cols(j):
            return pl.ds(pl.multiple_of(h * 384 + j * 128, 128), 128)

        if side == 0:
            wait(load_head(h, hs))

            @pl.when(h < n_head - 1)
            def _():
                start(load_head(h + 1, 1 - hs))

            dctx_b[...] = dot_nt(dy_v[...], wo_t[hs]).astype(BF16)
            dk_s[...] = jnp.zeros_like(dk_s)
            dv_s[...] = jnp.zeros_like(dv_s)

        for i in ((0, 3), (1, 2))[side]:
            rows, lo, n = slice(i * blk, (i + 1) * blk), i * blk, (i + 1) * blk
            qi, dci = qkv_b[hs, rows, 0:hd], dctx_b[rows, :]
            kn, vn = qkv_b[hs, :n, hd:2 * hd], qkv_b[hs, :n, 2 * hd:3 * hd]
            s = dot_nt(qi, kn)
            seen = lax.broadcasted_iota(jnp.int32, (blk, blk), 0) >= lax.broadcasted_iota(jnp.int32, (blk, blk), 1)
            diag = jnp.where(seen, s[:, lo:], -1e30)
            s = jnp.concatenate([s[:, :lo], diag], axis=1) if lo else diag
            e = jnp.exp((s - jnp.max(s, axis=1, keepdims=True)) * scale)
            p = e * (1.0 / jnp.sum(e, axis=1, keepdims=True))
            pb = p.astype(BF16)
            ctxt[pl.ds(al(h, hd), hd), rows] = dot_nn(pb, vn).astype(BF16).T
            dp_ = dot_nt(dci, vn).astype(BF16).astype(F32)
            dsb = (p * (dp_ - jnp.sum(p * dp_, axis=1, keepdims=True)) * scale).astype(BF16)
            dproj_v[rows, cols(0)] = unrope(dot_nn(dsb, kn), rows)
            dk_s[:n, :] = dk_s[:n, :] + dot_tt(dsb, qi)
            dv_s[:n, :] = dv_s[:n, :] + dot_tt(pb, dci)
        if side == 1:
            @pl.loop(0, 4)
            def _(m):
                at = pl.ds(al(m, blk), blk)
                dproj_v[at, cols(1)] = unrope(dk_s[at, :], at)
                dproj_v[at, cols(2)] = dv_s[at, :].astype(BF16)

    def down(k):
        ks = lax.rem(k, 2)
        wait(load_d(k, ks))

        @pl.when(k < 7)
        def _():
            start(load_d(k + 1, 1 - ks))

        d_gelu = dot_nt(dy_v[...], wu_t[ks]).astype(BF16).astype(F32)
        dh_v[:, pl.ds(al(k, 256), 256)] = (d_gelu * sl_buf[ks]).astype(BF16)

    def inputs(u):
        us = lax.rem(u, 2)
        cs = lax.rem(u, 5)
        wait(load_t(u, us))

        @pl.when(u < 7)
        def _():
            start(load_t(u + 1, 1 - us))

        at = pl.ds(al(u, 256), 256)
        gain_a, gain_m = ln_ref[0:1, at], ln_ref[2:3, at]
        sums = []
        for m in range(2):
            rows = slice(512 * m, 512 * m + 512)
            dha = dot_nt(dproj_v[rows, :], wq_t[us]).astype(BF16).astype(F32)
            dhm = dot_nt(dh_v[rows, :], wu_t[us]).astype(BF16).astype(F32)
            x_hat = (x_t[us, rows, :].astype(F32) - mean_ref[rows, :]) * rstd_ref[rows, :]
            c = (dha * gain_a + dhm * gain_m).astype(BF16)
            c_buf[cs, 2 * m] = c[:256]
            c_buf[cs, 2 * m + 1] = c[256:]
            sums.append([jnp.sum(v, axis=0, keepdims=True) for v in (dha * x_hat, dha, dhm * x_hat, dhm)])
        for i in range(4):
            lnb[0, core, i:i + 1, at] = sums[0][i] + sums[1][i]
        nxt, opp, prv = ring(tp, 1), ring(tp, 2), ring(tp, 3)
        remote(c_blk(u, opp, 0), cl1.at[u, 0], cs_l1.at[u], cr_l1.at[u], dev_x(nxt)).start()
        remote(c_blk(u, opp, 1), cl1.at[u, 1], cs_l1.at[u], cr_l1.at[u], dev_x(prv)).start()
        remote(c_blk(u, nxt, 1), cf1.at[u, 0, 1], cs_f1.at[u], cr_f1.at[u], dev_x(nxt)).start()
        remote(c_blk(u, prv, 0), cf1.at[u, 0, 0], cs_f1.at[u], cr_f1.at[u], dev_x(prv)).start()

    def c_blk(u, i, half):
        return c_buf.at[lax.rem(u, 5), i, pl.ds(128 * half, 128), :]

    def c_second(u):
        drain(cl1.at[u], cr_l1.at[u])
        for half, to in ((0, ring(tp, 1)), (1, ring(tp, 3))):
            ref = c_blk(u, to, half)
            ref[...] = (ref[...].astype(F32) + cl1[u, half].astype(F32)).astype(BF16)
            remote(ref, cf1.at[u, 1, half], cs_f1.at[u], cr_f1.at[u], dev_x(to)).start()

    def c_final(u):
        drain(cf1.at[u], cr_f1.at[u])
        for half in range(2):
            sl_buf[u // 4, pl.ds(pl.multiple_of(lax.rem(u, 4) * 256 + 128 * half, 128), 128), :] = c_blk(u, tp, half)[...].astype(F32) + (
                cf1[u, 0, half].astype(F32) + cf1[u, 1, half].astype(F32))
        drain(cl1.at[u], cs_l1.at[u])
        drain(cf1.at[u], cs_f1.at[u])

    def last():
        drain(x_t, g_sem)

        @pl.loop(0, 8)
        def _(r):
            def across(ref):
                return jnp.concatenate([ref[u // 4, pl.ds(pl.multiple_of(256 * (u % 4) + r * 32, 32), 32), :] for u in range(8)], axis=1).astype(F32)

            own = pl.ds(pl.multiple_of(tp * 256 + r * 32, 32), 32)
            rstd = rstd_ref[own, :]
            c = across(sl_buf)
            x_hat = (across(x_t) - mean_ref[own, :]) * rstd
            dx = rstd * (c - jnp.mean(c, axis=-1, keepdims=True) - x_hat * jnp.mean(c * x_hat, axis=-1, keepdims=True))
            o_gx[pl.ds(al(r, 32), 32), :] = (dy_v[own, :].astype(F32) + dx).astype(BF16)

    @pl.loop(0, STEPS)
    def _(p):
        @pl.when(p < PIECES)
        def _():
            compute(p)

        for lag, stage in ((7, stage_f2), (6, stage_l2), (5, stage_f1), (3, stage_l1), (1, stage_s)):
            @pl.when((p >= lag) & (p < PIECES + lag))
            def _():
                stage(p - lag)

        @pl.when((p >= 20) & (p < 28))
        def _():
            c_final(p - 20)

        @pl.when((p >= 18) & (p < 26))
        def _():
            c_second(p - 18)

        @pl.when(p < LATE)
        def _():
            slice_on(p)

        @pl.when(p < LATE - 2)
        def _():
            slice_own(p + 2)

        @pl.when((p >= 6) & (p < 14))
        def _():
            down(p - 6)

        for side in range(2):
            @pl.when((p >= 8) & (p < 16) & (lax.rem(p, 2) == side))
            def _():
                attend((p - 8) // 2, side)

        @pl.when(p == 10)
        def _():
            for j in range(LATE):
                for i in range(6):
                    slice_copy(j, i).wait_send()

        @pl.when(p == 14)
        def _():
            start(load_t(0, 0))

        @pl.when((p >= 16) & (p < 24))
        def _():
            inputs(p - 16)

        @pl.when(p == 24)
        def _():
            start(load_x())
            ln_send(0)

        for stage, me in ((1, tp), (2, y), (3, z)):
            @pl.when(p == 24 + stage)
            def _():
                lnb[stage, me] = ln_sum(stage - 1)
                ln_send(stage)

        @pl.when(p == 28)
        def _():
            last()

        @pl.when(p == 29)
        def _():
            o_ln[...] = ln_sum(3)

    for p in (PIECES - 2, PIECES - 1):
        drain(p_buf.at[p % 2, :, :, :, 0], ds.at[p % SLOTS])


def back_call(get, hmt, hat, dy_early, slope, qkv, w_out, w_down, w2, w_up, x_full, x_loc, dy_loc, ln_params, mean, rstd, cos_f, sin_f):
    hbm = pl.BlockSpec(memory_space=pl.ANY)
    vmem = pl.BlockSpec(memory_space=pltpu.VMEM)
    dma = pltpu.SemaphoreType.DMA
    shape = jax.ShapeDtypeStruct
    k = (SLOTS,)
    return pl.pallas_call(
        back_kernel,
        in_specs=[hbm] * 13 + [vmem] * 5,
        out_specs=[vmem] * 6,
        out_shape=[shape((256, 2048), BF16), shape((4, 2048), F32), shape((64, 1536), F32), shape((16, 2048), F32),
                   shape((64, 2048), F32), shape((64, 2048), F32)],
        scratch_shapes=[
            pltpu.VMEM((2, 1024, 1024), BF16), pltpu.VMEM((2, 1024, 256), BF16),
            pltpu.VMEM((2, 2, 4, 4, 2, 64, 128), F32), pltpu.VMEM(k + (2, 4, 4, 64, 128), F32),
            pltpu.VMEM(k + (2, 2, 4, 32, 128), F32), pltpu.VMEM(k + (2, 2, 2, 4, 32, 128), F32),
            pltpu.VMEM(k + (2, 2, 32, 128), F32), pltpu.VMEM(k + (2, 2, 2, 32, 128), F32),
            pltpu.VMEM((4, 4, 4, 2048), F32),
            pltpu.VMEM((1024, 2048), BF16), pltpu.VMEM((1024, 1536), BF16), pltpu.VMEM((512, 1024), BF16),
            pltpu.VMEM((2, 1024, 384), BF16), pltpu.VMEM((1024, 128), BF16),
            pltpu.VMEM((1024, 128), F32), pltpu.VMEM((1024, 128), F32),
            pltpu.VMEM((2, 256, 1536), BF16), pltpu.VMEM((2, 256, 2048), BF16), pltpu.VMEM((2, 1024, 256), BF16),
            pltpu.VMEM((5, 4, 256, 256), BF16), pltpu.VMEM((8, 2, 128, 256), BF16), pltpu.VMEM((8, 2, 2, 128, 256), BF16),
            pltpu.VMEM((2, 1024, 256), F32), pltpu.VMEM((1024, 2048), BF16), pltpu.VMEM((2, 128, 2048), BF16),
            dma((2,)), dma((2,)), dma((2, 2)), dma((2, 3)), dma((2, 2)), dma, dma((LATE, 6)), dma((LATE, 6)),
            dma(k), dma(k), dma(k), dma(k), dma(k), dma(k), dma(k), dma(k), dma(k), dma(k),
            dma((4,)), dma((4,)), dma((8,)), dma((8,)), dma((8,)), dma((8,)),
            pltpu.SemaphoreType.REGULAR((5,)),
        ],
        compiler_params=pltpu.CompilerParams(collective_id=0, has_side_effects=True, vmem_limit_bytes=65400 * 1024),
        cost_estimate=pl.CostEstimate(flops=50_000_000_000, bytes_accessed=100_000_000, transcendentals=0),
        name='back',
    )(get, hmt, hat, dy_early, slope, qkv, w_out, w_down, w2, w_up, x_full, x_loc, dy_loc, ln_params, mean, rstd, cos_f, sin_f)


def solution(mesh):
    def local_step(x_loc, dy_loc, ln_params, w_qkv, w_out, w_up, w_down):
        width, groups, slots, head_dim = w_qkv.shape
        cos_f, sin_f = (jnp.asarray(t) for t in rope_tables(4 * x_loc.shape[1], head_dim))
        w_rows = w_qkv.transpose(0, 2, 1, 3).reshape(width * slots * groups, head_dim)
        x_full, dy_early, hat, hmt, qkv, get, slope, w2, mean, rstd = front_call(x_loc[0], dy_loc[0], ln_params, cos_f, sin_f, w_rows, w_up)
        grad_x, g_ln, g_qkv, g_out, g_up, g_down = back_call(
            get, hmt, hat, dy_early, slope, qkv, w_out, w_down, w2, w_up, x_full, x_loc[0], dy_loc[0], ln_params, mean, rstd, cos_f, sin_f)
        return grad_x[None], g_ln, g_qkv.reshape(64, groups, slots, head_dim), g_out, g_up, g_down

    act_spec = P('dp', 'tp', None)
    in_specs = (act_spec, act_spec, P(None, None), P(None, 'tp', None, None), P('tp', None), P(None, 'tp'), P('tp', None))
    out_specs = (act_spec, P(None, None), P('dp', 'tp', None, None), P(('tp', 'dp'), None), P('dp', 'tp'), P(('tp', 'dp'), None))
    return jax.shard_map(local_step, mesh=mesh, in_specs=in_specs, out_specs=out_specs, check_vma=False)
```

```python
import functools

import jax
import jax.numpy as jnp
import numpy as np
from jax import lax
from jax.experimental import pallas as pl
from jax.experimental.pallas import tpu as pltpu
from jax.sharding import PartitionSpec as P

NORM_EPS = 1e-5
ROPE_BASE = 10000.0
MESH = pl.DeviceIdType.MESH
PIECES = 24
SLOTS = 10
STEPS = PIECES + 9
EARLY = 768
LATE = 5
VMEM_LIMIT = 60000 * 1024
F32 = jnp.float32
BF16 = jnp.bfloat16


def rope_tables(seq_len, head_dim):
    half_dim = head_dim // 2
    inv_freq = np.float32(ROPE_BASE) ** (np.float32(-2.0) * np.arange(half_dim, dtype=np.float32) / np.float32(head_dim))
    angles = np.arange(seq_len, dtype=np.float32)[:, None] * inv_freq[None, :].astype(np.float32)
    cos_t, sin_t = np.cos(angles), np.sin(angles)
    return np.concatenate([cos_t, cos_t], axis=1), np.concatenate([-sin_t, sin_t], axis=1)


def dot_nn(lhs, rhs):
    return lax.dot_general(lhs, rhs, (((1,), (0,)), ((), ())), preferred_element_type=F32)


def dot_nt(lhs, rhs):
    return lax.dot_general(lhs, rhs, (((1,), (1,)), ((), ())), preferred_element_type=F32)


def dot_tt(lhs, rhs):
    return lax.dot_general(lhs, rhs, (((0,), (0,)), ((), ())), preferred_element_type=F32)


def front_kernel(x_ref, dy_ref, ln_ref, cos_ref, sin_ref, wq_ref, wu_ref,
                 o_x, o_dy, o_ha, o_hm, o_qkv, o_gelu, o_slope, o_w, mean_ref, rstd_ref,
                 x_v, dy_v, w2, wu, wq_b, wq_f, slope, ha, hm, hat, hmt, get, qkv,
                 xs, xr, ds, dr, in_sem, wq_sem, out_sem, fin_sem):
    tp = lax.axis_index('tp')
    nxt, opp, prv = lax.rem(tp + 1, 4), lax.rem(tp + 2, 4), lax.rem(tp + 3, 4)
    d_model = x_ref.shape[1]
    rows = x_ref.shape[0]
    half = rows // 2
    part = wq_b.shape[1]
    barrier = pltpu.get_barrier_semaphore()
    for peer in (nxt, prv):
        pl.semaphore_signal(barrier, inc=1, device_id={'tp': peer}, device_id_type=MESH)

    def wq_copy(i):
        return pltpu.make_async_copy(wq_ref.at[pl.ds(i * part, part)], wq_b.at[i % 2], wq_sem.at[i % 2])

    dy_own = dy_ref.at[:, pl.ds(0, EARLY)]
    loads = [pltpu.make_async_copy(x_ref, x_v.at[tp], in_sem.at[0]), pltpu.make_async_copy(dy_own, dy_v.at[tp], in_sem.at[1]),
             pltpu.make_async_copy(wu_ref, wu, in_sem.at[2])]
    wq_copy(0).start()
    loads[0].start()
    wq_copy(1).start()
    loads[2].start()
    loads[1].start()
    pl.semaphore_wait(barrier, 2)

    A, B = pl.ds(0, half), pl.ds(half, half)

    def moves(src, buf, ssem, rsem):
        def one(i, ref, slot, piece, to):
            return pltpu.make_async_remote_copy(src_ref=ref, dst_ref=buf.at[slot, piece], send_sem=ssem.at[i], recv_sem=rsem.at[i],
                                                device_id={'tp': to}, device_id_type=MESH)
        return [one(0, src.at[A], tp, A, nxt), one(1, src.at[B], tp, B, prv), one(2, src.at[B], tp, B, nxt), one(3, src.at[A], tp, A, prv),
                one(4, buf.at[prv, A], prv, A, nxt), one(5, buf.at[nxt, B], nxt, B, prv)]

    xm = moves(x_ref, x_v, xs, xr)
    dm = moves(dy_own, dy_v, ds, dr)
    for i in range(4):
        xm[i].start()

    per = part // 12
    for i in range(wq_ref.shape[0] // part):
        wq_copy(i).wait()

        @pl.loop(0, part // 256)
        def _(r):
            at = pl.ds(pl.multiple_of(r * 256, 256), 256)
            wq_f[at, :] = wq_b[i % 2, at, :].astype(F32)

        if i + 2 < wq_ref.shape[0] // part:
            wq_copy(i + 2).start()
        for j in range(3):
            for g in range(4):
                w2[i * per:(i + 1) * per, g * 384 + j * 128:g * 384 + j * 128 + 128] = wq_f[pl.ds(j * 4 + g, per, stride=12), :].astype(BF16)
    w_out_copy = pltpu.make_async_copy(w2, o_w, fin_sem.at[8])
    w_out_copy.start()

    outs = {}

    def tokens(block, i):
        slot, side = block[i]
        return pl.ds(pl.multiple_of(slot * rows + side * half, half), half)

    def put(kind, n, buf, ref, block):
        for i in range(2):
            copy = pltpu.make_async_copy(buf.at[n % 2, pl.ds(i * half, half)], ref.at[tokens(block, i)], out_sem.at[kind, n % 2, i])
            copy.start()
            outs[kind, n % 2, i] = copy

    def put_t(kind, buf, ref, block):
        for i in range(2):
            copy = pltpu.make_async_copy(buf.at[:, pl.ds(i * half, half)], ref.at[:, tokens(block, i)], out_sem.at[kind, 0, i])
            copy.start()
            outs[kind, 0, i] = copy

    def free(kind, n):
        for i in range(2):
            if (kind, n % 2, i) in outs:
                outs.pop((kind, n % 2, i)).wait()

    def forward(block, n):
        s = n % 2
        for i in range(2):
            slot, side = block[i]

            @pl.loop(0, half // 32)
            def _(r):
                src = pl.ds(pl.multiple_of(side * half + r * 32, 32), 32)
                at = pl.ds(pl.multiple_of(i * half + r * 32, 32), 32)
                to = pl.ds(pl.multiple_of(slot * rows + side * half + r * 32, 32), 32)
                xf = x_v[slot, src, :].astype(F32)
                mean = jnp.mean(xf, axis=-1, keepdims=True)
                cen = xf - mean
                rstd = lax.rsqrt(jnp.mean(cen * cen, axis=-1, keepdims=True) + NORM_EPS)
                mean_ref[to, :] = mean
                rstd_ref[to, :] = rstd
                x_hat = cen * rstd
                ha[at, :] = (x_hat * ln_ref[0:1, :] + ln_ref[1:2, :]).astype(BF16)
                hm[at, :] = (x_hat * ln_ref[2:3, :] + ln_ref[3:4, :]).astype(BF16)

        for kind in (0, 1, 3):
            free(kind, 0)
        free(2, n)
        free(4, n)

        @pl.loop(0, d_model // 256)
        def _(c):
            cols = pl.ds(pl.multiple_of(c * 256, 256), 256)
            hat[cols, :] = ha[:, cols].T
            hmt[cols, :] = hm[:, cols].T

        put_t(0, hat, o_ha, block)
        put_t(1, hmt, o_hm, block)
        cos_t, sin_t = (jnp.concatenate([ref[tokens(block, 0), :], ref[tokens(block, 1), :]], axis=0) for ref in (cos_ref, sin_ref))

        @pl.loop(0, 4)
        def _(g):
            cols = pl.ds(pl.multiple_of(g * 384, 128), 384)
            t = dot_nn(ha[...], w2[:, cols]).astype(BF16)
            for j in range(2):
                v = t[:, j * 128:j * 128 + 128].astype(F32)
                qkv[s, :, pl.ds(pl.multiple_of(g * 384 + j * 128, 128), 128)] = (v * cos_t + pltpu.roll(v, 64, 1) * sin_t).astype(BF16)
            qkv[s, :, pl.ds(pl.multiple_of(g * 384 + 256, 128), 128)] = t[:, 256:384]

        put(2, n, qkv, o_qkv, block)

        @pl.loop(0, 4)
        def _(c):
            cols = pl.ds(pl.multiple_of(c * 512, 512), 512)
            u = dot_nn(hm[...], wu[:, cols]).astype(BF16).astype(F32)
            cdf = 0.5 * (1.0 + lax.erf(u * (0.5 ** 0.5)))
            get[cols, :] = (u * cdf).astype(BF16).T
            slope[s, :, cols] = cdf + u * (jnp.exp(-0.5 * u * u) * ((2.0 * jnp.pi) ** -0.5))

        put_t(3, get, o_gelu, block)
        put(4, n, slope, o_slope, block)

    fins = []

    def keep(buf, ref, slot, i):
        copy = pltpu.make_async_copy(buf.at[slot], ref.at[pl.ds(pl.multiple_of(slot * rows, rows), rows)], fin_sem.at[i])
        copy.start()
        fins.append(copy)

    loads[0].wait()
    loads[2].wait()
    keep(x_v, o_x, tp, 0)
    forward(((tp, 0), (tp, 1)), 0)
    xm[0].wait_recv()
    xm[4].start()
    xm[1].wait_recv()
    xm[5].start()
    for i in range(4):
        dm[i].start()
    forward(((prv, 0), (nxt, 1)), 1)
    xm[2].wait_recv()
    xm[3].wait_recv()
    keep(x_v, o_x, prv, 1)
    keep(x_v, o_x, nxt, 2)
    forward(((prv, 1), (nxt, 0)), 2)
    dm[0].wait_recv()
    dm[4].start()
    dm[1].wait_recv()
    dm[5].start()
    xm[4].wait_recv()
    xm[5].wait_recv()
    keep(x_v, o_x, opp, 3)
    forward(((opp, 0), (opp, 1)), 3)
    loads[1].wait()
    for i in range(2, 6):
        dm[i].wait_recv()
    for i, slot in enumerate((tp, prv, nxt, opp)):
        keep(dy_v, o_dy, slot, 4 + i)
    for m in xm + dm:
        m.wait_send()
    for copy in list(outs.values()) + fins + [w_out_copy]:
        copy.wait()


def front_call(x_loc, dy_loc, ln_params, cos_f, sin_f, w_rows, w_up):
    r, d = x_loc.shape
    t, f, n = 4 * r, w_up.shape[1], w_rows.shape[0] * 128 // d
    part = w_rows.shape[0] // 4
    hbm = pl.BlockSpec(memory_space=pl.ANY)
    vmem = pl.BlockSpec(memory_space=pltpu.VMEM)
    dma = pltpu.SemaphoreType.DMA
    shape = jax.ShapeDtypeStruct
    return pl.pallas_call(
        front_kernel,
        in_specs=[hbm, hbm, vmem, vmem, vmem, hbm, hbm],
        out_specs=[hbm] * 8 + [vmem] * 2,
        out_shape=[shape((t, d), BF16), shape((t, EARLY), BF16), shape((d, t), BF16), shape((d, t), BF16),
                   shape((t, n), BF16), shape((f, t), BF16), shape((t, f), F32), shape((d, n), BF16),
                   shape((t, 1), F32), shape((t, 1), F32)],
        scratch_shapes=[
            pltpu.VMEM((4, r, d), BF16), pltpu.VMEM((4, r, EARLY), BF16),
            pltpu.VMEM((d, n), BF16), pltpu.VMEM((d, f), BF16),
            pltpu.VMEM((2, part, 128), BF16), pltpu.VMEM((part, 128), F32),
            pltpu.VMEM((2, r, f), F32),
            pltpu.VMEM((r, d), BF16), pltpu.VMEM((r, d), BF16),
            pltpu.VMEM((d, r), BF16), pltpu.VMEM((d, r), BF16), pltpu.VMEM((f, r), BF16),
            pltpu.VMEM((2, r, n), BF16),
            dma((6,)), dma((6,)), dma((6,)), dma((6,)), dma((3,)), dma((2,)), dma((5, 2, 2)), dma((9,)),
        ],
        compiler_params=pltpu.CompilerParams(collective_id=1, has_side_effects=True, vmem_limit_bytes=64000 * 1024),
        cost_estimate=pl.CostEstimate(flops=2 * t * d * (n + f), bytes_accessed=70_000_000, transcendentals=2 * t * f),
        name='front',
    )(x_loc, dy_loc, ln_params, cos_f, sin_f, w_rows, w_up)


def back_kernel(get_ref, hmt_ref, hat_ref, dyp_ref, slope_ref, qkv_ref, wo_ref, wd_ref, w2_ref, wup_ref, x_ref, xloc_ref, dyloc_ref,
                ln_ref, mean_ref, rstd_ref, cos_ref, sin_ref,
                o_gx, o_ln, o_qkv, o_out, o_up, o_down,
                a_buf, b_buf, p_buf, d_buf, l1, f1, l2, f2, lnb, dh_v, dproj_v, ctxt, qkv_b, dctx_b, dk_s, dv_s,
                wq_t, wu_t, x_t, c_buf, cl1, cf1, sl_buf, dy_v, wo_t,
                a_sem, dy_sem, h_sem, t_sem, d_sem, g_sem, gs, gr, ds, dr, s_l1, r_l1, s_f1, r_f1, s_l2, r_l2, s_f2, r_f2, ln_s, ln_r,
                cs_l1, cr_l1, cs_f1, cr_f1, credit):
    tp = lax.axis_index('tp')
    dp = lax.axis_index('dp')
    core = lax.rem(dp, 2)
    y = lax.rem(dp // 2, 4)
    z = dp // 8
    partner = {'dp': dp + 1 - 2 * core}
    n_head = 4
    hd = 128
    blk = 256
    scale = hd ** -0.5

    def dev_y(i):
        return {'dp': z * 8 + i * 2 + core}

    def dev_z(i):
        return {'dp': i * 8 + y * 2 + core}

    def dev_x(i):
        return {'tp': i}

    def ring(i, d):
        return lax.rem(i + d, 4)

    def al(i, m):
        return pl.multiple_of(i * m, m)

    barrier = pltpu.get_barrier_semaphore()
    peers = [partner]
    for d in (1, 2, 3):
        peers += [dev_x(ring(tp, d)), dev_y(ring(y, d)), dev_z(ring(z, d))]
    for peer in peers:
        pl.semaphore_signal(barrier, inc=1, device_id=peer, device_id_type=MESH)

    def load_a(src, h):
        return pltpu.make_async_copy(src.at[pl.ds(al(h, 1024), 1024)], a_buf.at[h], a_sem.at[h])

    def load_x():
        return [pltpu.make_async_copy(xloc_ref.at[:, pl.ds(256 * u, 256)], x_t.at[u // 4, pl.ds(256 * (u % 4), 256)], g_sem) for u in range(8)]

    def load_head(h, slot):
        return [pltpu.make_async_copy(qkv_ref.at[:, pl.ds(pl.multiple_of(h * 384, 128), 384)], qkv_b.at[slot], h_sem.at[slot, 0]),
                pltpu.make_async_copy(wo_ref.at[pl.ds(al(h, 128), 128)], wo_t.at[slot], h_sem.at[slot, 1])]

    def load_d(k, slot):
        at = pl.ds(al(k, 256), 256)
        return [pltpu.make_async_copy(wd_ref.at[at], wu_t.at[slot], d_sem.at[slot, 0]),
                pltpu.make_async_copy(slope_ref.at[:, at], sl_buf.at[slot], d_sem.at[slot, 1])]

    def load_t(u, slot):
        at = pl.ds(al(u, 256), 256)
        return [pltpu.make_async_copy(w2_ref.at[at], wq_t.at[slot], t_sem.at[slot, 0]),
                pltpu.make_async_copy(wup_ref.at[at], wu_t.at[slot], t_sem.at[slot, 1]),
                pltpu.make_async_copy(x_ref.at[:, at], x_t.at[slot], t_sem.at[slot, 2])]

    def start(copies):
        for copy in copies:
            copy.start()

    def wait(copies):
        for copy in copies:
            copy.wait()

    for h in range(2):
        load_a(get_ref, jnp.int32(h)).start()
    early = pltpu.make_async_copy(dyp_ref, dy_v.at[:, pl.ds(0, EARLY)], dy_sem.at[0])
    early.start()
    late = pltpu.make_async_copy(dyloc_ref.at[:, pl.ds(EARLY, 256 * LATE)],
                                 dy_v.at[pl.ds(al(tp, 256), 256), pl.ds(EARLY, 256 * LATE)], dy_sem.at[1])
    late.start()
    start(load_head(jnp.int32(0), 0))
    start(load_d(jnp.int32(0), 0))
    pl.semaphore_wait(barrier, len(peers))

    def remote(src, dst, ssem, rsem, device):
        return pltpu.make_async_remote_copy(src_ref=src, dst_ref=dst, send_sem=ssem, recv_sem=rsem, device_id=device, device_id_type=MESH)

    def drain(ref, sem):
        pltpu.make_async_copy(ref, ref, sem).wait()

    def slice_copy(j, i):
        cols = pl.ds(pl.multiple_of(EARLY + j * 256, 256), 256)
        nxt, prv = ring(tp, 1), ring(tp, 3)
        owner, half, to = ((tp, 0, nxt), (tp, 1, prv), (tp, 1, nxt), (tp, 0, prv), (prv, 0, nxt), (nxt, 1, prv))[i]
        spot = dy_v.at[pl.ds(pl.multiple_of(owner * 256 + half * 128, 128), 128), cols]
        src = dyloc_ref.at[pl.ds(128 * half, 128), cols] if i < 4 else spot
        return remote(src, spot, gs.at[j, i], gr.at[j, i], dev_x(to))

    def slice_own(j):
        for i in range(4):
            slice_copy(j, i).start()

    def slice_on(j):
        for i in range(2):
            slice_copy(j, i).wait_recv()
            slice_copy(j, 4 + i).start()

    def slice_done(j):
        for i in range(2, 6):
            slice_copy(j, i).wait_recv()

    slice_own(jnp.int32(0))
    slice_own(jnp.int32(1))

    def pair_copy(p):
        slot = lax.rem(p, SLOTS)
        return remote(p_buf.at[lax.rem(p, 2), :, :, :, 1 - core], d_buf.at[slot], ds.at[slot], dr.at[slot], partner)

    def blk1(slot, col, i, half):
        rows = pl.ds(32 * half, 32)
        if col == 0:
            return d_buf.at[slot, 0, :, i, rows, :]
        return d_buf.at[slot, 1, i, :, rows, :]

    def blk2(slot, col, i, half):
        rows = pl.ds(32 * half, 32)
        if col == 0:
            return d_buf.at[slot, 0, i, y, rows, :]
        return d_buf.at[slot, 1, z, i, rows, :]

    me1 = (y, z)
    dev1 = (dev_y, dev_z)
    me2 = (z, y)
    dev2 = (dev_z, dev_y)

    def compute(p):
        ps = lax.rem(p, 2)

        @pl.when(p >= 2)
        def _():
            drain(p_buf.at[ps, :, :, :, 0], ds.at[lax.rem(p - 2, SLOTS)])

        @pl.when(p == 0)
        def _():
            early.wait()

        @pl.when(p == 3)
        def _():
            late.wait()

        @pl.when((p >= 3) & (p < 7))
        def _():
            slice_done(p - 3)

        @pl.when(p == 6)
        def _():
            slice_done(p - 2)

        @pl.when(p < 8)
        def _():
            b_buf[ps] = dy_v[:, pl.ds(al(p, 256), 256)]

        @pl.when((p >= 8) & (p < 16))
        def _():
            b_buf[ps] = dh_v[:, pl.ds(al(p - 8, 256), 256)]

        @pl.when((p >= 16) & (p < 22))
        def _():
            b_buf[ps] = dproj_v[:, pl.ds(al(p - 16, 256), 256)]

        @pl.when(p < 22)
        def _():
            @pl.loop(0, 2)
            def _(h):
                @pl.when((p == 0) | (p == 8) | (p == 16))
                def _():
                    load_a(get_ref, h).wait()

                tile = dot_nn(a_buf[h], b_buf[ps])
                for i in range(16):
                    for col in range(2):
                        p_buf[ps, col, 2 * h + i // 8, (i // 2) % 4, i % 2] = tile[64 * i:64 * i + 64, 128 * col:128 * col + 128]

                @pl.when(p == 7)
                def _():
                    load_a(hmt_ref, h).start()

                @pl.when(p == 15)
                def _():
                    load_a(hat_ref, h).start()

        @pl.when(p >= 22)
        def _():
            @pl.loop(0, 4)
            def _(k):
                tile = dot_nn(ctxt[...], dy_v[:, pl.ds(pl.multiple_of((p - 22) * 1024 + k * 256, 256), 256)])
                for i in range(32):
                    for col in range(2):
                        p_buf[ps, col, i // 8, (i // 2) % 4, i % 2, pl.ds(al(k, 16), 16), :] = tile[16 * i:16 * i + 16, 128 * col:128 * col + 128]

        @pl.when(p >= SLOTS)
        def _():
            pl.semaphore_wait(credit.at[0], 1)

        pair_copy(p).start()

    def first(blk, slot, me, dev, lands, finals, s_a, r_a, s_b, r_b):
        for col in range(2):
            nxt, opp, prv = ring(me[col], 1), ring(me[col], 2), ring(me[col], 3)
            remote(blk(slot, col, opp, 0), lands.at[slot, col, 0], s_a.at[slot], r_a.at[slot], dev[col](nxt)).start()
            remote(blk(slot, col, opp, 1), lands.at[slot, col, 1], s_a.at[slot], r_a.at[slot], dev[col](prv)).start()
        for col in range(2):
            nxt, prv = ring(me[col], 1), ring(me[col], 3)
            remote(blk(slot, col, nxt, 1), finals.at[slot, col, 0, 1], s_b.at[slot], r_b.at[slot], dev[col](nxt)).start()
            remote(blk(slot, col, prv, 0), finals.at[slot, col, 0, 0], s_b.at[slot], r_b.at[slot], dev[col](prv)).start()

    def second(blk, slot, me, dev, lands, finals, r_a, s_b, r_b):
        drain(lands.at[slot], r_a.at[slot])
        for col in range(2):
            nxt, prv = ring(me[col], 1), ring(me[col], 3)
            for half, to in ((0, nxt), (1, prv)):
                ref = blk(slot, col, to, half)
                ref[...] = ref[...] + lands[slot, col, half]
                remote(ref, finals.at[slot, col, 1, half], s_b.at[slot], r_b.at[slot], dev[col](to)).start()

    def stage_s(q):
        slot = lax.rem(q, SLOTS)
        ps = lax.rem(q, 2)
        drain(d_buf.at[slot], dr.at[slot])

        @pl.loop(0, 32)
        def _(i):
            col, zi, yi = i // 16, lax.rem(i // 4, 4), lax.rem(i, 4)
            d_buf[slot, col, zi, yi] = d_buf[slot, col, zi, yi] + p_buf[ps, col, zi, yi, core]

        @pl.when(q >= SLOTS)
        def _():
            for i in range(1, 5):
                pl.semaphore_wait(credit.at[i], 1)

        first(blk1, slot, me1, dev1, l1, f1, s_l1, r_l1, s_f1, r_f1)

    def stage_l1(q):
        second(blk1, lax.rem(q, SLOTS), me1, dev1, l1, f1, r_l1, s_f1, r_f1)

    def stage_f1(q):
        slot = lax.rem(q, SLOTS)
        drain(f1.at[slot], r_f1.at[slot])
        for col in range(2):
            for half in range(2):
                ref = blk1(slot, col, me1[col], half)
                ref[...] = ref[...] + (f1[slot, col, 0, half] + f1[slot, col, 1, half])
        first(blk2, slot, me2, dev2, l2, f2, s_l2, r_l2, s_f2, r_f2)

    def stage_l2(q):
        second(blk2, lax.rem(q, SLOTS), me2, dev2, l2, f2, r_l2, s_f2, r_f2)

    def stage_f2(q):
        slot = lax.rem(q, SLOTS)
        drain(f2.at[slot], r_f2.at[slot])
        for col in range(2):
            for half in range(2):
                rows = pl.ds(32 * half, 32)
                val = blk2(slot, col, me2[col], half)[...] + (f2[slot, col, 0, half] + f2[slot, col, 1, half])
                for out, lo, hi in ((o_down, 0, 8), (o_up, 8, 16), (o_qkv, 16, 22)):
                    @pl.when((q >= lo) & (q < hi))
                    def _():
                        out[rows, pl.ds(pl.multiple_of((q - lo) * 256 + col * 128, 128), 128)] = val

                @pl.when(q >= 22)
                def _():
                    for k in range(2):
                        at = (q - 22) * 1024 + (2 * half + k) * 256 + col * 128
                        o_out[:, pl.ds(pl.multiple_of(at, 128), 128)] = val[16 * k:16 * k + 16, :]
        drain(l1.at[slot], s_l1.at[slot])
        drain(f1.at[slot], s_f1.at[slot])
        drain(l2.at[slot], s_l2.at[slot])
        drain(f2.at[slot], s_f2.at[slot])

        @pl.when(q < PIECES - SLOTS)
        def _():
            to = (partner, dev_y(ring(y, 1)), dev_y(ring(y, 3)), dev_z(ring(z, 1)), dev_z(ring(z, 3)))
            for i in range(5):
                pl.semaphore_signal(credit.at[i], inc=1, device_id=to[i], device_id_type=MESH)

    def ln_send(stage):
        me, dev, n = ((core, None, 2), (tp, dev_x, 4), (y, dev_y, 4), (z, dev_z, 4))[stage]
        for d in range(1, n):
            to = partner if dev is None else dev(ring(me, d))
            remote(lnb.at[stage, me], lnb.at[stage, me], ln_s.at[stage], ln_r.at[stage], to).start()

    def ln_sum(stage):
        n = 2 if stage == 0 else 4
        ref = lnb.at[stage, pl.ds(0, n - 1)]
        drain(ref, ln_r.at[stage])
        drain(ref, ln_s.at[stage])
        if n == 2:
            return lnb[0, 0] + lnb[0, 1]
        return (lnb[stage, 0] + lnb[stage, 1]) + (lnb[stage, 2] + lnb[stage, 3])

    def unrope(d, rows):
        d = d.astype(BF16).astype(F32)
        return (d * cos_ref[rows, :] - pltpu.roll(d, hd // 2, 1) * sin_ref[rows, :]).astype(BF16)

    def attend(h, side):
        hs = lax.rem(h, 2)

        def cols(j):
            return pl.ds(pl.multiple_of(h * 384 + j * 128, 128), 128)

        if side == 0:
            wait(load_head(h, hs))

            @pl.when(h < n_head - 1)
            def _():
                start(load_head(h + 1, 1 - hs))

            dctx_b[...] = dot_nt(dy_v[...], wo_t[hs]).astype(BF16)
            dk_s[...] = jnp.zeros_like(dk_s)
            dv_s[...] = jnp.zeros_like(dv_s)

        for i in ((0, 3), (1, 2))[side]:
            rows, lo, n = slice(i * blk, (i + 1) * blk), i * blk, (i + 1) * blk
            qi, dci = qkv_b[hs, rows, 0:hd], dctx_b[rows, :]
            kn, vn = qkv_b[hs, :n, hd:2 * hd], qkv_b[hs, :n, 2 * hd:3 * hd]
            s = dot_nt(qi, kn)
            seen = lax.broadcasted_iota(jnp.int32, (blk, blk), 0) >= lax.broadcasted_iota(jnp.int32, (blk, blk), 1)
            diag = jnp.where(seen, s[:, lo:], -1e30)
            s = jnp.concatenate([s[:, :lo], diag], axis=1) if lo else diag
            e = jnp.exp((s - jnp.max(s, axis=1, keepdims=True)) * scale)
            p = e * (1.0 / jnp.sum(e, axis=1, keepdims=True))
            pb = p.astype(BF16)
            ctxt[pl.ds(al(h, hd), hd), rows] = dot_nn(pb, vn).astype(BF16).T
            dp_ = dot_nt(dci, vn).astype(BF16).astype(F32)
            dsb = (p * (dp_ - jnp.sum(p * dp_, axis=1, keepdims=True)) * scale).astype(BF16)
            dproj_v[rows, cols(0)] = unrope(dot_nn(dsb, kn), rows)
            dk_s[:n, :] = dk_s[:n, :] + dot_tt(dsb, qi)
            dv_s[:n, :] = dv_s[:n, :] + dot_tt(pb, dci)
        if side == 1:
            @pl.loop(0, 4)
            def _(m):
                at = pl.ds(al(m, blk), blk)
                dproj_v[at, cols(1)] = unrope(dk_s[at, :], at)
                dproj_v[at, cols(2)] = dv_s[at, :].astype(BF16)

    def down(k):
        ks = lax.rem(k, 2)
        wait(load_d(k, ks))

        @pl.when(k < 7)
        def _():
            start(load_d(k + 1, 1 - ks))

        d_gelu = dot_nt(dy_v[...], wu_t[ks]).astype(BF16).astype(F32)
        dh_v[:, pl.ds(al(k, 256), 256)] = (d_gelu * sl_buf[ks]).astype(BF16)

    def inputs(u):
        us = lax.rem(u, 2)
        cs = lax.rem(u, 5)
        wait(load_t(u, us))

        @pl.when(u < 7)
        def _():
            start(load_t(u + 1, 1 - us))

        at = pl.ds(al(u, 256), 256)
        gain_a, gain_m = ln_ref[0:1, at], ln_ref[2:3, at]
        sums = []
        for m in range(2):
            rows = slice(512 * m, 512 * m + 512)
            dha = dot_nt(dproj_v[rows, :], wq_t[us]).astype(BF16).astype(F32)
            dhm = dot_nt(dh_v[rows, :], wu_t[us]).astype(BF16).astype(F32)
            x_hat = (x_t[us, rows, :].astype(F32) - mean_ref[rows, :]) * rstd_ref[rows, :]
            c = (dha * gain_a + dhm * gain_m).astype(BF16)
            c_buf[cs, 2 * m] = c[:256]
            c_buf[cs, 2 * m + 1] = c[256:]
            sums.append([jnp.sum(v, axis=0, keepdims=True) for v in (dha * x_hat, dha, dhm * x_hat, dhm)])
        for i in range(4):
            lnb[0, core, i:i + 1, at] = sums[0][i] + sums[1][i]
        nxt, opp, prv = ring(tp, 1), ring(tp, 2), ring(tp, 3)
        remote(c_blk(u, opp, 0), cl1.at[u, 0], cs_l1.at[u], cr_l1.at[u], dev_x(nxt)).start()
        remote(c_blk(u, opp, 1), cl1.at[u, 1], cs_l1.at[u], cr_l1.at[u], dev_x(prv)).start()
        remote(c_blk(u, nxt, 1), cf1.at[u, 0, 1], cs_f1.at[u], cr_f1.at[u], dev_x(nxt)).start()
        remote(c_blk(u, prv, 0), cf1.at[u, 0, 0], cs_f1.at[u], cr_f1.at[u], dev_x(prv)).start()

    def c_blk(u, i, half):
        return c_buf.at[lax.rem(u, 5), i, pl.ds(128 * half, 128), :]

    def c_second(u):
        drain(cl1.at[u], cr_l1.at[u])
        for half, to in ((0, ring(tp, 1)), (1, ring(tp, 3))):
            ref = c_blk(u, to, half)
            ref[...] = (ref[...].astype(F32) + cl1[u, half].astype(F32)).astype(BF16)
            remote(ref, cf1.at[u, 1, half], cs_f1.at[u], cr_f1.at[u], dev_x(to)).start()

    def c_final(u):
        drain(cf1.at[u], cr_f1.at[u])
        for half in range(2):
            sl_buf[u // 4, pl.ds(pl.multiple_of(lax.rem(u, 4) * 256 + 128 * half, 128), 128), :] = c_blk(u, tp, half)[...].astype(F32) + (
                cf1[u, 0, half].astype(F32) + cf1[u, 1, half].astype(F32))
        drain(cl1.at[u], cs_l1.at[u])
        drain(cf1.at[u], cs_f1.at[u])

    def last():
        drain(x_t, g_sem)

        @pl.loop(0, 8)
        def _(r):
            def across(ref):
                return jnp.concatenate([ref[u // 4, pl.ds(pl.multiple_of(256 * (u % 4) + r * 32, 32), 32), :] for u in range(8)], axis=1).astype(F32)

            own = pl.ds(pl.multiple_of(tp * 256 + r * 32, 32), 32)
            rstd = rstd_ref[own, :]
            c = across(sl_buf)
            x_hat = (across(x_t) - mean_ref[own, :]) * rstd
            dx = rstd * (c - jnp.mean(c, axis=-1, keepdims=True) - x_hat * jnp.mean(c * x_hat, axis=-1, keepdims=True))
            o_gx[pl.ds(al(r, 32), 32), :] = (dy_v[own, :].astype(F32) + dx).astype(BF16)

    @pl.loop(0, STEPS)
    def _(p):
        @pl.when(p < PIECES)
        def _():
            compute(p)

        for lag, stage in ((9, stage_f2), (8, stage_l2), (7, stage_f1), (4, stage_l1), (1, stage_s)):
            @pl.when((p >= lag) & (p < PIECES + lag))
            def _():
                stage(p - lag)

        @pl.when((p >= 22) & (p < 30))
        def _():
            c_final(p - 22)

        @pl.when((p >= 20) & (p < 28))
        def _():
            c_second(p - 20)

        @pl.when(p < LATE)
        def _():
            slice_on(p)

        @pl.when(p < LATE - 2)
        def _():
            slice_own(p + 2)

        @pl.when((p >= 6) & (p < 14))
        def _():
            down(p - 6)

        for side, steps in enumerate(((7, 11, 14, 16), (9, 13, 15, 17))):
            @pl.when((p == steps[0]) | (p == steps[1]) | (p == steps[2]) | (p == steps[3]))
            def _():
                attend(sum((p >= at).astype(jnp.int32) for at in steps[1:]), side)

        @pl.when(p == 10)
        def _():
            for j in range(LATE):
                for i in range(6):
                    slice_copy(j, i).wait_send()

        @pl.when(p == 14)
        def _():
            start(load_t(0, 0))

        @pl.when((p >= 18) & (p < 26))
        def _():
            inputs(p - 18)

        @pl.when(p == 26)
        def _():
            start(load_x())
            ln_send(0)

        for stage, me in ((1, tp), (2, y), (3, z)):
            @pl.when(p == 26 + stage)
            def _():
                lnb[stage, me] = ln_sum(stage - 1)
                ln_send(stage)

        @pl.when(p == 30)
        def _():
            last()

        @pl.when(p == 30)
        def _():
            o_ln[...] = ln_sum(3)

    for p in (PIECES - 2, PIECES - 1):
        drain(p_buf.at[p % 2, :, :, :, 0], ds.at[p % SLOTS])


def back_call(get, hmt, hat, dy_early, slope, qkv, w_out, w_down, w2, w_up, x_full, x_loc, dy_loc, ln_params, mean, rstd, cos_f, sin_f):
    hbm = pl.BlockSpec(memory_space=pl.ANY)
    vmem = pl.BlockSpec(memory_space=pltpu.VMEM)
    dma = pltpu.SemaphoreType.DMA
    shape = jax.ShapeDtypeStruct
    k = (SLOTS,)
    return pl.pallas_call(
        back_kernel,
        in_specs=[hbm] * 13 + [vmem] * 5,
        out_specs=[vmem] * 6,
        out_shape=[shape((256, 2048), BF16), shape((4, 2048), F32), shape((64, 1536), F32), shape((16, 2048), F32),
                   shape((64, 2048), F32), shape((64, 2048), F32)],
        scratch_shapes=[
            pltpu.VMEM((2, 1024, 1024), BF16), pltpu.VMEM((2, 1024, 256), BF16),
            pltpu.VMEM((2, 2, 4, 4, 2, 64, 128), F32), pltpu.VMEM(k + (2, 4, 4, 64, 128), F32),
            pltpu.VMEM(k + (2, 2, 4, 32, 128), F32), pltpu.VMEM(k + (2, 2, 2, 4, 32, 128), F32),
            pltpu.VMEM(k + (2, 2, 32, 128), F32), pltpu.VMEM(k + (2, 2, 2, 32, 128), F32),
            pltpu.VMEM((4, 4, 4, 2048), F32),
            pltpu.VMEM((1024, 2048), BF16), pltpu.VMEM((1024, 1536), BF16), pltpu.VMEM((512, 1024), BF16),
            pltpu.VMEM((2, 1024, 384), BF16), pltpu.VMEM((1024, 128), BF16),
            pltpu.VMEM((1024, 128), F32), pltpu.VMEM((1024, 128), F32),
            pltpu.VMEM((2, 256, 1536), BF16), pltpu.VMEM((2, 256, 2048), BF16), pltpu.VMEM((2, 1024, 256), BF16),
            pltpu.VMEM((5, 4, 256, 256), BF16), pltpu.VMEM((8, 2, 128, 256), BF16), pltpu.VMEM((8, 2, 2, 128, 256), BF16),
            pltpu.VMEM((2, 1024, 256), F32), pltpu.VMEM((1024, 2048), BF16), pltpu.VMEM((2, 128, 2048), BF16),
            dma((2,)), dma((2,)), dma((2, 2)), dma((2, 3)), dma((2, 2)), dma, dma((LATE, 6)), dma((LATE, 6)),
            dma(k), dma(k), dma(k), dma(k), dma(k), dma(k), dma(k), dma(k), dma(k), dma(k),
            dma((4,)), dma((4,)), dma((8,)), dma((8,)), dma((8,)), dma((8,)),
            pltpu.SemaphoreType.REGULAR((5,)),
        ],
        compiler_params=pltpu.CompilerParams(collective_id=0, has_side_effects=True, vmem_limit_bytes=65400 * 1024),
        cost_estimate=pl.CostEstimate(flops=50_000_000_000, bytes_accessed=100_000_000, transcendentals=0),
        name='back',
    )(get, hmt, hat, dy_early, slope, qkv, w_out, w_down, w2, w_up, x_full, x_loc, dy_loc, ln_params, mean, rstd, cos_f, sin_f)


def place_kernel(gx, ln, qkv, out, up, down, o_gx, o_ln, o_qkv, o_out, o_up, o_down, b_gx, b_ln, b_qkv, b_out, b_up, b_down, b_rows, in_sem, out_sem):
    ins = [pltpu.make_async_copy(src, buf, in_sem.at[i]) for i, (src, buf) in enumerate(
        ((qkv, b_qkv), (gx, b_gx), (ln, b_ln), (out, b_out), (up, b_up), (down, b_down)))]
    outs = [pltpu.make_async_copy(buf, dst, out_sem.at[i]) for i, (buf, dst) in enumerate(
        ((b_rows, o_qkv), (b_gx, o_gx), (b_ln, o_ln), (b_out, o_out), (b_up, o_up), (b_down, o_down)))]
    for copy in ins:
        copy.start()
    for i in range(1, 6):
        ins[i].wait()
        outs[i].start()
    ins[0].wait()
    for g in range(4):
        for j in range(3):
            b_rows[:, j, g, :] = b_qkv[:, g * 384 + j * 128:g * 384 + j * 128 + 128]
    outs[0].start()
    for copy in outs:
        copy.wait()


def place_call(gx, ln, qkv, out, up, down):
    hbm = pl.BlockSpec(memory_space=pl.ANY)
    dma = pltpu.SemaphoreType.DMA
    arrays = (gx, ln, qkv, out, up, down)
    rows = (qkv.shape[0], 3, 4, 128)
    shapes = [jax.ShapeDtypeStruct(rows if v is qkv else v.shape, v.dtype) for v in arrays]
    return pl.pallas_call(
        place_kernel,
        in_specs=[hbm] * 6,
        out_specs=[hbm] * 6,
        out_shape=shapes,
        scratch_shapes=[pltpu.VMEM(v.shape, v.dtype) for v in arrays] + [pltpu.VMEM(rows, F32), dma((6,)), dma((6,))],
        compiler_params=pltpu.CompilerParams(vmem_limit_bytes=VMEM_LIMIT),
        name='place',
    )(*arrays)


def solution(mesh):
    def local_step(x_loc, dy_loc, ln_params, w_qkv, w_out, w_up, w_down):
        width, groups, slots, head_dim = w_qkv.shape
        cos_f, sin_f = (jnp.asarray(t) for t in rope_tables(4 * x_loc.shape[1], head_dim))
        w_rows = w_qkv.transpose(0, 2, 1, 3).reshape(width * slots * groups, head_dim)
        x_full, dy_early, hat, hmt, qkv, get, slope, w2, mean, rstd = front_call(x_loc[0], dy_loc[0], ln_params, cos_f, sin_f, w_rows, w_up)
        grad_x, g_ln, g_qkv, g_out, g_up, g_down = back_call(
            get, hmt, hat, dy_early, slope, qkv, w_out, w_down, w2, w_up, x_full, x_loc[0], dy_loc[0], ln_params, mean, rstd, cos_f, sin_f)
        grad_x, g_ln, g_qkv, g_out, g_up, g_down = place_call(grad_x, g_ln, g_qkv, g_out, g_up, g_down)
        return grad_x[None], g_ln, g_qkv.transpose(0, 2, 1, 3), g_out, g_up, g_down

    act_spec = P('dp', 'tp', None)
    in_specs = (act_spec, act_spec, P(None, None), P(None, 'tp', None, None), P('tp', None), P(None, 'tp'), P('tp', None))
    out_specs = (act_spec, P(None, None), P('dp', 'tp', None, None), P(('tp', 'dp'), None), P('dp', 'tp'), P(('tp', 'dp'), None))
    return jax.shard_map(local_step, mesh=mesh, in_specs=in_specs, out_specs=out_specs, check_vma=False)
```

```python
import functools

import jax
import jax.numpy as jnp
import numpy as np
from jax import lax
from jax.experimental import pallas as pl
from jax.experimental.pallas import tpu as pltpu
from jax.sharding import PartitionSpec as P

NORM_EPS = 1e-5
ROPE_BASE = 10000.0
MESH = pl.DeviceIdType.MESH
PIECES = 24
SLOTS = 8
STEPS = PIECES + 7
EARLY = 768
LATE = 5
VMEM_LIMIT = 60000 * 1024
F32 = jnp.float32
BF16 = jnp.bfloat16


def rope_tables(seq_len, head_dim):
    half_dim = head_dim // 2
    inv_freq = np.float32(ROPE_BASE) ** (np.float32(-2.0) * np.arange(half_dim, dtype=np.float32) / np.float32(head_dim))
    angles = np.arange(seq_len, dtype=np.float32)[:, None] * inv_freq[None, :].astype(np.float32)
    cos_t, sin_t = np.cos(angles), np.sin(angles)
    return np.concatenate([cos_t, cos_t], axis=1), np.concatenate([-sin_t, sin_t], axis=1)


def dot_nn(lhs, rhs):
    return lax.dot_general(lhs, rhs, (((1,), (0,)), ((), ())), preferred_element_type=F32)


def dot_nt(lhs, rhs):
    return lax.dot_general(lhs, rhs, (((1,), (1,)), ((), ())), preferred_element_type=F32)


def dot_tt(lhs, rhs):
    return lax.dot_general(lhs, rhs, (((0,), (0,)), ((), ())), preferred_element_type=F32)


def front_kernel(x_ref, dy_ref, ln_ref, cos_ref, sin_ref, wq_ref, wu_ref,
                 o_x, o_dy, o_ha, o_hm, o_qkv, o_gelu, o_slope, o_w, mean_ref, rstd_ref,
                 x_v, dy_v, w2, wu, wq_b, wq_f, slope, ha, hm, hat, hmt, get, qkv,
                 xs, xr, ds, dr, in_sem, wq_sem, out_sem, fin_sem):
    tp = lax.axis_index('tp')
    nxt, opp, prv = lax.rem(tp + 1, 4), lax.rem(tp + 2, 4), lax.rem(tp + 3, 4)
    d_model = x_ref.shape[1]
    rows = x_ref.shape[0]
    half = rows // 2
    part = wq_b.shape[1]
    barrier = pltpu.get_barrier_semaphore()
    for peer in (nxt, prv):
        pl.semaphore_signal(barrier, inc=1, device_id={'tp': peer}, device_id_type=MESH)

    def wq_copy(i):
        return pltpu.make_async_copy(wq_ref.at[pl.ds(i * part, part)], wq_b.at[i % 2], wq_sem.at[i % 2])

    dy_own = dy_ref.at[:, pl.ds(0, EARLY)]
    loads = [pltpu.make_async_copy(x_ref, x_v.at[tp], in_sem.at[0]), pltpu.make_async_copy(dy_own, dy_v.at[tp], in_sem.at[1]),
             pltpu.make_async_copy(wu_ref, wu, in_sem.at[2])]
    wq_copy(0).start()
    loads[0].start()
    wq_copy(1).start()
    loads[2].start()
    loads[1].start()
    pl.semaphore_wait(barrier, 2)

    A, B = pl.ds(0, half), pl.ds(half, half)

    def moves(src, buf, ssem, rsem):
        def one(i, ref, slot, piece, to):
            return pltpu.make_async_remote_copy(src_ref=ref, dst_ref=buf.at[slot, piece], send_sem=ssem.at[i], recv_sem=rsem.at[i],
                                                device_id={'tp': to}, device_id_type=MESH)
        return [one(0, src.at[A], tp, A, nxt), one(1, src.at[B], tp, B, prv), one(2, src.at[B], tp, B, nxt), one(3, src.at[A], tp, A, prv),
                one(4, buf.at[prv, A], prv, A, nxt), one(5, buf.at[nxt, B], nxt, B, prv)]

    xm = moves(x_ref, x_v, xs, xr)
    dm = moves(dy_own, dy_v, ds, dr)
    for i in range(4):
        xm[i].start()

    per = part // 12
    for i in range(wq_ref.shape[0] // part):
        wq_copy(i).wait()

        @pl.loop(0, part // 256)
        def _(r):
            at = pl.ds(pl.multiple_of(r * 256, 256), 256)
            wq_f[at, :] = wq_b[i % 2, at, :].astype(F32)

        if i + 2 < wq_ref.shape[0] // part:
            wq_copy(i + 2).start()
        for j in range(3):
            for g in range(4):
                w2[i * per:(i + 1) * per, g * 384 + j * 128:g * 384 + j * 128 + 128] = wq_f[pl.ds(j * 4 + g, per, stride=12), :].astype(BF16)
    w_out_copy = pltpu.make_async_copy(w2, o_w, fin_sem.at[8])
    w_out_copy.start()

    outs = {}

    def tokens(block, i):
        slot, side = block[i]
        return pl.ds(pl.multiple_of(slot * rows + side * half, half), half)

    def put(kind, n, buf, ref, block):
        for i in range(2):
            copy = pltpu.make_async_copy(buf.at[n % 2, pl.ds(i * half, half)], ref.at[tokens(block, i)], out_sem.at[kind, n % 2, i])
            copy.start()
            outs[kind, n % 2, i] = copy

    def put_t(kind, buf, ref, block):
        for i in range(2):
            copy = pltpu.make_async_copy(buf.at[:, pl.ds(i * half, half)], ref.at[:, tokens(block, i)], out_sem.at[kind, 0, i])
            copy.start()
            outs[kind, 0, i] = copy

    def free(kind, n):
        for i in range(2):
            if (kind, n % 2, i) in outs:
                outs.pop((kind, n % 2, i)).wait()

    def forward(block, n):
        s = n % 2
        for i in range(2):
            slot, side = block[i]

            @pl.loop(0, half // 32)
            def _(r):
                src = pl.ds(pl.multiple_of(side * half + r * 32, 32), 32)
                at = pl.ds(pl.multiple_of(i * half + r * 32, 32), 32)
                to = pl.ds(pl.multiple_of(slot * rows + side * half + r * 32, 32), 32)
                xf = x_v[slot, src, :].astype(F32)
                mean = jnp.mean(xf, axis=-1, keepdims=True)
                cen = xf - mean
                rstd = lax.rsqrt(jnp.mean(cen * cen, axis=-1, keepdims=True) + NORM_EPS)
                mean_ref[to, :] = mean
                rstd_ref[to, :] = rstd
                x_hat = cen * rstd
                ha[at, :] = (x_hat * ln_ref[0:1, :] + ln_ref[1:2, :]).astype(BF16)
                hm[at, :] = (x_hat * ln_ref[2:3, :] + ln_ref[3:4, :]).astype(BF16)

        for kind in (0, 1, 3):
            free(kind, 0)
        free(2, n)
        free(4, n)

        @pl.loop(0, d_model // 256)
        def _(c):
            cols = pl.ds(pl.multiple_of(c * 256, 256), 256)
            hat[cols, :] = ha[:, cols].T
            hmt[cols, :] = hm[:, cols].T

        put_t(0, hat, o_ha, block)
        put_t(1, hmt, o_hm, block)
        cos_t, sin_t = (jnp.concatenate([ref[tokens(block, 0), :], ref[tokens(block, 1), :]], axis=0) for ref in (cos_ref, sin_ref))

        @pl.loop(0, 4)
        def _(g):
            cols = pl.ds(pl.multiple_of(g * 384, 128), 384)
            t = dot_nn(ha[...], w2[:, cols]).astype(BF16)
            for j in range(2):
                v = t[:, j * 128:j * 128 + 128].astype(F32)
                qkv[s, :, pl.ds(pl.multiple_of(g * 384 + j * 128, 128), 128)] = (v * cos_t + pltpu.roll(v, 64, 1) * sin_t).astype(BF16)
            qkv[s, :, pl.ds(pl.multiple_of(g * 384 + 256, 128), 128)] = t[:, 256:384]

        put(2, n, qkv, o_qkv, block)

        @pl.loop(0, 4)
        def _(c):
            cols = pl.ds(pl.multiple_of(c * 512, 512), 512)
            u = dot_nn(hm[...], wu[:, cols]).astype(BF16).astype(F32)
            cdf = 0.5 * (1.0 + lax.erf(u * (0.5 ** 0.5)))
            get[cols, :] = (u * cdf).astype(BF16).T
            slope[s, :, cols] = cdf + u * (jnp.exp(-0.5 * u * u) * ((2.0 * jnp.pi) ** -0.5))

        put_t(3, get, o_gelu, block)
        put(4, n, slope, o_slope, block)

    fins = []

    def keep(buf, ref, slot, i):
        copy = pltpu.make_async_copy(buf.at[slot], ref.at[pl.ds(pl.multiple_of(slot * rows, rows), rows)], fin_sem.at[i])
        copy.start()
        fins.append(copy)

    loads[0].wait()
    loads[2].wait()
    keep(x_v, o_x, tp, 0)
    forward(((tp, 0), (tp, 1)), 0)
    xm[0].wait_recv()
    xm[4].start()
    xm[1].wait_recv()
    xm[5].start()
    for i in range(4):
        dm[i].start()
    forward(((prv, 0), (nxt, 1)), 1)
    xm[2].wait_recv()
    xm[3].wait_recv()
    keep(x_v, o_x, prv, 1)
    keep(x_v, o_x, nxt, 2)
    forward(((prv, 1), (nxt, 0)), 2)
    dm[0].wait_recv()
    dm[4].start()
    dm[1].wait_recv()
    dm[5].start()
    xm[4].wait_recv()
    xm[5].wait_recv()
    keep(x_v, o_x, opp, 3)
    forward(((opp, 0), (opp, 1)), 3)
    loads[1].wait()
    for i in range(2, 6):
        dm[i].wait_recv()
    for i, slot in enumerate((tp, prv, nxt, opp)):
        keep(dy_v, o_dy, slot, 4 + i)
    for m in xm + dm:
        m.wait_send()
    for copy in list(outs.values()) + fins + [w_out_copy]:
        copy.wait()


def front_call(x_loc, dy_loc, ln_params, cos_f, sin_f, w_rows, w_up):
    r, d = x_loc.shape
    t, f, n = 4 * r, w_up.shape[1], w_rows.shape[0] * 128 // d
    part = w_rows.shape[0] // 4
    hbm = pl.BlockSpec(memory_space=pl.ANY)
    vmem = pl.BlockSpec(memory_space=pltpu.VMEM)
    dma = pltpu.SemaphoreType.DMA
    shape = jax.ShapeDtypeStruct
    return pl.pallas_call(
        front_kernel,
        in_specs=[hbm, hbm, vmem, vmem, vmem, hbm, hbm],
        out_specs=[hbm] * 8 + [vmem] * 2,
        out_shape=[shape((t, d), BF16), shape((t, EARLY), BF16), shape((d, t), BF16), shape((d, t), BF16),
                   shape((t, n), BF16), shape((f, t), BF16), shape((t, f), F32), shape((d, n), BF16),
                   shape((t, 1), F32), shape((t, 1), F32)],
        scratch_shapes=[
            pltpu.VMEM((4, r, d), BF16), pltpu.VMEM((4, r, EARLY), BF16),
            pltpu.VMEM((d, n), BF16), pltpu.VMEM((d, f), BF16),
            pltpu.VMEM((2, part, 128), BF16), pltpu.VMEM((part, 128), F32),
            pltpu.VMEM((2, r, f), F32),
            pltpu.VMEM((r, d), BF16), pltpu.VMEM((r, d), BF16),
            pltpu.VMEM((d, r), BF16), pltpu.VMEM((d, r), BF16), pltpu.VMEM((f, r), BF16),
            pltpu.VMEM((2, r, n), BF16),
            dma((6,)), dma((6,)), dma((6,)), dma((6,)), dma((3,)), dma((2,)), dma((5, 2, 2)), dma((9,)),
        ],
        compiler_params=pltpu.CompilerParams(collective_id=1, has_side_effects=True, vmem_limit_bytes=64000 * 1024),
        cost_estimate=pl.CostEstimate(flops=2 * t * d * (n + f), bytes_accessed=70_000_000, transcendentals=2 * t * f),
        name='front',
    )(x_loc, dy_loc, ln_params, cos_f, sin_f, w_rows, w_up)


def back_kernel(get_ref, hmt_ref, hat_ref, dyp_ref, slope_ref, qkv_ref, wo_ref, wd_ref, w2_ref, wup_ref, x_ref, xloc_ref, dyloc_ref,
                ln_ref, mean_ref, rstd_ref, cos_ref, sin_ref,
                o_gx, o_ln, o_qkv, o_out, o_up, o_down,
                a_buf, b_buf, p_buf, d_buf, l1, f1, l2, f2, lnb, dh_v, dproj_v, ctxt, qkv_b, dctx_b, dk_s, dv_s,
                wq_t, wu_t, x_t, c_buf, cl1, cf1, sl_buf, dy_v, wo_t, kt, vt,
                a_sem, dy_sem, h_sem, t_sem, d_sem, g_sem, gs, gr, ds, dr, s_l1, r_l1, s_f1, r_f1, s_l2, r_l2, s_f2, r_f2, ln_s, ln_r,
                cs_l1, cr_l1, cs_f1, cr_f1, credit):
    tp = lax.axis_index('tp')
    dp = lax.axis_index('dp')
    core = lax.rem(dp, 2)
    y = lax.rem(dp // 2, 4)
    z = dp // 8
    partner = {'dp': dp + 1 - 2 * core}
    n_head = 4
    hd = 128
    blk = 256
    scale = hd ** -0.5

    def dev_y(i):
        return {'dp': z * 8 + i * 2 + core}

    def dev_z(i):
        return {'dp': i * 8 + y * 2 + core}

    def dev_x(i):
        return {'tp': i}

    def ring(i, d):
        return lax.rem(i + d, 4)

    def al(i, m):
        return pl.multiple_of(i * m, m)

    barrier = pltpu.get_barrier_semaphore()
    peers = [partner]
    for d in (1, 2, 3):
        peers += [dev_x(ring(tp, d)), dev_y(ring(y, d)), dev_z(ring(z, d))]
    for peer in peers:
        pl.semaphore_signal(barrier, inc=1, device_id=peer, device_id_type=MESH)

    def load_a(src, h):
        return pltpu.make_async_copy(src.at[pl.ds(al(h, 1024), 1024)], a_buf.at[h], a_sem.at[h])

    def load_x():
        return [pltpu.make_async_copy(xloc_ref.at[:, pl.ds(256 * u, 256)], x_t.at[u // 4, pl.ds(256 * (u % 4), 256)], g_sem) for u in range(8)]

    def load_head(h, slot):
        return [pltpu.make_async_copy(qkv_ref.at[:, pl.ds(pl.multiple_of(h * 384, 128), 384)], qkv_b.at[slot], h_sem.at[slot, 0]),
                pltpu.make_async_copy(wo_ref.at[pl.ds(al(h, 128), 128)], wo_t.at[slot], h_sem.at[slot, 1])]

    def load_d(k, slot):
        at = pl.ds(al(k, 256), 256)
        return [pltpu.make_async_copy(wd_ref.at[at], wu_t.at[slot], d_sem.at[slot, 0]),
                pltpu.make_async_copy(slope_ref.at[:, at], sl_buf.at[slot], d_sem.at[slot, 1])]

    def load_t(u, slot):
        at = pl.ds(al(u, 256), 256)
        return [pltpu.make_async_copy(w2_ref.at[at], wq_t.at[slot], t_sem.at[slot, 0]),
                pltpu.make_async_copy(wup_ref.at[at], wu_t.at[slot], t_sem.at[slot, 1]),
                pltpu.make_async_copy(x_ref.at[:, at], x_t.at[slot], t_sem.at[slot, 2])]

    def start(copies):
        for copy in copies:
            copy.start()

    def wait(copies):
        for copy in copies:
            copy.wait()

    for h in range(2):
        load_a(get_ref, jnp.int32(h)).start()
    early = pltpu.make_async_copy(dyp_ref, dy_v.at[:, pl.ds(0, EARLY)], dy_sem.at[0])
    early.start()
    late = pltpu.make_async_copy(dyloc_ref.at[:, pl.ds(EARLY, 256 * LATE)],
                                 dy_v.at[pl.ds(al(tp, 256), 256), pl.ds(EARLY, 256 * LATE)], dy_sem.at[1])
    late.start()
    start(load_head(jnp.int32(0), 0))
    start(load_d(jnp.int32(0), 0))
    pl.semaphore_wait(barrier, len(peers))

    def remote(src, dst, ssem, rsem, device):
        return pltpu.make_async_remote_copy(src_ref=src, dst_ref=dst, send_sem=ssem, recv_sem=rsem, device_id=device, device_id_type=MESH)

    def drain(ref, sem):
        pltpu.make_async_copy(ref, ref, sem).wait()

    def slice_copy(j, i):
        cols = pl.ds(pl.multiple_of(EARLY + j * 256, 256), 256)
        nxt, prv = ring(tp, 1), ring(tp, 3)
        owner, half, to = ((tp, 0, nxt), (tp, 1, prv), (tp, 1, nxt), (tp, 0, prv), (prv, 0, nxt), (nxt, 1, prv))[i]
        spot = dy_v.at[pl.ds(pl.multiple_of(owner * 256 + half * 128, 128), 128), cols]
        src = dyloc_ref.at[pl.ds(128 * half, 128), cols] if i < 4 else spot
        return remote(src, spot, gs.at[j, i], gr.at[j, i], dev_x(to))

    def slice_own(j):
        for i in range(4):
            slice_copy(j, i).start()

    def slice_on(j):
        for i in range(2):
            slice_copy(j, i).wait_recv()
            slice_copy(j, 4 + i).start()

    def slice_done(j):
        for i in range(2, 6):
            slice_copy(j, i).wait_recv()

    slice_own(jnp.int32(0))
    slice_own(jnp.int32(1))

    def pair_copy(p):
        slot = lax.rem(p, SLOTS)
        return remote(p_buf.at[lax.rem(p, 2), :, :, :, 1 - core], d_buf.at[slot], ds.at[slot], dr.at[slot], partner)

    def blk1(slot, col, i, half):
        rows = pl.ds(32 * half, 32)
        if col == 0:
            return d_buf.at[slot, 0, :, i, rows, :]
        return d_buf.at[slot, 1, i, :, rows, :]

    def blk2(slot, col, i, half):
        rows = pl.ds(32 * half, 32)
        if col == 0:
            return d_buf.at[slot, 0, i, y, rows, :]
        return d_buf.at[slot, 1, z, i, rows, :]

    me1 = (y, z)
    dev1 = (dev_y, dev_z)
    me2 = (z, y)
    dev2 = (dev_z, dev_y)

    def compute(p):
        ps = lax.rem(p, 2)

        @pl.when(p >= 2)
        def _():
            drain(p_buf.at[ps, :, :, :, 0], ds.at[lax.rem(p - 2, SLOTS)])

        @pl.when(p == 0)
        def _():
            early.wait()

        @pl.when(p == 3)
        def _():
            late.wait()

        @pl.when((p >= 3) & (p < 7))
        def _():
            slice_done(p - 3)

        @pl.when(p == 6)
        def _():
            slice_done(p - 2)

        @pl.when(p < 8)
        def _():
            b_buf[ps] = dy_v[:, pl.ds(al(p, 256), 256)]

        @pl.when((p >= 8) & (p < 16))
        def _():
            b_buf[ps] = dh_v[:, pl.ds(al(p - 8, 256), 256)]

        @pl.when((p >= 16) & (p < 22))
        def _():
            b_buf[ps] = dproj_v[:, pl.ds(al(p - 16, 256), 256)]

        @pl.when(p < 22)
        def _():
            @pl.loop(0, 2)
            def _(h):
                @pl.when((p == 0) | (p == 8) | (p == 16))
                def _():
                    load_a(get_ref, h).wait()

                tile = dot_nn(a_buf[h], b_buf[ps])
                for i in range(16):
                    for col in range(2):
                        p_buf[ps, col, 2 * h + i // 8, (i // 2) % 4, i % 2] = tile[64 * i:64 * i + 64, 128 * col:128 * col + 128]

                @pl.when(p == 7)
                def _():
                    load_a(hmt_ref, h).start()

                @pl.when(p == 15)
                def _():
                    load_a(hat_ref, h).start()

        @pl.when(p >= 22)
        def _():
            @pl.loop(0, 4)
            def _(k):
                tile = dot_nn(ctxt[...], dy_v[:, pl.ds(pl.multiple_of((p - 22) * 1024 + k * 256, 256), 256)])
                for i in range(32):
                    for col in range(2):
                        p_buf[ps, col, i // 8, (i // 2) % 4, i % 2, pl.ds(al(k, 16), 16), :] = tile[16 * i:16 * i + 16, 128 * col:128 * col + 128]

        @pl.when(p >= SLOTS)
        def _():
            pl.semaphore_wait(credit.at[0], 1)

        pair_copy(p).start()

    def first(blk, slot, me, dev, lands, finals, s_a, r_a, s_b, r_b):
        for col in range(2):
            nxt, opp, prv = ring(me[col], 1), ring(me[col], 2), ring(me[col], 3)
            remote(blk(slot, col, opp, 0), lands.at[slot, col, 0], s_a.at[slot], r_a.at[slot], dev[col](nxt)).start()
            remote(blk(slot, col, opp, 1), lands.at[slot, col, 1], s_a.at[slot], r_a.at[slot], dev[col](prv)).start()
        for col in range(2):
            nxt, prv = ring(me[col], 1), ring(me[col], 3)
            remote(blk(slot, col, nxt, 1), finals.at[slot, col, 0, 1], s_b.at[slot], r_b.at[slot], dev[col](nxt)).start()
            remote(blk(slot, col, prv, 0), finals.at[slot, col, 0, 0], s_b.at[slot], r_b.at[slot], dev[col](prv)).start()

    def second(blk, slot, me, dev, lands, finals, r_a, s_b, r_b):
        drain(lands.at[slot], r_a.at[slot])
        for col in range(2):
            nxt, prv = ring(me[col], 1), ring(me[col], 3)
            for half, to in ((0, nxt), (1, prv)):
                ref = blk(slot, col, to, half)
                ref[...] = ref[...] + lands[slot, col, half]
                remote(ref, finals.at[slot, col, 1, half], s_b.at[slot], r_b.at[slot], dev[col](to)).start()

    def stage_s(q):
        slot = lax.rem(q, SLOTS)
        ps = lax.rem(q, 2)
        drain(d_buf.at[slot], dr.at[slot])

        @pl.loop(0, 8)
        def _(i):
            col, zi = i // 4, lax.rem(i, 4)
            d_buf[slot, col, zi] = d_buf[slot, col, zi] + p_buf[ps, col, zi, :, core]

        @pl.when(q >= SLOTS)
        def _():
            for i in range(1, 5):
                pl.semaphore_wait(credit.at[i], 1)

        first(blk1, slot, me1, dev1, l1, f1, s_l1, r_l1, s_f1, r_f1)

    def stage_l1(q):
        second(blk1, lax.rem(q, SLOTS), me1, dev1, l1, f1, r_l1, s_f1, r_f1)

    def stage_f1(q):
        slot = lax.rem(q, SLOTS)
        drain(f1.at[slot], r_f1.at[slot])
        for col in range(2):
            for half in range(2):
                ref = blk1(slot, col, me1[col], half)
                ref[...] = ref[...] + (f1[slot, col, 0, half] + f1[slot, col, 1, half])
        first(blk2, slot, me2, dev2, l2, f2, s_l2, r_l2, s_f2, r_f2)

    def stage_l2(q):
        second(blk2, lax.rem(q, SLOTS), me2, dev2, l2, f2, r_l2, s_f2, r_f2)

    def stage_f2(q):
        slot = lax.rem(q, SLOTS)
        drain(f2.at[slot], r_f2.at[slot])
        for col in range(2):
            for half in range(2):
                rows = pl.ds(32 * half, 32)
                val = blk2(slot, col, me2[col], half)[...] + (f2[slot, col, 0, half] + f2[slot, col, 1, half])
                for out, lo, hi in ((o_down, 0, 8), (o_up, 8, 16), (o_qkv, 16, 22)):
                    @pl.when((q >= lo) & (q < hi))
                    def _():
                        out[rows, pl.ds(pl.multiple_of((q - lo) * 256 + col * 128, 128), 128)] = val

                @pl.when(q >= 22)
                def _():
                    for k in range(2):
                        at = (q - 22) * 1024 + (2 * half + k) * 256 + col * 128
                        o_out[:, pl.ds(pl.multiple_of(at, 128), 128)] = val[16 * k:16 * k + 16, :]
        drain(l1.at[slot], s_l1.at[slot])
        drain(f1.at[slot], s_f1.at[slot])
        drain(l2.at[slot], s_l2.at[slot])
        drain(f2.at[slot], s_f2.at[slot])

        @pl.when(q < PIECES - SLOTS)
        def _():
            to = (partner, dev_y(ring(y, 1)), dev_y(ring(y, 3)), dev_z(ring(z, 1)), dev_z(ring(z, 3)))
            for i in range(5):
                pl.semaphore_signal(credit.at[i], inc=1, device_id=to[i], device_id_type=MESH)

    def ln_send(stage):
        me, dev, n = ((core, None, 2), (tp, dev_x, 4), (y, dev_y, 4), (z, dev_z, 4))[stage]
        for d in range(1, n):
            to = partner if dev is None else dev(ring(me, d))
            remote(lnb.at[stage, me], lnb.at[stage, me], ln_s.at[stage], ln_r.at[stage], to).start()

    def ln_sum(stage):
        n = 2 if stage == 0 else 4
        ref = lnb.at[stage, pl.ds(0, n - 1)]
        drain(ref, ln_r.at[stage])
        drain(ref, ln_s.at[stage])
        if n == 2:
            return lnb[0, 0] + lnb[0, 1]
        return (lnb[stage, 0] + lnb[stage, 1]) + (lnb[stage, 2] + lnb[stage, 3])

    def unrope(d, rows):
        d = d.astype(BF16).astype(F32)
        return (d * cos_ref[rows, :] - pltpu.roll(d, hd // 2, 1) * sin_ref[rows, :]).astype(BF16)

    def attend(h, side):
        hs = lax.rem(h, 2)

        def cols(j):
            return pl.ds(pl.multiple_of(h * 384 + j * 128, 128), 128)

        if side == 0:
            wait(load_head(h, hs))

            @pl.when(h < n_head - 1)
            def _():
                start(load_head(h + 1, 1 - hs))

            dctx_b[...] = dot_nt(dy_v[...], wo_t[hs]).astype(BF16)
            kt[...] = qkv_b[hs, :, hd:2 * hd].T
            vt[...] = qkv_b[hs, :, 2 * hd:3 * hd].T
            dk_s[...] = jnp.zeros_like(dk_s)
            dv_s[...] = jnp.zeros_like(dv_s)

        for i in ((0, 3), (1, 2))[side]:
            rows, lo, n = slice(i * blk, (i + 1) * blk), i * blk, (i + 1) * blk
            qi, dci = qkv_b[hs, rows, 0:hd], dctx_b[rows, :]
            kn, vn = qkv_b[hs, :n, hd:2 * hd], qkv_b[hs, :n, 2 * hd:3 * hd]
            s = dot_nt(kn, qi)
            seen = lax.broadcasted_iota(jnp.int32, (blk, blk), 0) <= lax.broadcasted_iota(jnp.int32, (blk, blk), 1)
            diag = jnp.where(seen, s[lo:, :], -1e30)
            s = jnp.concatenate([s[:lo, :], diag], axis=0) if lo else diag
            e = jnp.exp((s - jnp.max(s, axis=0, keepdims=True)) * scale)
            p = e * (1.0 / jnp.sum(e, axis=0, keepdims=True))
            pb = p.astype(BF16)
            ctxt[pl.ds(al(h, hd), hd), rows] = dot_nn(vt[:, :n], pb).astype(BF16)
            dp_ = dot_nt(vn, dci).astype(BF16).astype(F32)
            dsb = (p * (dp_ - jnp.sum(p * dp_, axis=0, keepdims=True)) * scale).astype(BF16)
            dproj_v[rows, cols(0)] = unrope(dot_nn(kt[:, :n], dsb).T, rows)
            dk_s[:n, :] = dk_s[:n, :] + dot_nn(dsb, qi)
            dv_s[:n, :] = dv_s[:n, :] + dot_nn(pb, dci)
        if side == 1:
            @pl.loop(0, 4)
            def _(m):
                at = pl.ds(al(m, blk), blk)
                dproj_v[at, cols(1)] = unrope(dk_s[at, :], at)
                dproj_v[at, cols(2)] = dv_s[at, :].astype(BF16)

    def down(k):
        ks = lax.rem(k, 2)
        wait(load_d(k, ks))

        @pl.when(k < 7)
        def _():
            start(load_d(k + 1, 1 - ks))

        d_gelu = dot_nt(dy_v[...], wu_t[ks]).astype(BF16).astype(F32)
        dh_v[:, pl.ds(al(k, 256), 256)] = (d_gelu * sl_buf[ks]).astype(BF16)

    def inputs(u):
        us = lax.rem(u, 2)
        cs = lax.rem(u, 5)
        wait(load_t(u, us))

        @pl.when(u < 7)
        def _():
            start(load_t(u + 1, 1 - us))

        at = pl.ds(al(u, 256), 256)
        gain_a, gain_m = ln_ref[0:1, at], ln_ref[2:3, at]
        sums = []
        for m in range(2):
            rows = slice(512 * m, 512 * m + 512)
            dha = dot_nt(dproj_v[rows, :], wq_t[us]).astype(BF16).astype(F32)
            dhm = dot_nt(dh_v[rows, :], wu_t[us]).astype(BF16).astype(F32)
            x_hat = (x_t[us, rows, :].astype(F32) - mean_ref[rows, :]) * rstd_ref[rows, :]
            c = (dha * gain_a + dhm * gain_m).astype(BF16)
            c_buf[cs, 2 * m] = c[:256]
            c_buf[cs, 2 * m + 1] = c[256:]
            sums.append([jnp.sum(v, axis=0, keepdims=True) for v in (dha * x_hat, dha, dhm * x_hat, dhm)])
        for i in range(4):
            lnb[0, core, i:i + 1, at] = sums[0][i] + sums[1][i]
        nxt, opp, prv = ring(tp, 1), ring(tp, 2), ring(tp, 3)
        remote(c_blk(u, opp, 0), cl1.at[u, 0], cs_l1.at[u], cr_l1.at[u], dev_x(nxt)).start()
        remote(c_blk(u, opp, 1), cl1.at[u, 1], cs_l1.at[u], cr_l1.at[u], dev_x(prv)).start()
        remote(c_blk(u, nxt, 1), cf1.at[u, 0, 1], cs_f1.at[u], cr_f1.at[u], dev_x(nxt)).start()
        remote(c_blk(u, prv, 0), cf1.at[u, 0, 0], cs_f1.at[u], cr_f1.at[u], dev_x(prv)).start()

    def c_blk(u, i, half):
        return c_buf.at[lax.rem(u, 5), i, pl.ds(128 * half, 128), :]

    def c_second(u):
        drain(cl1.at[u], cr_l1.at[u])
        for half, to in ((0, ring(tp, 1)), (1, ring(tp, 3))):
            ref = c_blk(u, to, half)
            ref[...] = (ref[...].astype(F32) + cl1[u, half].astype(F32)).astype(BF16)
            remote(ref, cf1.at[u, 1, half], cs_f1.at[u], cr_f1.at[u], dev_x(to)).start()

    def c_final(u):
        drain(cf1.at[u], cr_f1.at[u])
        for half in range(2):
            sl_buf[u // 4, pl.ds(pl.multiple_of(lax.rem(u, 4) * 256 + 128 * half, 128), 128), :] = c_blk(u, tp, half)[...].astype(F32) + (
                cf1[u, 0, half].astype(F32) + cf1[u, 1, half].astype(F32))
        drain(cl1.at[u], cs_l1.at[u])
        drain(cf1.at[u], cs_f1.at[u])

    def last():
        drain(x_t, g_sem)

        @pl.loop(0, 8)
        def _(r):
            def across(ref):
                return jnp.concatenate([ref[u // 4, pl.ds(pl.multiple_of(256 * (u % 4) + r * 32, 32), 32), :] for u in range(8)], axis=1).astype(F32)

            own = pl.ds(pl.multiple_of(tp * 256 + r * 32, 32), 32)
            rstd = rstd_ref[own, :]
            c = across(sl_buf)
            x_hat = (across(x_t) - mean_ref[own, :]) * rstd
            dx = rstd * (c - jnp.mean(c, axis=-1, keepdims=True) - x_hat * jnp.mean(c * x_hat, axis=-1, keepdims=True))
            o_gx[pl.ds(al(r, 32), 32), :] = (dy_v[own, :].astype(F32) + dx).astype(BF16)

    @pl.loop(0, STEPS)
    def _(p):
        @pl.when(p < PIECES)
        def _():
            compute(p)

        for lag, stage in ((7, stage_f2), (6, stage_l2), (5, stage_f1), (3, stage_l1), (1, stage_s)):
            @pl.when((p >= lag) & (p < PIECES + lag))
            def _():
                stage(p - lag)

        @pl.when((p >= 22) & (p < 30))
        def _():
            c_final(p - 22)

        @pl.when((p >= 20) & (p < 28))
        def _():
            c_second(p - 20)

        @pl.when(p < LATE)
        def _():
            slice_on(p)

        @pl.when(p < LATE - 2)
        def _():
            slice_own(p + 2)

        @pl.when((p >= 6) & (p < 14))
        def _():
            down(p - 6)

        for side, steps in enumerate(((7, 11, 14, 16), (9, 13, 15, 17))):
            @pl.when((p == steps[0]) | (p == steps[1]) | (p == steps[2]) | (p == steps[3]))
            def _():
                attend(sum((p >= at).astype(jnp.int32) for at in steps[1:]), side)

        @pl.when(p == 10)
        def _():
            for j in range(LATE):
                for i in range(6):
                    slice_copy(j, i).wait_send()

        @pl.when(p == 14)
        def _():
            start(load_t(0, 0))

        @pl.when((p >= 18) & (p < 26))
        def _():
            inputs(p - 18)

        @pl.when(p == 26)
        def _():
            start(load_x())
            ln_send(0)

        for stage, me in ((1, tp), (2, y), (3, z)):
            @pl.when(p == 26 + stage)
            def _():
                lnb[stage, me] = ln_sum(stage - 1)
                ln_send(stage)

        @pl.when(p == 30)
        def _():
            last()

        @pl.when(p == 30)
        def _():
            o_ln[...] = ln_sum(3)

    for p in (PIECES - 2, PIECES - 1):
        drain(p_buf.at[p % 2, :, :, :, 0], ds.at[p % SLOTS])


def back_call(get, hmt, hat, dy_early, slope, qkv, w_out, w_down, w2, w_up, x_full, x_loc, dy_loc, ln_params, mean, rstd, cos_f, sin_f):
    hbm = pl.BlockSpec(memory_space=pl.ANY)
    vmem = pl.BlockSpec(memory_space=pltpu.VMEM)
    dma = pltpu.SemaphoreType.DMA
    shape = jax.ShapeDtypeStruct
    k = (SLOTS,)
    return pl.pallas_call(
        back_kernel,
        in_specs=[hbm] * 13 + [vmem] * 5,
        out_specs=[vmem] * 6,
        out_shape=[shape((256, 2048), BF16), shape((4, 2048), F32), shape((64, 1536), F32), shape((16, 2048), F32),
                   shape((64, 2048), F32), shape((64, 2048), F32)],
        scratch_shapes=[
            pltpu.VMEM((2, 1024, 1024), BF16), pltpu.VMEM((2, 1024, 256), BF16),
            pltpu.VMEM((2, 2, 4, 4, 2, 64, 128), F32), pltpu.VMEM(k + (2, 4, 4, 64, 128), F32),
            pltpu.VMEM(k + (2, 2, 4, 32, 128), F32), pltpu.VMEM(k + (2, 2, 2, 4, 32, 128), F32),
            pltpu.VMEM(k + (2, 2, 32, 128), F32), pltpu.VMEM(k + (2, 2, 2, 32, 128), F32),
            pltpu.VMEM((4, 4, 4, 2048), F32),
            pltpu.VMEM((1024, 2048), BF16), pltpu.VMEM((1024, 1536), BF16), pltpu.VMEM((512, 1024), BF16),
            pltpu.VMEM((2, 1024, 384), BF16), pltpu.VMEM((1024, 128), BF16),
            pltpu.VMEM((1024, 128), F32), pltpu.VMEM((1024, 128), F32),
            pltpu.VMEM((2, 256, 1536), BF16), pltpu.VMEM((2, 256, 2048), BF16), pltpu.VMEM((2, 1024, 256), BF16),
            pltpu.VMEM((5, 4, 256, 256), BF16), pltpu.VMEM((8, 2, 128, 256), BF16), pltpu.VMEM((8, 2, 2, 128, 256), BF16),
            pltpu.VMEM((2, 1024, 256), F32), pltpu.VMEM((1024, 2048), BF16), pltpu.VMEM((2, 128, 2048), BF16),
            pltpu.VMEM((128, 1024), BF16), pltpu.VMEM((128, 1024), BF16),
            dma((2,)), dma((2,)), dma((2, 2)), dma((2, 3)), dma((2, 2)), dma, dma((LATE, 6)), dma((LATE, 6)),
            dma(k), dma(k), dma(k), dma(k), dma(k), dma(k), dma(k), dma(k), dma(k), dma(k),
            dma((4,)), dma((4,)), dma((8,)), dma((8,)), dma((8,)), dma((8,)),
            pltpu.SemaphoreType.REGULAR((5,)),
        ],
        compiler_params=pltpu.CompilerParams(collective_id=0, has_side_effects=True, vmem_limit_bytes=65400 * 1024),
        cost_estimate=pl.CostEstimate(flops=50_000_000_000, bytes_accessed=100_000_000, transcendentals=0),
        name='back',
    )(get, hmt, hat, dy_early, slope, qkv, w_out, w_down, w2, w_up, x_full, x_loc, dy_loc, ln_params, mean, rstd, cos_f, sin_f)


def place_kernel(gx, ln, qkv, out, up, down, o_gx, o_ln, o_qkv, o_out, o_up, o_down, b_gx, b_ln, b_qkv, b_out, b_up, b_down, b_rows, in_sem, out_sem):
    ins = [pltpu.make_async_copy(src, buf, in_sem.at[i]) for i, (src, buf) in enumerate(
        ((qkv, b_qkv), (gx, b_gx), (ln, b_ln), (out, b_out), (up, b_up), (down, b_down)))]
    outs = [pltpu.make_async_copy(buf, dst, out_sem.at[i]) for i, (buf, dst) in enumerate(
        ((b_rows, o_qkv), (b_gx, o_gx), (b_ln, o_ln), (b_out, o_out), (b_up, o_up), (b_down, o_down)))]
    for copy in ins:
        copy.start()
    for i in range(1, 6):
        ins[i].wait()
        outs[i].start()
    ins[0].wait()
    for g in range(4):
        for j in range(3):
            b_rows[:, j, g, :] = b_qkv[:, g * 384 + j * 128:g * 384 + j * 128 + 128]
    outs[0].start()
    for copy in outs:
        copy.wait()


def place_call(gx, ln, qkv, out, up, down):
    hbm = pl.BlockSpec(memory_space=pl.ANY)
    dma = pltpu.SemaphoreType.DMA
    arrays = (gx, ln, qkv, out, up, down)
    rows = (qkv.shape[0], 3, 4, 128)
    shapes = [jax.ShapeDtypeStruct(rows if v is qkv else v.shape, v.dtype) for v in arrays]
    return pl.pallas_call(
        place_kernel,
        in_specs=[hbm] * 6,
        out_specs=[hbm] * 6,
        out_shape=shapes,
        scratch_shapes=[pltpu.VMEM(v.shape, v.dtype) for v in arrays] + [pltpu.VMEM(rows, F32), dma((6,)), dma((6,))],
        compiler_params=pltpu.CompilerParams(vmem_limit_bytes=VMEM_LIMIT),
        name='place',
    )(*arrays)


def solution(mesh):
    def local_step(x_loc, dy_loc, ln_params, w_qkv, w_out, w_up, w_down):
        width, groups, slots, head_dim = w_qkv.shape
        cos_f, sin_f = (jnp.asarray(t) for t in rope_tables(4 * x_loc.shape[1], head_dim))
        w_rows = w_qkv.transpose(0, 2, 1, 3).reshape(width * slots * groups, head_dim)
        x_full, dy_early, hat, hmt, qkv, get, slope, w2, mean, rstd = front_call(x_loc[0], dy_loc[0], ln_params, cos_f, sin_f, w_rows, w_up)
        grad_x, g_ln, g_qkv, g_out, g_up, g_down = back_call(
            get, hmt, hat, dy_early, slope, qkv, w_out, w_down, w2, w_up, x_full, x_loc[0], dy_loc[0], ln_params, mean, rstd, cos_f, sin_f)
        grad_x, g_ln, g_qkv, g_out, g_up, g_down = place_call(grad_x, g_ln, g_qkv, g_out, g_up, g_down)
        return grad_x[None], g_ln, g_qkv.transpose(0, 2, 1, 3), g_out, g_up, g_down

    act_spec = P('dp', 'tp', None)
    in_specs = (act_spec, act_spec, P(None, None), P(None, 'tp', None, None), P('tp', None), P(None, 'tp'), P('tp', None))
    out_specs = (act_spec, P(None, None), P('dp', 'tp', None, None), P(('tp', 'dp'), None), P('dp', 'tp'), P(('tp', 'dp'), None))
    return jax.shard_map(local_step, mesh=mesh, in_specs=in_specs, out_specs=out_specs, check_vma=False)
```

```python
import functools

import jax
import jax.numpy as jnp
import numpy as np
from jax import lax
from jax.experimental import pallas as pl
from jax.experimental.pallas import tpu as pltpu
from jax.sharding import PartitionSpec as P

NORM_EPS = 1e-5
ROPE_BASE = 10000.0
MESH = pl.DeviceIdType.MESH
PIECES = 24
SLOTS = 8
STEPS = PIECES + 7
EARLY = 512
LATE = 6
VMEM_LIMIT = 60000 * 1024
F32 = jnp.float32
BF16 = jnp.bfloat16


def rope_tables(seq_len, head_dim):
    half_dim = head_dim // 2
    inv_freq = np.float32(ROPE_BASE) ** (np.float32(-2.0) * np.arange(half_dim, dtype=np.float32) / np.float32(head_dim))
    angles = np.arange(seq_len, dtype=np.float32)[:, None] * inv_freq[None, :].astype(np.float32)
    cos_t, sin_t = np.cos(angles), np.sin(angles)
    return np.concatenate([cos_t, cos_t], axis=1), np.concatenate([-sin_t, sin_t], axis=1)


def dot_nn(lhs, rhs):
    return lax.dot_general(lhs, rhs, (((1,), (0,)), ((), ())), preferred_element_type=F32)


def dot_nt(lhs, rhs):
    return lax.dot_general(lhs, rhs, (((1,), (1,)), ((), ())), preferred_element_type=F32)


def dot_tt(lhs, rhs):
    return lax.dot_general(lhs, rhs, (((0,), (0,)), ((), ())), preferred_element_type=F32)


def front_kernel(x_ref, dy_ref, ln_ref, cos_ref, sin_ref, wq_ref, wu_ref,
                 o_x, o_dy, o_ha, o_hm, o_qkv, o_gelu, o_slope, o_w, mean_ref, rstd_ref,
                 x_v, dy_v, w2, wu, wq_b, wq_f, slope, ha, hm, hat, hmt, get, qkv,
                 xs, xr, ds, dr, in_sem, wq_sem, out_sem, fin_sem):
    tp = lax.axis_index('tp')
    nxt, opp, prv = lax.rem(tp + 1, 4), lax.rem(tp + 2, 4), lax.rem(tp + 3, 4)
    d_model = x_ref.shape[1]
    rows = x_ref.shape[0]
    half = rows // 2
    part = wq_b.shape[1]
    barrier = pltpu.get_barrier_semaphore()
    for peer in (nxt, prv):
        pl.semaphore_signal(barrier, inc=1, device_id={'tp': peer}, device_id_type=MESH)

    def wq_copy(i):
        return pltpu.make_async_copy(wq_ref.at[pl.ds(i * part, part)], wq_b.at[i % 2], wq_sem.at[i % 2])

    dy_own = dy_ref.at[:, pl.ds(0, EARLY)]
    loads = [pltpu.make_async_copy(x_ref, x_v.at[tp], in_sem.at[0]), pltpu.make_async_copy(dy_own, dy_v.at[tp], in_sem.at[1]),
             pltpu.make_async_copy(wu_ref, wu, in_sem.at[2])]
    wq_copy(0).start()
    loads[0].start()
    wq_copy(1).start()
    loads[2].start()
    loads[1].start()
    pl.semaphore_wait(barrier, 2)

    A, B = pl.ds(0, half), pl.ds(half, half)

    def moves(src, buf, ssem, rsem):
        def one(i, ref, slot, piece, to):
            return pltpu.make_async_remote_copy(src_ref=ref, dst_ref=buf.at[slot, piece], send_sem=ssem.at[i], recv_sem=rsem.at[i],
                                                device_id={'tp': to}, device_id_type=MESH)
        return [one(0, src.at[A], tp, A, nxt), one(1, src.at[B], tp, B, prv), one(2, src.at[B], tp, B, nxt), one(3, src.at[A], tp, A, prv),
                one(4, buf.at[prv, A], prv, A, nxt), one(5, buf.at[nxt, B], nxt, B, prv)]

    xm = moves(x_ref, x_v, xs, xr)
    dm = moves(dy_own, dy_v, ds, dr)
    for i in range(4):
        xm[i].start()

    per = part // 12
    for i in range(wq_ref.shape[0] // part):
        wq_copy(i).wait()

        @pl.loop(0, part // 256)
        def _(r):
            at = pl.ds(pl.multiple_of(r * 256, 256), 256)
            wq_f[at, :] = wq_b[i % 2, at, :].astype(F32)

        if i + 2 < wq_ref.shape[0] // part:
            wq_copy(i + 2).start()
        for j in range(3):
            for g in range(4):
                w2[i * per:(i + 1) * per, g * 384 + j * 128:g * 384 + j * 128 + 128] = wq_f[pl.ds(j * 4 + g, per, stride=12), :].astype(BF16)
    w_out_copy = pltpu.make_async_copy(w2, o_w, fin_sem.at[8])
    w_out_copy.start()

    outs = {}

    def tokens(block, i):
        slot, side = block[i]
        return pl.ds(pl.multiple_of(slot * rows + side * half, half), half)

    def put(kind, n, buf, ref, block):
        for i in range(2):
            copy = pltpu.make_async_copy(buf.at[n % 2, pl.ds(i * half, half)], ref.at[tokens(block, i)], out_sem.at[kind, n % 2, i])
            copy.start()
            outs[kind, n % 2, i] = copy

    def put_t(kind, buf, ref, block):
        for i in range(2):
            copy = pltpu.make_async_copy(buf.at[:, pl.ds(i * half, half)], ref.at[:, tokens(block, i)], out_sem.at[kind, 0, i])
            copy.start()
            outs[kind, 0, i] = copy

    def free(kind, n):
        for i in range(2):
            if (kind, n % 2, i) in outs:
                outs.pop((kind, n % 2, i)).wait()

    def forward(block, n):
        s = n % 2
        for i in range(2):
            slot, side = block[i]

            @pl.loop(0, half // 32)
            def _(r):
                src = pl.ds(pl.multiple_of(side * half + r * 32, 32), 32)
                at = pl.ds(pl.multiple_of(i * half + r * 32, 32), 32)
                to = pl.ds(pl.multiple_of(slot * rows + side * half + r * 32, 32), 32)
                xf = x_v[slot, src, :].astype(F32)
                mean = jnp.mean(xf, axis=-1, keepdims=True)
                cen = xf - mean
                rstd = lax.rsqrt(jnp.mean(cen * cen, axis=-1, keepdims=True) + NORM_EPS)
                mean_ref[to, :] = mean
                rstd_ref[to, :] = rstd
                x_hat = cen * rstd
                ha[at, :] = (x_hat * ln_ref[0:1, :] + ln_ref[1:2, :]).astype(BF16)
                hm[at, :] = (x_hat * ln_ref[2:3, :] + ln_ref[3:4, :]).astype(BF16)

        for kind in (0, 1, 3):
            free(kind, 0)
        free(2, n)
        free(4, n)

        @pl.loop(0, d_model // 256)
        def _(c):
            cols = pl.ds(pl.multiple_of(c * 256, 256), 256)
            hat[cols, :] = ha[:, cols].T
            hmt[cols, :] = hm[:, cols].T

        put_t(0, hat, o_ha, block)
        put_t(1, hmt, o_hm, block)
        cos_t, sin_t = (jnp.concatenate([ref[tokens(block, 0), :], ref[tokens(block, 1), :]], axis=0) for ref in (cos_ref, sin_ref))

        @pl.loop(0, 4)
        def _(g):
            cols = pl.ds(pl.multiple_of(g * 384, 128), 384)
            t = dot_nn(ha[...], w2[:, cols]).astype(BF16)
            for j in range(2):
                v = t[:, j * 128:j * 128 + 128].astype(F32)
                qkv[s, :, pl.ds(pl.multiple_of(g * 384 + j * 128, 128), 128)] = (v * cos_t + pltpu.roll(v, 64, 1) * sin_t).astype(BF16)
            qkv[s, :, pl.ds(pl.multiple_of(g * 384 + 256, 128), 128)] = t[:, 256:384]

        put(2, n, qkv, o_qkv, block)

        @pl.loop(0, 4)
        def _(c):
            cols = pl.ds(pl.multiple_of(c * 512, 512), 512)
            u = dot_nn(hm[...], wu[:, cols]).astype(BF16).astype(F32)
            cdf = 0.5 * (1.0 + lax.erf(u * (0.5 ** 0.5)))
            get[cols, :] = (u * cdf).astype(BF16).T
            slope[s, :, cols] = cdf + u * (jnp.exp(-0.5 * u * u) * ((2.0 * jnp.pi) ** -0.5))

        put_t(3, get, o_gelu, block)
        put(4, n, slope, o_slope, block)

    fins = []

    def keep(buf, ref, slot, i):
        copy = pltpu.make_async_copy(buf.at[slot], ref.at[pl.ds(pl.multiple_of(slot * rows, rows), rows)], fin_sem.at[i])
        copy.start()
        fins.append(copy)

    loads[0].wait()
    loads[2].wait()
    keep(x_v, o_x, tp, 0)
    forward(((tp, 0), (tp, 1)), 0)
    xm[0].wait_recv()
    xm[4].start()
    xm[1].wait_recv()
    xm[5].start()
    for i in range(4):
        dm[i].start()
    forward(((prv, 0), (nxt, 1)), 1)
    xm[2].wait_recv()
    xm[3].wait_recv()
    keep(x_v, o_x, prv, 1)
    keep(x_v, o_x, nxt, 2)
    forward(((prv, 1), (nxt, 0)), 2)
    dm[0].wait_recv()
    dm[4].start()
    dm[1].wait_recv()
    dm[5].start()
    xm[4].wait_recv()
    xm[5].wait_recv()
    keep(x_v, o_x, opp, 3)
    forward(((opp, 0), (opp, 1)), 3)
    loads[1].wait()
    for i in range(2, 6):
        dm[i].wait_recv()
    for i, slot in enumerate((tp, prv, nxt, opp)):
        keep(dy_v, o_dy, slot, 4 + i)
    for m in xm + dm:
        m.wait_send()
    for copy in list(outs.values()) + fins + [w_out_copy]:
        copy.wait()


def front_call(x_loc, dy_loc, ln_params, cos_f, sin_f, w_rows, w_up):
    r, d = x_loc.shape
    t, f, n = 4 * r, w_up.shape[1], w_rows.shape[0] * 128 // d
    part = w_rows.shape[0] // 4
    hbm = pl.BlockSpec(memory_space=pl.ANY)
    vmem = pl.BlockSpec(memory_space=pltpu.VMEM)
    dma = pltpu.SemaphoreType.DMA
    shape = jax.ShapeDtypeStruct
    return pl.pallas_call(
        front_kernel,
        in_specs=[hbm, hbm, vmem, vmem, vmem, hbm, hbm],
        out_specs=[hbm] * 8 + [vmem] * 2,
        out_shape=[shape((t, d), BF16), shape((t, EARLY), BF16), shape((d, t), BF16), shape((d, t), BF16),
                   shape((t, n), BF16), shape((f, t), BF16), shape((t, f), F32), shape((d, n), BF16),
                   shape((t, 1), F32), shape((t, 1), F32)],
        scratch_shapes=[
            pltpu.VMEM((4, r, d), BF16), pltpu.VMEM((4, r, EARLY), BF16),
            pltpu.VMEM((d, n), BF16), pltpu.VMEM((d, f), BF16),
            pltpu.VMEM((2, part, 128), BF16), pltpu.VMEM((part, 128), F32),
            pltpu.VMEM((2, r, f), F32),
            pltpu.VMEM((r, d), BF16), pltpu.VMEM((r, d), BF16),
            pltpu.VMEM((d, r), BF16), pltpu.VMEM((d, r), BF16), pltpu.VMEM((f, r), BF16),
            pltpu.VMEM((2, r, n), BF16),
            dma((6,)), dma((6,)), dma((6,)), dma((6,)), dma((3,)), dma((2,)), dma((5, 2, 2)), dma((9,)),
        ],
        compiler_params=pltpu.CompilerParams(collective_id=1, has_side_effects=True, vmem_limit_bytes=64000 * 1024),
        cost_estimate=pl.CostEstimate(flops=2 * t * d * (n + f), bytes_accessed=70_000_000, transcendentals=2 * t * f),
        name='front',
    )(x_loc, dy_loc, ln_params, cos_f, sin_f, w_rows, w_up)


def back_kernel(get_ref, hmt_ref, hat_ref, dyp_ref, slope_ref, qkv_ref, wo_ref, wd_ref, w2_ref, wup_ref, x_ref, xloc_ref, dyloc_ref,
                ln_ref, mean_ref, rstd_ref, cos_ref, sin_ref,
                o_gx, o_ln, o_qkv, o_out, o_up, o_down,
                a_buf, b_buf, p_buf, d_buf, l1, f1, l2, f2, lnb, dh_v, dproj_v, ctxt, qkv_b, dctx_b, dk_s, dv_s,
                wq_t, wu_t, x_t, c_buf, cl1, cf1, sl_buf, dy_v, wo_t, kt, vt,
                a_sem, dy_sem, h_sem, t_sem, d_sem, g_sem, gs, gr, ds, dr, s_l1, r_l1, s_f1, r_f1, s_l2, r_l2, s_f2, r_f2, ln_s, ln_r,
                cs_l1, cr_l1, cs_f1, cr_f1, credit):
    tp = lax.axis_index('tp')
    dp = lax.axis_index('dp')
    core = lax.rem(dp, 2)
    y = lax.rem(dp // 2, 4)
    z = dp // 8
    partner = {'dp': dp + 1 - 2 * core}
    n_head = 4
    hd = 128
    blk = 256
    scale = hd ** -0.5

    def dev_y(i):
        return {'dp': z * 8 + i * 2 + core}

    def dev_z(i):
        return {'dp': i * 8 + y * 2 + core}

    def dev_x(i):
        return {'tp': i}

    def ring(i, d):
        return lax.rem(i + d, 4)

    def al(i, m):
        return pl.multiple_of(i * m, m)

    barrier = pltpu.get_barrier_semaphore()
    peers = [partner]
    for d in (1, 2, 3):
        peers += [dev_x(ring(tp, d)), dev_y(ring(y, d)), dev_z(ring(z, d))]
    for peer in peers:
        pl.semaphore_signal(barrier, inc=1, device_id=peer, device_id_type=MESH)

    def load_a(src, h):
        return pltpu.make_async_copy(src.at[pl.ds(al(h, 1024), 1024)], a_buf.at[h], a_sem.at[h])

    def load_x():
        return [pltpu.make_async_copy(xloc_ref.at[:, pl.ds(256 * u, 256)], x_t.at[u // 4, pl.ds(256 * (u % 4), 256)], g_sem) for u in range(8)]

    def load_head(h, slot):
        return [pltpu.make_async_copy(qkv_ref.at[:, pl.ds(pl.multiple_of(h * 384, 128), 384)], qkv_b.at[slot], h_sem.at[slot, 0]),
                pltpu.make_async_copy(wo_ref.at[pl.ds(al(h, 128), 128)], wo_t.at[slot], h_sem.at[slot, 1])]

    def load_d(k, slot):
        at = pl.ds(al(k, 256), 256)
        return [pltpu.make_async_copy(wd_ref.at[at], wu_t.at[slot], d_sem.at[slot, 0]),
                pltpu.make_async_copy(slope_ref.at[:, at], sl_buf.at[slot], d_sem.at[slot, 1])]

    def load_t(u, slot):
        at = pl.ds(al(u, 256), 256)
        return [pltpu.make_async_copy(w2_ref.at[at], wq_t.at[slot], t_sem.at[slot, 0]),
                pltpu.make_async_copy(wup_ref.at[at], wu_t.at[slot], t_sem.at[slot, 1]),
                pltpu.make_async_copy(x_ref.at[:, at], x_t.at[slot], t_sem.at[slot, 2])]

    def start(copies):
        for copy in copies:
            copy.start()

    def wait(copies):
        for copy in copies:
            copy.wait()

    for h in range(2):
        load_a(get_ref, jnp.int32(h)).start()
    early = pltpu.make_async_copy(dyp_ref, dy_v.at[:, pl.ds(0, EARLY)], dy_sem.at[0])
    early.start()
    late = pltpu.make_async_copy(dyloc_ref.at[:, pl.ds(EARLY, 256 * LATE)],
                                 dy_v.at[pl.ds(al(tp, 256), 256), pl.ds(EARLY, 256 * LATE)], dy_sem.at[1])
    late.start()
    start(load_head(jnp.int32(0), 0))
    start(load_d(jnp.int32(0), 0))
    pl.semaphore_wait(barrier, len(peers))

    def remote(src, dst, ssem, rsem, device):
        return pltpu.make_async_remote_copy(src_ref=src, dst_ref=dst, send_sem=ssem, recv_sem=rsem, device_id=device, device_id_type=MESH)

    def drain(ref, sem):
        pltpu.make_async_copy(ref, ref, sem).wait()

    def slice_copy(j, i):
        cols = pl.ds(pl.multiple_of(EARLY + j * 256, 256), 256)
        nxt, prv = ring(tp, 1), ring(tp, 3)
        owner, half, to = ((tp, 0, nxt), (tp, 1, prv), (tp, 1, nxt), (tp, 0, prv), (prv, 0, nxt), (nxt, 1, prv))[i]
        spot = dy_v.at[pl.ds(pl.multiple_of(owner * 256 + half * 128, 128), 128), cols]
        src = dyloc_ref.at[pl.ds(128 * half, 128), cols] if i < 4 else spot
        return remote(src, spot, gs.at[j, i], gr.at[j, i], dev_x(to))

    def slice_own(j):
        for i in range(4):
            slice_copy(j, i).start()

    def slice_on(j):
        for i in range(2):
            slice_copy(j, i).wait_recv()
            slice_copy(j, 4 + i).start()

    def slice_done(j):
        for i in range(2, 6):
            slice_copy(j, i).wait_recv()

    slice_own(jnp.int32(0))
    slice_own(jnp.int32(1))

    def pair_copy(p):
        slot = lax.rem(p, SLOTS)
        return remote(p_buf.at[lax.rem(p, 2), :, :, :, 1 - core], d_buf.at[slot], ds.at[slot], dr.at[slot], partner)

    def blk1(slot, col, i, half):
        rows = pl.ds(32 * half, 32)
        if col == 0:
            return d_buf.at[slot, 0, :, i, rows, :]
        return d_buf.at[slot, 1, i, :, rows, :]

    def blk2(slot, col, i, half):
        rows = pl.ds(32 * half, 32)
        if col == 0:
            return d_buf.at[slot, 0, i, y, rows, :]
        return d_buf.at[slot, 1, z, i, rows, :]

    me1 = (y, z)
    dev1 = (dev_y, dev_z)
    me2 = (z, y)
    dev2 = (dev_z, dev_y)

    def compute(p):
        ps = lax.rem(p, 2)

        @pl.when(p >= 2)
        def _():
            drain(p_buf.at[ps, :, :, :, 0], ds.at[lax.rem(p - 2, SLOTS)])

        @pl.when(p == 0)
        def _():
            early.wait()

        @pl.when(p == 2)
        def _():
            late.wait()

        @pl.when((p >= 2) & (p < 8))
        def _():
            slice_done(p - 2)

        @pl.when(p < 8)
        def _():
            b_buf[ps] = dy_v[:, pl.ds(al(p, 256), 256)]

        @pl.when((p >= 8) & (p < 16))
        def _():
            b_buf[ps] = dh_v[:, pl.ds(al(p - 8, 256), 256)]

        @pl.when((p >= 16) & (p < 22))
        def _():
            b_buf[ps] = dproj_v[:, pl.ds(al(p - 16, 256), 256)]

        @pl.when(p < 22)
        def _():
            @pl.loop(0, 2)
            def _(h):
                @pl.when((p == 0) | (p == 8) | (p == 16))
                def _():
                    load_a(get_ref, h).wait()

                tile = dot_nn(a_buf[h], b_buf[ps])
                for i in range(16):
                    for col in range(2):
                        p_buf[ps, col, 2 * h + i // 8, (i // 2) % 4, i % 2] = tile[64 * i:64 * i + 64, 128 * col:128 * col + 128]

                @pl.when(p == 7)
                def _():
                    load_a(hmt_ref, h).start()

                @pl.when(p == 15)
                def _():
                    load_a(hat_ref, h).start()

        @pl.when(p >= 22)
        def _():
            @pl.loop(0, 4)
            def _(k):
                tile = dot_nn(ctxt[...], dy_v[:, pl.ds(pl.multiple_of((p - 22) * 1024 + k * 256, 256), 256)])
                for i in range(32):
                    for col in range(2):
                        p_buf[ps, col, i // 8, (i // 2) % 4, i % 2, pl.ds(al(k, 16), 16), :] = tile[16 * i:16 * i + 16, 128 * col:128 * col + 128]

        @pl.when(p >= SLOTS)
        def _():
            pl.semaphore_wait(credit.at[0], 1)

        pair_copy(p).start()

    def first(blk, slot, me, dev, lands, finals, s_a, r_a, s_b, r_b):
        for col in range(2):
            nxt, opp, prv = ring(me[col], 1), ring(me[col], 2), ring(me[col], 3)
            remote(blk(slot, col, opp, 0), lands.at[slot, col, 0], s_a.at[slot], r_a.at[slot], dev[col](nxt)).start()
            remote(blk(slot, col, opp, 1), lands.at[slot, col, 1], s_a.at[slot], r_a.at[slot], dev[col](prv)).start()
        for col in range(2):
            nxt, prv = ring(me[col], 1), ring(me[col], 3)
            remote(blk(slot, col, nxt, 1), finals.at[slot, col, 0, 1], s_b.at[slot], r_b.at[slot], dev[col](nxt)).start()
            remote(blk(slot, col, prv, 0), finals.at[slot, col, 0, 0], s_b.at[slot], r_b.at[slot], dev[col](prv)).start()

    def second(blk, slot, me, dev, lands, finals, r_a, s_b, r_b):
        drain(lands.at[slot], r_a.at[slot])
        for col in range(2):
            nxt, prv = ring(me[col], 1), ring(me[col], 3)
            for half, to in ((0, nxt), (1, prv)):
                ref = blk(slot, col, to, half)
                ref[...] = ref[...] + lands[slot, col, half]
                remote(ref, finals.at[slot, col, 1, half], s_b.at[slot], r_b.at[slot], dev[col](to)).start()

    def stage_s(q):
        slot = lax.rem(q, SLOTS)
        ps = lax.rem(q, 2)
        drain(d_buf.at[slot], dr.at[slot])

        @pl.loop(0, 8)
        def _(i):
            col, zi = i // 4, lax.rem(i, 4)
            d_buf[slot, col, zi] = d_buf[slot, col, zi] + p_buf[ps, col, zi, :, core]

        @pl.when(q >= SLOTS)
        def _():
            for i in range(1, 5):
                pl.semaphore_wait(credit.at[i], 1)

        first(blk1, slot, me1, dev1, l1, f1, s_l1, r_l1, s_f1, r_f1)

    def stage_l1(q):
        second(blk1, lax.rem(q, SLOTS), me1, dev1, l1, f1, r_l1, s_f1, r_f1)

    def stage_f1(q):
        slot = lax.rem(q, SLOTS)
        drain(f1.at[slot], r_f1.at[slot])
        for col in range(2):
            for half in range(2):
                ref = blk1(slot, col, me1[col], half)
                ref[...] = ref[...] + (f1[slot, col, 0, half] + f1[slot, col, 1, half])
        first(blk2, slot, me2, dev2, l2, f2, s_l2, r_l2, s_f2, r_f2)

    def stage_l2(q):
        second(blk2, lax.rem(q, SLOTS), me2, dev2, l2, f2, r_l2, s_f2, r_f2)

    def stage_f2(q):
        slot = lax.rem(q, SLOTS)
        drain(f2.at[slot], r_f2.at[slot])
        for col in range(2):
            for half in range(2):
                rows = pl.ds(32 * half, 32)
                val = blk2(slot, col, me2[col], half)[...] + (f2[slot, col, 0, half] + f2[slot, col, 1, half])
                for out, lo, hi in ((o_down, 0, 8), (o_up, 8, 16), (o_qkv, 16, 22)):
                    @pl.when((q >= lo) & (q < hi))
                    def _():
                        out[rows, pl.ds(pl.multiple_of((q - lo) * 256 + col * 128, 128), 128)] = val

                @pl.when(q >= 22)
                def _():
                    for k in range(2):
                        at = (q - 22) * 1024 + (2 * half + k) * 256 + col * 128
                        o_out[:, pl.ds(pl.multiple_of(at, 128), 128)] = val[16 * k:16 * k + 16, :]
        drain(l1.at[slot], s_l1.at[slot])
        drain(f1.at[slot], s_f1.at[slot])
        drain(l2.at[slot], s_l2.at[slot])
        drain(f2.at[slot], s_f2.at[slot])

        @pl.when(q < PIECES - SLOTS)
        def _():
            to = (partner, dev_y(ring(y, 1)), dev_y(ring(y, 3)), dev_z(ring(z, 1)), dev_z(ring(z, 3)))
            for i in range(5):
                pl.semaphore_signal(credit.at[i], inc=1, device_id=to[i], device_id_type=MESH)

    def ln_send(stage):
        me, dev, n = ((core, None, 2), (tp, dev_x, 4), (y, dev_y, 4), (z, dev_z, 4))[stage]
        for d in range(1, n):
            to = partner if dev is None else dev(ring(me, d))
            remote(lnb.at[stage, me], lnb.at[stage, me], ln_s.at[stage], ln_r.at[stage], to).start()

    def ln_sum(stage):
        n = 2 if stage == 0 else 4
        ref = lnb.at[stage, pl.ds(0, n - 1)]
        drain(ref, ln_r.at[stage])
        drain(ref, ln_s.at[stage])
        if n == 2:
            return lnb[0, 0] + lnb[0, 1]
        return (lnb[stage, 0] + lnb[stage, 1]) + (lnb[stage, 2] + lnb[stage, 3])

    def unrope(d, rows):
        d = d.astype(BF16).astype(F32)
        return (d * cos_ref[rows, :] - pltpu.roll(d, hd // 2, 1) * sin_ref[rows, :]).astype(BF16)

    def attend(h, side):
        hs = lax.rem(h, 2)

        def cols(j):
            return pl.ds(pl.multiple_of(h * 384 + j * 128, 128), 128)

        if side == 0:
            wait(load_head(h, hs))

            @pl.when(h < n_head - 1)
            def _():
                start(load_head(h + 1, 1 - hs))

            dctx_b[...] = dot_nt(dy_v[...], wo_t[hs]).astype(BF16)
            kt[...] = qkv_b[hs, :, hd:2 * hd].T
            vt[...] = qkv_b[hs, :, 2 * hd:3 * hd].T
            dk_s[...] = jnp.zeros_like(dk_s)
            dv_s[...] = jnp.zeros_like(dv_s)

        for i in ((0, 3), (1, 2))[side]:
            rows, lo, n = slice(i * blk, (i + 1) * blk), i * blk, (i + 1) * blk
            qi, dci = qkv_b[hs, rows, 0:hd], dctx_b[rows, :]
            kn, vn = qkv_b[hs, :n, hd:2 * hd], qkv_b[hs, :n, 2 * hd:3 * hd]
            s = dot_nt(kn, qi)
            seen = lax.broadcasted_iota(jnp.int32, (blk, blk), 0) <= lax.broadcasted_iota(jnp.int32, (blk, blk), 1)
            diag = jnp.where(seen, s[lo:, :], -1e30)
            s = jnp.concatenate([s[:lo, :], diag], axis=0) if lo else diag
            e = jnp.exp((s - jnp.max(s, axis=0, keepdims=True)) * scale)
            p = e * (1.0 / jnp.sum(e, axis=0, keepdims=True))
            pb = p.astype(BF16)
            ctxt[pl.ds(al(h, hd), hd), rows] = dot_nn(vt[:, :n], pb).astype(BF16)
            dp_ = dot_nt(vn, dci).astype(BF16).astype(F32)
            dsb = (p * (dp_ - jnp.sum(p * dp_, axis=0, keepdims=True)) * scale).astype(BF16)
            dproj_v[rows, cols(0)] = unrope(dot_nn(kt[:, :n], dsb).T, rows)
            dk_s[:n, :] = dk_s[:n, :] + dot_nn(dsb, qi)
            dv_s[:n, :] = dv_s[:n, :] + dot_nn(pb, dci)
        if side == 1:
            @pl.loop(0, 4)
            def _(m):
                at = pl.ds(al(m, blk), blk)
                dproj_v[at, cols(1)] = unrope(dk_s[at, :], at)
                dproj_v[at, cols(2)] = dv_s[at, :].astype(BF16)

    def down(k):
        ks = lax.rem(k, 2)
        wait(load_d(k, ks))

        @pl.when(k < 7)
        def _():
            start(load_d(k + 1, 1 - ks))

        d_gelu = dot_nt(dy_v[...], wu_t[ks]).astype(BF16).astype(F32)
        dh_v[:, pl.ds(al(k, 256), 256)] = (d_gelu * sl_buf[ks]).astype(BF16)

    def inputs(u):
        us = lax.rem(u, 2)
        cs = lax.rem(u, 5)
        wait(load_t(u, us))

        @pl.when(u < 7)
        def _():
            start(load_t(u + 1, 1 - us))

        at = pl.ds(al(u, 256), 256)
        gain_a, gain_m = ln_ref[0:1, at], ln_ref[2:3, at]
        sums = []
        for m in range(2):
            rows = slice(512 * m, 512 * m + 512)
            dha = dot_nt(dproj_v[rows, :], wq_t[us]).astype(BF16).astype(F32)
            dhm = dot_nt(dh_v[rows, :], wu_t[us]).astype(BF16).astype(F32)
            x_hat = (x_t[us, rows, :].astype(F32) - mean_ref[rows, :]) * rstd_ref[rows, :]
            c = (dha * gain_a + dhm * gain_m).astype(BF16)
            c_buf[cs, 2 * m] = c[:256]
            c_buf[cs, 2 * m + 1] = c[256:]
            sums.append([jnp.sum(v, axis=0, keepdims=True) for v in (dha * x_hat, dha, dhm * x_hat, dhm)])
        for i in range(4):
            lnb[0, core, i:i + 1, at] = sums[0][i] + sums[1][i]
        nxt, opp, prv = ring(tp, 1), ring(tp, 2), ring(tp, 3)
        remote(c_blk(u, opp, 0), cl1.at[u, 0], cs_l1.at[u], cr_l1.at[u], dev_x(nxt)).start()
        remote(c_blk(u, opp, 1), cl1.at[u, 1], cs_l1.at[u], cr_l1.at[u], dev_x(prv)).start()
        remote(c_blk(u, nxt, 1), cf1.at[u, 0, 1], cs_f1.at[u], cr_f1.at[u], dev_x(nxt)).start()
        remote(c_blk(u, prv, 0), cf1.at[u, 0, 0], cs_f1.at[u], cr_f1.at[u], dev_x(prv)).start()

    def c_blk(u, i, half):
        return c_buf.at[lax.rem(u, 5), i, pl.ds(128 * half, 128), :]

    def c_second(u):
        drain(cl1.at[u], cr_l1.at[u])
        for half, to in ((0, ring(tp, 1)), (1, ring(tp, 3))):
            ref = c_blk(u, to, half)
            ref[...] = (ref[...].astype(F32) + cl1[u, half].astype(F32)).astype(BF16)
            remote(ref, cf1.at[u, 1, half], cs_f1.at[u], cr_f1.at[u], dev_x(to)).start()

    def c_final(u):
        drain(cf1.at[u], cr_f1.at[u])
        for half in range(2):
            sl_buf[u // 4, pl.ds(pl.multiple_of(lax.rem(u, 4) * 256 + 128 * half, 128), 128), :] = c_blk(u, tp, half)[...].astype(F32) + (
                cf1[u, 0, half].astype(F32) + cf1[u, 1, half].astype(F32))
        drain(cl1.at[u], cs_l1.at[u])
        drain(cf1.at[u], cs_f1.at[u])

    def last():
        drain(x_t, g_sem)

        @pl.loop(0, 8)
        def _(r):
            def across(ref):
                return jnp.concatenate([ref[u // 4, pl.ds(pl.multiple_of(256 * (u % 4) + r * 32, 32), 32), :] for u in range(8)], axis=1).astype(F32)

            own = pl.ds(pl.multiple_of(tp * 256 + r * 32, 32), 32)
            rstd = rstd_ref[own, :]
            c = across(sl_buf)
            x_hat = (across(x_t) - mean_ref[own, :]) * rstd
            dx = rstd * (c - jnp.mean(c, axis=-1, keepdims=True) - x_hat * jnp.mean(c * x_hat, axis=-1, keepdims=True))
            o_gx[pl.ds(al(r, 32), 32), :] = (dy_v[own, :].astype(F32) + dx).astype(BF16)

    @pl.loop(0, STEPS)
    def _(p):
        @pl.when(p < PIECES)
        def _():
            compute(p)

        for lag, stage in ((7, stage_f2), (6, stage_l2), (5, stage_f1), (3, stage_l1), (1, stage_s)):
            @pl.when((p >= lag) & (p < PIECES + lag))
            def _():
                stage(p - lag)

        @pl.when((p >= 22) & (p < 30))
        def _():
            c_final(p - 22)

        @pl.when((p >= 20) & (p < 28))
        def _():
            c_second(p - 20)

        @pl.when(p < LATE)
        def _():
            slice_on(p)

        @pl.when(p < LATE - 2)
        def _():
            slice_own(p + 2)

        @pl.when((p >= 7) & (p < 15))
        def _():
            down(p - 7)

        for side, steps in enumerate(((7, 11, 14, 16), (9, 13, 15, 17))):
            @pl.when((p == steps[0]) | (p == steps[1]) | (p == steps[2]) | (p == steps[3]))
            def _():
                attend(sum((p >= at).astype(jnp.int32) for at in steps[1:]), side)

        @pl.when(p == 10)
        def _():
            for j in range(LATE):
                for i in range(6):
                    slice_copy(j, i).wait_send()

        @pl.when(p == 14)
        def _():
            start(load_t(0, 0))

        @pl.when((p >= 18) & (p < 26))
        def _():
            inputs(p - 18)

        @pl.when(p == 26)
        def _():
            start(load_x())
            ln_send(0)

        for stage, me in ((1, tp), (2, y), (3, z)):
            @pl.when(p == 26 + stage)
            def _():
                lnb[stage, me] = ln_sum(stage - 1)
                ln_send(stage)

        @pl.when(p == 30)
        def _():
            last()

        @pl.when(p == 30)
        def _():
            o_ln[...] = ln_sum(3)

    for p in (PIECES - 2, PIECES - 1):
        drain(p_buf.at[p % 2, :, :, :, 0], ds.at[p % SLOTS])


def back_call(get, hmt, hat, dy_early, slope, qkv, w_out, w_down, w2, w_up, x_full, x_loc, dy_loc, ln_params, mean, rstd, cos_f, sin_f):
    hbm = pl.BlockSpec(memory_space=pl.ANY)
    vmem = pl.BlockSpec(memory_space=pltpu.VMEM)
    dma = pltpu.SemaphoreType.DMA
    shape = jax.ShapeDtypeStruct
    k = (SLOTS,)
    return pl.pallas_call(
        back_kernel,
        in_specs=[hbm] * 13 + [vmem] * 5,
        out_specs=[vmem] * 6,
        out_shape=[shape((256, 2048), BF16), shape((4, 2048), F32), shape((64, 1536), F32), shape((16, 2048), F32),
                   shape((64, 2048), F32), shape((64, 2048), F32)],
        scratch_shapes=[
            pltpu.VMEM((2, 1024, 1024), BF16), pltpu.VMEM((2, 1024, 256), BF16),
            pltpu.VMEM((2, 2, 4, 4, 2, 64, 128), F32), pltpu.VMEM(k + (2, 4, 4, 64, 128), F32),
            pltpu.VMEM(k + (2, 2, 4, 32, 128), F32), pltpu.VMEM(k + (2, 2, 2, 4, 32, 128), F32),
            pltpu.VMEM(k + (2, 2, 32, 128), F32), pltpu.VMEM(k + (2, 2, 2, 32, 128), F32),
            pltpu.VMEM((4, 4, 4, 2048), F32),
            pltpu.VMEM((1024, 2048), BF16), pltpu.VMEM((1024, 1536), BF16), pltpu.VMEM((512, 1024), BF16),
            pltpu.VMEM((2, 1024, 384), BF16), pltpu.VMEM((1024, 128), BF16),
            pltpu.VMEM((1024, 128), F32), pltpu.VMEM((1024, 128), F32),
            pltpu.VMEM((2, 256, 1536), BF16), pltpu.VMEM((2, 256, 2048), BF16), pltpu.VMEM((2, 1024, 256), BF16),
            pltpu.VMEM((5, 4, 256, 256), BF16), pltpu.VMEM((8, 2, 128, 256), BF16), pltpu.VMEM((8, 2, 2, 128, 256), BF16),
            pltpu.VMEM((2, 1024, 256), F32), pltpu.VMEM((1024, 2048), BF16), pltpu.VMEM((2, 128, 2048), BF16),
            pltpu.VMEM((128, 1024), BF16), pltpu.VMEM((128, 1024), BF16),
            dma((2,)), dma((2,)), dma((2, 2)), dma((2, 3)), dma((2, 2)), dma, dma((LATE, 6)), dma((LATE, 6)),
            dma(k), dma(k), dma(k), dma(k), dma(k), dma(k), dma(k), dma(k), dma(k), dma(k),
            dma((4,)), dma((4,)), dma((8,)), dma((8,)), dma((8,)), dma((8,)),
            pltpu.SemaphoreType.REGULAR((5,)),
        ],
        compiler_params=pltpu.CompilerParams(collective_id=0, has_side_effects=True, vmem_limit_bytes=65400 * 1024),
        cost_estimate=pl.CostEstimate(flops=50_000_000_000, bytes_accessed=100_000_000, transcendentals=0),
        name='back',
    )(get, hmt, hat, dy_early, slope, qkv, w_out, w_down, w2, w_up, x_full, x_loc, dy_loc, ln_params, mean, rstd, cos_f, sin_f)


def place_kernel(gx, ln, qkv, out, up, down, o_gx, o_ln, o_qkv, o_out, o_up, o_down, b_gx, b_ln, b_qkv, b_out, b_up, b_down, b_rows, in_sem, out_sem):
    ins = [pltpu.make_async_copy(src, buf, in_sem.at[i]) for i, (src, buf) in enumerate(
        ((qkv, b_qkv), (gx, b_gx), (ln, b_ln), (out, b_out), (up, b_up), (down, b_down)))]
    outs = [pltpu.make_async_copy(buf, dst, out_sem.at[i]) for i, (buf, dst) in enumerate(
        ((b_rows, o_qkv), (b_gx, o_gx), (b_ln, o_ln), (b_out, o_out), (b_up, o_up), (b_down, o_down)))]
    for copy in ins:
        copy.start()
    for i in range(1, 6):
        ins[i].wait()
        outs[i].start()
    ins[0].wait()
    for g in range(4):
        for j in range(3):
            b_rows[:, j, g, :] = b_qkv[:, g * 384 + j * 128:g * 384 + j * 128 + 128]
    outs[0].start()
    for copy in outs:
        copy.wait()


def place_call(gx, ln, qkv, out, up, down):
    hbm = pl.BlockSpec(memory_space=pl.ANY)
    dma = pltpu.SemaphoreType.DMA
    arrays = (gx, ln, qkv, out, up, down)
    rows = (qkv.shape[0], 3, 4, 128)
    shapes = [jax.ShapeDtypeStruct(rows if v is qkv else v.shape, v.dtype) for v in arrays]
    return pl.pallas_call(
        place_kernel,
        in_specs=[hbm] * 6,
        out_specs=[hbm] * 6,
        out_shape=shapes,
        scratch_shapes=[pltpu.VMEM(v.shape, v.dtype) for v in arrays] + [pltpu.VMEM(rows, F32), dma((6,)), dma((6,))],
        compiler_params=pltpu.CompilerParams(vmem_limit_bytes=VMEM_LIMIT),
        name='place',
    )(*arrays)


def solution(mesh):
    def local_step(x_loc, dy_loc, ln_params, w_qkv, w_out, w_up, w_down):
        width, groups, slots, head_dim = w_qkv.shape
        cos_f, sin_f = (jnp.asarray(t) for t in rope_tables(4 * x_loc.shape[1], head_dim))
        w_rows = w_qkv.transpose(0, 2, 1, 3).reshape(width * slots * groups, head_dim)
        x_full, dy_early, hat, hmt, qkv, get, slope, w2, mean, rstd = front_call(x_loc[0], dy_loc[0], ln_params, cos_f, sin_f, w_rows, w_up)
        grad_x, g_ln, g_qkv, g_out, g_up, g_down = back_call(
            get, hmt, hat, dy_early, slope, qkv, w_out, w_down, w2, w_up, x_full, x_loc[0], dy_loc[0], ln_params, mean, rstd, cos_f, sin_f)
        grad_x, g_ln, g_qkv, g_out, g_up, g_down = place_call(grad_x, g_ln, g_qkv, g_out, g_up, g_down)
        return grad_x[None], g_ln, g_qkv.transpose(0, 2, 1, 3), g_out, g_up, g_down

    act_spec = P('dp', 'tp', None)
    in_specs = (act_spec, act_spec, P(None, None), P(None, 'tp', None, None), P('tp', None), P(None, 'tp'), P('tp', None))
    out_specs = (act_spec, P(None, None), P('dp', 'tp', None, None), P(('tp', 'dp'), None), P('dp', 'tp'), P(('tp', 'dp'), None))
    return jax.shard_map(local_step, mesh=mesh, in_specs=in_specs, out_specs=out_specs, check_vma=False)
```

```python
import functools

import jax
import jax.numpy as jnp
import numpy as np
from jax import lax
from jax.experimental import pallas as pl
from jax.experimental.pallas import tpu as pltpu
from jax.sharding import PartitionSpec as P

NORM_EPS = 1e-5
ROPE_BASE = 10000.0
MESH = pl.DeviceIdType.MESH
PIECES = 24
SLOTS = 8
STEPS = PIECES + 7
EARLY = 768
LATE = 5
VMEM_LIMIT = 60000 * 1024
F32 = jnp.float32
BF16 = jnp.bfloat16


def rope_tables(seq_len, head_dim):
    half_dim = head_dim // 2
    inv_freq = np.float32(ROPE_BASE) ** (np.float32(-2.0) * np.arange(half_dim, dtype=np.float32) / np.float32(head_dim))
    angles = np.arange(seq_len, dtype=np.float32)[:, None] * inv_freq[None, :].astype(np.float32)
    cos_t, sin_t = np.cos(angles), np.sin(angles)
    return np.concatenate([cos_t, cos_t], axis=1), np.concatenate([-sin_t, sin_t], axis=1)


def dot_nn(lhs, rhs):
    return lax.dot_general(lhs, rhs, (((1,), (0,)), ((), ())), preferred_element_type=F32)


def dot_nt(lhs, rhs):
    return lax.dot_general(lhs, rhs, (((1,), (1,)), ((), ())), preferred_element_type=F32)


def dot_tt(lhs, rhs):
    return lax.dot_general(lhs, rhs, (((0,), (0,)), ((), ())), preferred_element_type=F32)


def front_kernel(x_ref, dy_ref, ln_ref, cos_ref, sin_ref, wq_ref, wu_ref,
                 o_x, o_dy, o_ha, o_hm, o_qkv, o_gelu, o_slope, o_w, mean_ref, rstd_ref,
                 x_v, dy_v, w2, wu, wq_b, wq_f, slope, ha, hm, hat, hmt, get, qkv,
                 xs, xr, ds, dr, in_sem, wq_sem, out_sem, fin_sem):
    tp = lax.axis_index('tp')
    nxt, opp, prv = lax.rem(tp + 1, 4), lax.rem(tp + 2, 4), lax.rem(tp + 3, 4)
    d_model = x_ref.shape[1]
    rows = x_ref.shape[0]
    half = rows // 2
    part = wq_b.shape[1]
    barrier = pltpu.get_barrier_semaphore()
    for peer in (nxt, prv):
        pl.semaphore_signal(barrier, inc=1, device_id={'tp': peer}, device_id_type=MESH)

    def wq_copy(i):
        return pltpu.make_async_copy(wq_ref.at[pl.ds(i * part, part)], wq_b.at[i % 2], wq_sem.at[i % 2])

    dy_own = dy_ref.at[:, pl.ds(0, EARLY)]
    loads = [pltpu.make_async_copy(x_ref, x_v.at[tp], in_sem.at[0]), pltpu.make_async_copy(dy_own, dy_v.at[tp], in_sem.at[1]),
             pltpu.make_async_copy(wu_ref, wu, in_sem.at[2])]
    wq_copy(0).start()
    loads[0].start()
    wq_copy(1).start()
    loads[2].start()
    loads[1].start()
    pl.semaphore_wait(barrier, 2)

    A, B = pl.ds(0, half), pl.ds(half, half)

    def moves(src, buf, ssem, rsem):
        def one(i, ref, slot, piece, to):
            return pltpu.make_async_remote_copy(src_ref=ref, dst_ref=buf.at[slot, piece], send_sem=ssem.at[i], recv_sem=rsem.at[i],
                                                device_id={'tp': to}, device_id_type=MESH)
        return [one(0, src.at[A], tp, A, nxt), one(1, src.at[B], tp, B, prv), one(2, src.at[B], tp, B, nxt), one(3, src.at[A], tp, A, prv),
                one(4, buf.at[prv, A], prv, A, nxt), one(5, buf.at[nxt, B], nxt, B, prv)]

    xm = moves(x_ref, x_v, xs, xr)
    dm = moves(dy_own, dy_v, ds, dr)
    for i in range(4):
        xm[i].start()

    per = part // 12
    for i in range(wq_ref.shape[0] // part):
        wq_copy(i).wait()

        @pl.loop(0, part // 256)
        def _(r):
            at = pl.ds(pl.multiple_of(r * 256, 256), 256)
            wq_f[at, :] = wq_b[i % 2, at, :].astype(F32)

        if i + 2 < wq_ref.shape[0] // part:
            wq_copy(i + 2).start()
        for j in range(3):
            for g in range(4):
                w2[i * per:(i + 1) * per, g * 384 + j * 128:g * 384 + j * 128 + 128] = wq_f[pl.ds(j * 4 + g, per, stride=12), :].astype(BF16)
    w_out_copy = pltpu.make_async_copy(w2, o_w, fin_sem.at[8])
    w_out_copy.start()

    outs = {}

    def tokens(block, i):
        slot, side = block[i]
        return pl.ds(pl.multiple_of(slot * rows + side * half, half), half)

    def put(kind, n, buf, ref, block):
        for i in range(2):
            copy = pltpu.make_async_copy(buf.at[n % 2, pl.ds(i * half, half)], ref.at[tokens(block, i)], out_sem.at[kind, n % 2, i])
            copy.start()
            outs[kind, n % 2, i] = copy

    def put_t(kind, buf, ref, block):
        for i in range(2):
            copy = pltpu.make_async_copy(buf.at[:, pl.ds(i * half, half)], ref.at[:, tokens(block, i)], out_sem.at[kind, 0, i])
            copy.start()
            outs[kind, 0, i] = copy

    def free(kind, n):
        for i in range(2):
            if (kind, n % 2, i) in outs:
                outs.pop((kind, n % 2, i)).wait()

    def forward(block, n):
        s = n % 2
        for i in range(2):
            slot, side = block[i]

            @pl.loop(0, half // 32)
            def _(r):
                src = pl.ds(pl.multiple_of(side * half + r * 32, 32), 32)
                at = pl.ds(pl.multiple_of(i * half + r * 32, 32), 32)
                to = pl.ds(pl.multiple_of(slot * rows + side * half + r * 32, 32), 32)
                xf = x_v[slot, src, :].astype(F32)
                mean = jnp.mean(xf, axis=-1, keepdims=True)
                cen = xf - mean
                rstd = lax.rsqrt(jnp.mean(cen * cen, axis=-1, keepdims=True) + NORM_EPS)
                mean_ref[to, :] = mean
                rstd_ref[to, :] = rstd
                x_hat = cen * rstd
                ha[at, :] = (x_hat * ln_ref[0:1, :] + ln_ref[1:2, :]).astype(BF16)
                hm[at, :] = (x_hat * ln_ref[2:3, :] + ln_ref[3:4, :]).astype(BF16)

        for kind in (0, 1, 3):
            free(kind, 0)
        free(2, n)
        free(4, n)

        @pl.loop(0, d_model // 256)
        def _(c):
            cols = pl.ds(pl.multiple_of(c * 256, 256), 256)
            hat[cols, :] = ha[:, cols].T
            hmt[cols, :] = hm[:, cols].T

        put_t(0, hat, o_ha, block)
        put_t(1, hmt, o_hm, block)
        cos_t, sin_t = (jnp.concatenate([ref[tokens(block, 0), :], ref[tokens(block, 1), :]], axis=0) for ref in (cos_ref, sin_ref))

        @pl.loop(0, 4)
        def _(g):
            cols = pl.ds(pl.multiple_of(g * 384, 128), 384)
            t = dot_nn(ha[...], w2[:, cols]).astype(BF16)
            for j in range(2):
                v = t[:, j * 128:j * 128 + 128].astype(F32)
                qkv[s, :, pl.ds(pl.multiple_of(g * 384 + j * 128, 128), 128)] = (v * cos_t + pltpu.roll(v, 64, 1) * sin_t).astype(BF16)
            qkv[s, :, pl.ds(pl.multiple_of(g * 384 + 256, 128), 128)] = t[:, 256:384]

        put(2, n, qkv, o_qkv, block)

        @pl.loop(0, 4)
        def _(c):
            cols = pl.ds(pl.multiple_of(c * 512, 512), 512)
            u = dot_nn(hm[...], wu[:, cols]).astype(BF16).astype(F32)
            cdf = 0.5 * (1.0 + lax.erf(u * (0.5 ** 0.5)))
            get[cols, :] = (u * cdf).astype(BF16).T
            slope[s, :, cols] = cdf + u * (jnp.exp(-0.5 * u * u) * ((2.0 * jnp.pi) ** -0.5))

        put_t(3, get, o_gelu, block)
        put(4, n, slope, o_slope, block)

    fins = []

    def keep(buf, ref, slot, i):
        copy = pltpu.make_async_copy(buf.at[slot], ref.at[pl.ds(pl.multiple_of(slot * rows, rows), rows)], fin_sem.at[i])
        copy.start()
        fins.append(copy)

    loads[0].wait()
    loads[2].wait()
    keep(x_v, o_x, tp, 0)
    forward(((tp, 0), (tp, 1)), 0)
    xm[0].wait_recv()
    xm[4].start()
    xm[1].wait_recv()
    xm[5].start()
    for i in range(4):
        dm[i].start()
    forward(((prv, 0), (nxt, 1)), 1)
    xm[2].wait_recv()
    xm[3].wait_recv()
    keep(x_v, o_x, prv, 1)
    keep(x_v, o_x, nxt, 2)
    forward(((prv, 1), (nxt, 0)), 2)
    dm[0].wait_recv()
    dm[4].start()
    dm[1].wait_recv()
    dm[5].start()
    xm[4].wait_recv()
    xm[5].wait_recv()
    keep(x_v, o_x, opp, 3)
    forward(((opp, 0), (opp, 1)), 3)
    loads[1].wait()
    for i in range(2, 6):
        dm[i].wait_recv()
    for i, slot in enumerate((tp, prv, nxt, opp)):
        keep(dy_v, o_dy, slot, 4 + i)
    for m in xm + dm:
        m.wait_send()
    for copy in list(outs.values()) + fins + [w_out_copy]:
        copy.wait()


def front_call(x_loc, dy_loc, ln_params, cos_f, sin_f, w_rows, w_up):
    r, d = x_loc.shape
    t, f, n = 4 * r, w_up.shape[1], w_rows.shape[0] * 128 // d
    part = w_rows.shape[0] // 4
    hbm = pl.BlockSpec(memory_space=pl.ANY)
    vmem = pl.BlockSpec(memory_space=pltpu.VMEM)
    dma = pltpu.SemaphoreType.DMA
    shape = jax.ShapeDtypeStruct
    return pl.pallas_call(
        front_kernel,
        in_specs=[hbm, hbm, vmem, vmem, vmem, hbm, hbm],
        out_specs=[hbm] * 8 + [vmem] * 2,
        out_shape=[shape((t, d), BF16), shape((t, EARLY), BF16), shape((d, t), BF16), shape((d, t), BF16),
                   shape((t, n), BF16), shape((f, t), BF16), shape((t, f), F32), shape((d, n), BF16),
                   shape((t, 1), F32), shape((t, 1), F32)],
        scratch_shapes=[
            pltpu.VMEM((4, r, d), BF16), pltpu.VMEM((4, r, EARLY), BF16),
            pltpu.VMEM((d, n), BF16), pltpu.VMEM((d, f), BF16),
            pltpu.VMEM((2, part, 128), BF16), pltpu.VMEM((part, 128), F32),
            pltpu.VMEM((2, r, f), F32),
            pltpu.VMEM((r, d), BF16), pltpu.VMEM((r, d), BF16),
            pltpu.VMEM((d, r), BF16), pltpu.VMEM((d, r), BF16), pltpu.VMEM((f, r), BF16),
            pltpu.VMEM((2, r, n), BF16),
            dma((6,)), dma((6,)), dma((6,)), dma((6,)), dma((3,)), dma((2,)), dma((5, 2, 2)), dma((9,)),
        ],
        compiler_params=pltpu.CompilerParams(collective_id=1, has_side_effects=True, vmem_limit_bytes=64000 * 1024),
        cost_estimate=pl.CostEstimate(flops=2 * t * d * (n + f), bytes_accessed=70_000_000, transcendentals=2 * t * f),
        name='front',
    )(x_loc, dy_loc, ln_params, cos_f, sin_f, w_rows, w_up)


def back_kernel(get_ref, hmt_ref, hat_ref, dyp_ref, slope_ref, qkv_ref, wo_ref, wd_ref, w2_ref, wup_ref, x_ref, xloc_ref, dyloc_ref,
                ln_ref, mean_ref, rstd_ref, cos_ref, sin_ref,
                o_gx, o_ln, o_qkv, o_out, o_up, o_down,
                a_buf, b_buf, p_buf, d_buf, l1, f1, l2, f2, lnb, dh_v, dproj_v, ctxt, qkv_b, dctx_b, dk_s, dv_s,
                wq_t, wu_t, x_t, c_buf, cl1, cf1, sl_buf, dy_v, wo_t, kt, vt,
                a_sem, dy_sem, h_sem, t_sem, d_sem, g_sem, gs, gr, ds, dr, s_l1, r_l1, s_f1, r_f1, s_l2, r_l2, s_f2, r_f2, ln_s, ln_r,
                cs_l1, cr_l1, cs_f1, cr_f1, credit):
    tp = lax.axis_index('tp')
    dp = lax.axis_index('dp')
    core = lax.rem(dp, 2)
    y = lax.rem(dp // 2, 4)
    z = dp // 8
    partner = {'dp': dp + 1 - 2 * core}
    n_head = 4
    hd = 128
    blk = 256
    scale = hd ** -0.5

    def dev_y(i):
        return {'dp': z * 8 + i * 2 + core}

    def dev_z(i):
        return {'dp': i * 8 + y * 2 + core}

    def dev_x(i):
        return {'tp': i}

    def ring(i, d):
        return lax.rem(i + d, 4)

    def al(i, m):
        return pl.multiple_of(i * m, m)

    barrier = pltpu.get_barrier_semaphore()
    peers = [partner]
    for d in (1, 2, 3):
        peers += [dev_x(ring(tp, d)), dev_y(ring(y, d)), dev_z(ring(z, d))]
    for peer in peers:
        pl.semaphore_signal(barrier, inc=1, device_id=peer, device_id_type=MESH)

    def load_a(src, h):
        return pltpu.make_async_copy(src.at[pl.ds(al(h, 1024), 1024)], a_buf.at[h], a_sem.at[h])

    def load_x():
        return [pltpu.make_async_copy(xloc_ref.at[:, pl.ds(256 * u, 256)], x_t.at[u // 4, pl.ds(256 * (u % 4), 256)], g_sem) for u in range(8)]

    def load_head(h, slot):
        return [pltpu.make_async_copy(qkv_ref.at[:, pl.ds(pl.multiple_of(h * 384, 128), 384)], qkv_b.at[slot], h_sem.at[slot, 0]),
                pltpu.make_async_copy(wo_ref.at[pl.ds(al(h, 128), 128)], wo_t.at[slot], h_sem.at[slot, 1])]

    def load_d(k, slot):
        at = pl.ds(al(k, 256), 256)
        return [pltpu.make_async_copy(wd_ref.at[at], wu_t.at[slot], d_sem.at[slot, 0]),
                pltpu.make_async_copy(slope_ref.at[:, at], sl_buf.at[slot], d_sem.at[slot, 1])]

    def load_t(u, slot):
        at = pl.ds(al(u, 256), 256)
        return [pltpu.make_async_copy(w2_ref.at[at], wq_t.at[slot], t_sem.at[slot, 0]),
                pltpu.make_async_copy(wup_ref.at[at], wu_t.at[slot], t_sem.at[slot, 1]),
                pltpu.make_async_copy(x_ref.at[:, at], x_t.at[slot], t_sem.at[slot, 2])]

    def start(copies):
        for copy in copies:
            copy.start()

    def wait(copies):
        for copy in copies:
            copy.wait()

    for h in range(2):
        load_a(get_ref, jnp.int32(h)).start()
    early = pltpu.make_async_copy(dyp_ref, dy_v.at[:, pl.ds(0, EARLY)], dy_sem.at[0])
    early.start()
    late = pltpu.make_async_copy(dyloc_ref.at[:, pl.ds(EARLY, 256 * LATE)],
                                 dy_v.at[pl.ds(al(tp, 256), 256), pl.ds(EARLY, 256 * LATE)], dy_sem.at[1])
    late.start()
    start(load_head(jnp.int32(0), 0))
    start(load_d(jnp.int32(0), 0))
    pl.semaphore_wait(barrier, len(peers))

    def remote(src, dst, ssem, rsem, device):
        return pltpu.make_async_remote_copy(src_ref=src, dst_ref=dst, send_sem=ssem, recv_sem=rsem, device_id=device, device_id_type=MESH)

    def drain(ref, sem):
        pltpu.make_async_copy(ref, ref, sem).wait()

    def slice_copy(j, i):
        cols = pl.ds(pl.multiple_of(EARLY + j * 256, 256), 256)
        nxt, prv = ring(tp, 1), ring(tp, 3)
        owner, half, to = ((tp, 0, nxt), (tp, 1, prv), (tp, 1, nxt), (tp, 0, prv), (prv, 0, nxt), (nxt, 1, prv))[i]
        spot = dy_v.at[pl.ds(pl.multiple_of(owner * 256 + half * 128, 128), 128), cols]
        src = dyloc_ref.at[pl.ds(128 * half, 128), cols] if i < 4 else spot
        return remote(src, spot, gs.at[j, i], gr.at[j, i], dev_x(to))

    def slice_own(j):
        for i in range(4):
            slice_copy(j, i).start()

    def slice_on(j):
        for i in range(2):
            slice_copy(j, i).wait_recv()
            slice_copy(j, 4 + i).start()

    def slice_done(j):
        for i in range(2, 6):
            slice_copy(j, i).wait_recv()

    slice_own(jnp.int32(0))
    slice_own(jnp.int32(1))

    def pair_copy(p):
        slot = lax.rem(p, SLOTS)
        return remote(p_buf.at[lax.rem(p, 2), :, :, :, 1 - core], d_buf.at[slot], ds.at[slot], dr.at[slot], partner)

    def blk1(slot, col, i, half):
        rows = pl.ds(32 * half, 32)
        if col == 0:
            return d_buf.at[slot, 0, :, i, rows, :]
        return d_buf.at[slot, 1, i, :, rows, :]

    def blk2(slot, col, i, half):
        rows = pl.ds(32 * half, 32)
        if col == 0:
            return d_buf.at[slot, 0, i, y, rows, :]
        return d_buf.at[slot, 1, z, i, rows, :]

    me1 = (y, z)
    dev1 = (dev_y, dev_z)
    me2 = (z, y)
    dev2 = (dev_z, dev_y)

    def compute(p):
        ps = lax.rem(p, 2)

        @pl.when(p >= 2)
        def _():
            drain(p_buf.at[ps, :, :, :, 0], ds.at[lax.rem(p - 2, SLOTS)])

        @pl.when(p == 0)
        def _():
            early.wait()

        @pl.when(p == 3)
        def _():
            late.wait()

        @pl.when((p >= 3) & (p < 6))
        def _():
            slice_done(p - 3)

        @pl.when(p == 5)
        def _():
            slice_done(p - 2)
            slice_done(p - 1)

        @pl.when(p < 8)
        def _():
            b_buf[ps] = dy_v[:, pl.ds(al(p, 256), 256)]

        @pl.when((p >= 8) & (p < 16))
        def _():
            b_buf[ps] = dh_v[:, pl.ds(al(p - 8, 256), 256)]

        @pl.when((p >= 16) & (p < 22))
        def _():
            b_buf[ps] = dproj_v[:, pl.ds(al(p - 16, 256), 256)]

        @pl.when(p < 22)
        def _():
            @pl.loop(0, 2)
            def _(h):
                @pl.when((p == 0) | (p == 8) | (p == 16))
                def _():
                    load_a(get_ref, h).wait()

                tile = dot_nn(a_buf[h], b_buf[ps])
                for i in range(16):
                    for col in range(2):
                        p_buf[ps, col, 2 * h + i // 8, (i // 2) % 4, i % 2] = tile[64 * i:64 * i + 64, 128 * col:128 * col + 128]

                @pl.when(p == 7)
                def _():
                    load_a(hmt_ref, h).start()

                @pl.when(p == 15)
                def _():
                    load_a(hat_ref, h).start()

        @pl.when(p >= 22)
        def _():
            @pl.loop(0, 4)
            def _(k):
                tile = dot_nn(ctxt[...], dy_v[:, pl.ds(pl.multiple_of((p - 22) * 1024 + k * 256, 256), 256)])
                for i in range(32):
                    for col in range(2):
                        p_buf[ps, col, i // 8, (i // 2) % 4, i % 2, pl.ds(al(k, 16), 16), :] = tile[16 * i:16 * i + 16, 128 * col:128 * col + 128]

        @pl.when(p >= SLOTS)
        def _():
            pl.semaphore_wait(credit.at[0], 1)

        pair_copy(p).start()

    def first(blk, slot, me, dev, lands, finals, s_a, r_a, s_b, r_b):
        for col in range(2):
            nxt, opp, prv = ring(me[col], 1), ring(me[col], 2), ring(me[col], 3)
            remote(blk(slot, col, opp, 0), lands.at[slot, col, 0], s_a.at[slot], r_a.at[slot], dev[col](nxt)).start()
            remote(blk(slot, col, opp, 1), lands.at[slot, col, 1], s_a.at[slot], r_a.at[slot], dev[col](prv)).start()
        for col in range(2):
            nxt, prv = ring(me[col], 1), ring(me[col], 3)
            remote(blk(slot, col, nxt, 1), finals.at[slot, col, 0, 1], s_b.at[slot], r_b.at[slot], dev[col](nxt)).start()
            remote(blk(slot, col, prv, 0), finals.at[slot, col, 0, 0], s_b.at[slot], r_b.at[slot], dev[col](prv)).start()

    def second(blk, slot, me, dev, lands, finals, r_a, s_b, r_b):
        drain(lands.at[slot], r_a.at[slot])
        for col in range(2):
            nxt, prv = ring(me[col], 1), ring(me[col], 3)
            for half, to in ((0, nxt), (1, prv)):
                ref = blk(slot, col, to, half)
                ref[...] = ref[...] + lands[slot, col, half]
                remote(ref, finals.at[slot, col, 1, half], s_b.at[slot], r_b.at[slot], dev[col](to)).start()

    def stage_s(q):
        slot = lax.rem(q, SLOTS)
        ps = lax.rem(q, 2)
        drain(d_buf.at[slot], dr.at[slot])

        @pl.loop(0, 8)
        def _(i):
            col, zi = i // 4, lax.rem(i, 4)
            d_buf[slot, col, zi] = d_buf[slot, col, zi] + p_buf[ps, col, zi, :, core]

        @pl.when(q >= SLOTS)
        def _():
            for i in range(1, 5):
                pl.semaphore_wait(credit.at[i], 1)

        first(blk1, slot, me1, dev1, l1, f1, s_l1, r_l1, s_f1, r_f1)

    def stage_l1(q):
        second(blk1, lax.rem(q, SLOTS), me1, dev1, l1, f1, r_l1, s_f1, r_f1)

    def stage_f1(q):
        slot = lax.rem(q, SLOTS)
        drain(f1.at[slot], r_f1.at[slot])
        for col in range(2):
            for half in range(2):
                ref = blk1(slot, col, me1[col], half)
                ref[...] = ref[...] + (f1[slot, col, 0, half] + f1[slot, col, 1, half])
        first(blk2, slot, me2, dev2, l2, f2, s_l2, r_l2, s_f2, r_f2)

    def stage_l2(q):
        second(blk2, lax.rem(q, SLOTS), me2, dev2, l2, f2, r_l2, s_f2, r_f2)

    def stage_f2(q):
        slot = lax.rem(q, SLOTS)
        drain(f2.at[slot], r_f2.at[slot])
        for col in range(2):
            for half in range(2):
                rows = pl.ds(32 * half, 32)
                val = blk2(slot, col, me2[col], half)[...] + (f2[slot, col, 0, half] + f2[slot, col, 1, half])
                for out, lo, hi in ((o_down, 0, 8), (o_up, 8, 16), (o_qkv, 16, 22)):
                    @pl.when((q >= lo) & (q < hi))
                    def _():
                        out[rows, pl.ds(pl.multiple_of((q - lo) * 256 + col * 128, 128), 128)] = val

                @pl.when(q >= 22)
                def _():
                    for k in range(2):
                        at = (q - 22) * 1024 + (2 * half + k) * 256 + col * 128
                        o_out[:, pl.ds(pl.multiple_of(at, 128), 128)] = val[16 * k:16 * k + 16, :]
        drain(l1.at[slot], s_l1.at[slot])
        drain(f1.at[slot], s_f1.at[slot])
        drain(l2.at[slot], s_l2.at[slot])
        drain(f2.at[slot], s_f2.at[slot])

        @pl.when(q < PIECES - SLOTS)
        def _():
            to = (partner, dev_y(ring(y, 1)), dev_y(ring(y, 3)), dev_z(ring(z, 1)), dev_z(ring(z, 3)))
            for i in range(5):
                pl.semaphore_signal(credit.at[i], inc=1, device_id=to[i], device_id_type=MESH)

    def ln_send(stage):
        me, dev, n = ((core, None, 2), (tp, dev_x, 4), (y, dev_y, 4), (z, dev_z, 4))[stage]
        for d in range(1, n):
            to = partner if dev is None else dev(ring(me, d))
            remote(lnb.at[stage, me], lnb.at[stage, me], ln_s.at[stage], ln_r.at[stage], to).start()

    def ln_sum(stage):
        n = 2 if stage == 0 else 4
        ref = lnb.at[stage, pl.ds(0, n - 1)]
        drain(ref, ln_r.at[stage])
        drain(ref, ln_s.at[stage])
        if n == 2:
            return lnb[0, 0] + lnb[0, 1]
        return (lnb[stage, 0] + lnb[stage, 1]) + (lnb[stage, 2] + lnb[stage, 3])

    def unrope(d, rows):
        d = d.astype(BF16).astype(F32)
        return (d * cos_ref[rows, :] - pltpu.roll(d, hd // 2, 1) * sin_ref[rows, :]).astype(BF16)

    def attend(h, side):
        hs = lax.rem(h, 2)

        def cols(j):
            return pl.ds(pl.multiple_of(h * 384 + j * 128, 128), 128)

        if side == 0:
            wait(load_head(h, hs))

            @pl.when(h < n_head - 1)
            def _():
                start(load_head(h + 1, 1 - hs))

            dctx_b[...] = dot_nt(dy_v[...], wo_t[hs]).astype(BF16)
            kt[...] = qkv_b[hs, :, hd:2 * hd].T
            vt[...] = qkv_b[hs, :, 2 * hd:3 * hd].T
            dk_s[...] = jnp.zeros_like(dk_s)
            dv_s[...] = jnp.zeros_like(dv_s)

        for i in ((0, 3), (1, 2))[side]:
            rows, lo, n = slice(i * blk, (i + 1) * blk), i * blk, (i + 1) * blk
            qi, dci = qkv_b[hs, rows, 0:hd], dctx_b[rows, :]
            kn, vn = qkv_b[hs, :n, hd:2 * hd], qkv_b[hs, :n, 2 * hd:3 * hd]
            s = dot_nt(kn, qi)
            seen = lax.broadcasted_iota(jnp.int32, (blk, blk), 0) <= lax.broadcasted_iota(jnp.int32, (blk, blk), 1)
            diag = jnp.where(seen, s[lo:, :], -1e30)
            s = jnp.concatenate([s[:lo, :], diag], axis=0) if lo else diag
            e = jnp.exp((s - jnp.max(s, axis=0, keepdims=True)) * scale)
            p = e * (1.0 / jnp.sum(e, axis=0, keepdims=True))
            pb = p.astype(BF16)
            ctxt[pl.ds(al(h, hd), hd), rows] = dot_nn(vt[:, :n], pb).astype(BF16)
            dp_ = dot_nt(vn, dci).astype(BF16).astype(F32)
            dsb = (p * (dp_ - jnp.sum(p * dp_, axis=0, keepdims=True)) * scale).astype(BF16)
            dproj_v[rows, cols(0)] = unrope(dot_nn(kt[:, :n], dsb).T, rows)
            dk_s[:n, :] = dk_s[:n, :] + dot_nn(dsb, qi)
            dv_s[:n, :] = dv_s[:n, :] + dot_nn(pb, dci)
        if side == 1:
            @pl.loop(0, 4)
            def _(m):
                at = pl.ds(al(m, blk), blk)
                dproj_v[at, cols(1)] = unrope(dk_s[at, :], at)
                dproj_v[at, cols(2)] = dv_s[at, :].astype(BF16)

    def down(k):
        ks = lax.rem(k, 2)
        wait(load_d(k, ks))

        @pl.when(k < 7)
        def _():
            start(load_d(k + 1, 1 - ks))

        d_gelu = dot_nt(dy_v[...], wu_t[ks]).astype(BF16).astype(F32)
        dh_v[:, pl.ds(al(k, 256), 256)] = (d_gelu * sl_buf[ks]).astype(BF16)

    def inputs(u):
        us = lax.rem(u, 2)
        cs = lax.rem(u, 5)
        wait(load_t(u, us))

        @pl.when(u < 7)
        def _():
            start(load_t(u + 1, 1 - us))

        at = pl.ds(al(u, 256), 256)
        gain_a, gain_m = ln_ref[0:1, at], ln_ref[2:3, at]
        sums = []
        for m in range(2):
            rows = slice(512 * m, 512 * m + 512)
            dha = dot_nt(dproj_v[rows, :], wq_t[us]).astype(BF16).astype(F32)
            dhm = dot_nt(dh_v[rows, :], wu_t[us]).astype(BF16).astype(F32)
            x_hat = (x_t[us, rows, :].astype(F32) - mean_ref[rows, :]) * rstd_ref[rows, :]
            c = (dha * gain_a + dhm * gain_m).astype(BF16)
            c_buf[cs, 2 * m] = c[:256]
            c_buf[cs, 2 * m + 1] = c[256:]
            sums.append([jnp.sum(v, axis=0, keepdims=True) for v in (dha * x_hat, dha, dhm * x_hat, dhm)])
        for i in range(4):
            lnb[0, core, i:i + 1, at] = sums[0][i] + sums[1][i]
        nxt, opp, prv = ring(tp, 1), ring(tp, 2), ring(tp, 3)
        remote(c_blk(u, opp, 0), cl1.at[u, 0], cs_l1.at[u], cr_l1.at[u], dev_x(nxt)).start()
        remote(c_blk(u, opp, 1), cl1.at[u, 1], cs_l1.at[u], cr_l1.at[u], dev_x(prv)).start()
        remote(c_blk(u, nxt, 1), cf1.at[u, 0, 1], cs_f1.at[u], cr_f1.at[u], dev_x(nxt)).start()
        remote(c_blk(u, prv, 0), cf1.at[u, 0, 0], cs_f1.at[u], cr_f1.at[u], dev_x(prv)).start()

    def c_blk(u, i, half):
        return c_buf.at[lax.rem(u, 5), i, pl.ds(128 * half, 128), :]

    def c_second(u):
        drain(cl1.at[u], cr_l1.at[u])
        for half, to in ((0, ring(tp, 1)), (1, ring(tp, 3))):
            ref = c_blk(u, to, half)
            ref[...] = (ref[...].astype(F32) + cl1[u, half].astype(F32)).astype(BF16)
            remote(ref, cf1.at[u, 1, half], cs_f1.at[u], cr_f1.at[u], dev_x(to)).start()

    def c_final(u):
        drain(cf1.at[u], cr_f1.at[u])
        for half in range(2):
            sl_buf[u // 4, pl.ds(pl.multiple_of(lax.rem(u, 4) * 256 + 128 * half, 128), 128), :] = c_blk(u, tp, half)[...].astype(F32) + (
                cf1[u, 0, half].astype(F32) + cf1[u, 1, half].astype(F32))
        drain(cl1.at[u], cs_l1.at[u])
        drain(cf1.at[u], cs_f1.at[u])

    def last():
        drain(x_t, g_sem)

        @pl.loop(0, 8)
        def _(r):
            def across(ref):
                return jnp.concatenate([ref[u // 4, pl.ds(pl.multiple_of(256 * (u % 4) + r * 32, 32), 32), :] for u in range(8)], axis=1).astype(F32)

            own = pl.ds(pl.multiple_of(tp * 256 + r * 32, 32), 32)
            rstd = rstd_ref[own, :]
            c = across(sl_buf)
            x_hat = (across(x_t) - mean_ref[own, :]) * rstd
            dx = rstd * (c - jnp.mean(c, axis=-1, keepdims=True) - x_hat * jnp.mean(c * x_hat, axis=-1, keepdims=True))
            o_gx[pl.ds(al(r, 32), 32), :] = (dy_v[own, :].astype(F32) + dx).astype(BF16)

    @pl.loop(0, STEPS)
    def _(p):
        @pl.when(p < PIECES)
        def _():
            compute(p)

        @pl.when(p < LATE)
        def _():
            slice_on(p)

        @pl.when(p < LATE - 2)
        def _():
            slice_own(p + 2)

        for lag, stage in ((7, stage_f2), (6, stage_l2), (5, stage_f1), (3, stage_l1), (1, stage_s)):
            @pl.when((p >= lag) & (p < PIECES + lag))
            def _():
                stage(p - lag)

        @pl.when((p >= 21) & (p < 29))
        def _():
            c_final(p - 21)

        @pl.when((p >= 19) & (p < 27))
        def _():
            c_second(p - 19)

        @pl.when((p >= 5) & (p < 13))
        def _():
            down(p - 5)

        for side, steps in enumerate(((6, 9, 12, 15), (7, 10, 13, 16))):
            @pl.when((p == steps[0]) | (p == steps[1]) | (p == steps[2]) | (p == steps[3]))
            def _():
                attend(sum((p >= at).astype(jnp.int32) for at in steps[1:]), side)

        @pl.when(p == 10)
        def _():
            for j in range(LATE):
                for i in range(6):
                    slice_copy(j, i).wait_send()

        @pl.when(p == 14)
        def _():
            start(load_t(0, 0))

        @pl.when((p >= 17) & (p < 25))
        def _():
            inputs(p - 17)

        @pl.when(p == 25)
        def _():
            start(load_x())
            ln_send(0)

        for stage, me in ((1, tp), (2, y), (3, z)):
            @pl.when(p == 25 + stage)
            def _():
                lnb[stage, me] = ln_sum(stage - 1)
                ln_send(stage)

        @pl.when(p == 29)
        def _():
            last()

        @pl.when(p == 29)
        def _():
            o_ln[...] = ln_sum(3)

    for p in (PIECES - 2, PIECES - 1):
        drain(p_buf.at[p % 2, :, :, :, 0], ds.at[p % SLOTS])


def back_call(get, hmt, hat, dy_early, slope, qkv, w_out, w_down, w2, w_up, x_full, x_loc, dy_loc, ln_params, mean, rstd, cos_f, sin_f):
    hbm = pl.BlockSpec(memory_space=pl.ANY)
    vmem = pl.BlockSpec(memory_space=pltpu.VMEM)
    dma = pltpu.SemaphoreType.DMA
    shape = jax.ShapeDtypeStruct
    k = (SLOTS,)
    return pl.pallas_call(
        back_kernel,
        in_specs=[hbm] * 13 + [vmem] * 5,
        out_specs=[vmem] * 6,
        out_shape=[shape((256, 2048), BF16), shape((4, 2048), F32), shape((64, 1536), F32), shape((16, 2048), F32),
                   shape((64, 2048), F32), shape((64, 2048), F32)],
        scratch_shapes=[
            pltpu.VMEM((2, 1024, 1024), BF16), pltpu.VMEM((2, 1024, 256), BF16),
            pltpu.VMEM((2, 2, 4, 4, 2, 64, 128), F32), pltpu.VMEM(k + (2, 4, 4, 64, 128), F32),
            pltpu.VMEM(k + (2, 2, 4, 32, 128), F32), pltpu.VMEM(k + (2, 2, 2, 4, 32, 128), F32),
            pltpu.VMEM(k + (2, 2, 32, 128), F32), pltpu.VMEM(k + (2, 2, 2, 32, 128), F32),
            pltpu.VMEM((4, 4, 4, 2048), F32),
            pltpu.VMEM((1024, 2048), BF16), pltpu.VMEM((1024, 1536), BF16), pltpu.VMEM((512, 1024), BF16),
            pltpu.VMEM((2, 1024, 384), BF16), pltpu.VMEM((1024, 128), BF16),
            pltpu.VMEM((1024, 128), F32), pltpu.VMEM((1024, 128), F32),
            pltpu.VMEM((2, 256, 1536), BF16), pltpu.VMEM((2, 256, 2048), BF16), pltpu.VMEM((2, 1024, 256), BF16),
            pltpu.VMEM((5, 4, 256, 256), BF16), pltpu.VMEM((8, 2, 128, 256), BF16), pltpu.VMEM((8, 2, 2, 128, 256), BF16),
            pltpu.VMEM((2, 1024, 256), F32), pltpu.VMEM((1024, 2048), BF16), pltpu.VMEM((2, 128, 2048), BF16),
            pltpu.VMEM((128, 1024), BF16), pltpu.VMEM((128, 1024), BF16),
            dma((2,)), dma((2,)), dma((2, 2)), dma((2, 3)), dma((2, 2)), dma, dma((LATE, 6)), dma((LATE, 6)),
            dma(k), dma(k), dma(k), dma(k), dma(k), dma(k), dma(k), dma(k), dma(k), dma(k),
            dma((4,)), dma((4,)), dma((8,)), dma((8,)), dma((8,)), dma((8,)),
            pltpu.SemaphoreType.REGULAR((5,)),
        ],
        compiler_params=pltpu.CompilerParams(collective_id=0, has_side_effects=True, vmem_limit_bytes=65400 * 1024),
        cost_estimate=pl.CostEstimate(flops=50_000_000_000, bytes_accessed=100_000_000, transcendentals=0),
        name='back',
    )(get, hmt, hat, dy_early, slope, qkv, w_out, w_down, w2, w_up, x_full, x_loc, dy_loc, ln_params, mean, rstd, cos_f, sin_f)


def place_kernel(gx, ln, qkv, out, up, down, o_gx, o_ln, o_qkv, o_out, o_up, o_down, b_gx, b_ln, b_qkv, b_out, b_up, b_down, b_rows, in_sem, out_sem):
    ins = [pltpu.make_async_copy(src, buf, in_sem.at[i]) for i, (src, buf) in enumerate(
        ((qkv, b_qkv), (gx, b_gx), (ln, b_ln), (out, b_out), (up, b_up), (down, b_down)))]
    outs = [pltpu.make_async_copy(buf, dst, out_sem.at[i]) for i, (buf, dst) in enumerate(
        ((b_rows, o_qkv), (b_gx, o_gx), (b_ln, o_ln), (b_out, o_out), (b_up, o_up), (b_down, o_down)))]
    for copy in ins:
        copy.start()
    for i in range(1, 6):
        ins[i].wait()
        outs[i].start()
    ins[0].wait()
    for g in range(4):
        for j in range(3):
            b_rows[:, j, g, :] = b_qkv[:, g * 384 + j * 128:g * 384 + j * 128 + 128]
    outs[0].start()
    for copy in outs:
        copy.wait()


def place_call(gx, ln, qkv, out, up, down):
    hbm = pl.BlockSpec(memory_space=pl.ANY)
    dma = pltpu.SemaphoreType.DMA
    arrays = (gx, ln, qkv, out, up, down)
    rows = (qkv.shape[0], 3, 4, 128)
    shapes = [jax.ShapeDtypeStruct(rows if v is qkv else v.shape, v.dtype) for v in arrays]
    return pl.pallas_call(
        place_kernel,
        in_specs=[hbm] * 6,
        out_specs=[hbm] * 6,
        out_shape=shapes,
        scratch_shapes=[pltpu.VMEM(v.shape, v.dtype) for v in arrays] + [pltpu.VMEM(rows, F32), dma((6,)), dma((6,))],
        compiler_params=pltpu.CompilerParams(vmem_limit_bytes=VMEM_LIMIT),
        name='place',
    )(*arrays)


def solution(mesh):
    def local_step(x_loc, dy_loc, ln_params, w_qkv, w_out, w_up, w_down):
        width, groups, slots, head_dim = w_qkv.shape
        cos_f, sin_f = (jnp.asarray(t) for t in rope_tables(4 * x_loc.shape[1], head_dim))
        w_rows = w_qkv.transpose(0, 2, 1, 3).reshape(width * slots * groups, head_dim)
        x_full, dy_early, hat, hmt, qkv, get, slope, w2, mean, rstd = front_call(x_loc[0], dy_loc[0], ln_params, cos_f, sin_f, w_rows, w_up)
        grad_x, g_ln, g_qkv, g_out, g_up, g_down = back_call(
            get, hmt, hat, dy_early, slope, qkv, w_out, w_down, w2, w_up, x_full, x_loc[0], dy_loc[0], ln_params, mean, rstd, cos_f, sin_f)
        grad_x, g_ln, g_qkv, g_out, g_up, g_down = place_call(grad_x, g_ln, g_qkv, g_out, g_up, g_down)
        return grad_x[None], g_ln, g_qkv.transpose(0, 2, 1, 3), g_out, g_up, g_down

    act_spec = P('dp', 'tp', None)
    in_specs = (act_spec, act_spec, P(None, None), P(None, 'tp', None, None), P('tp', None), P(None, 'tp'), P('tp', None))
    out_specs = (act_spec, P(None, None), P('dp', 'tp', None, None), P(('tp', 'dp'), None), P('dp', 'tp'), P(('tp', 'dp'), None))
    return jax.shard_map(local_step, mesh=mesh, in_specs=in_specs, out_specs=out_specs, check_vma=False)
```
